768 devices in a mesh: tm: 8 (over x, core), space: 96 (over y, z).
Axes of the slice: x: 4, y: 8, z: 12, core: 2. Of those that a mesh axis runs over, the one named last changes fastest.
Arguments:
- start_value: float32 [8, 96, 512, 256], P('tm', 'space'), may hold values from -6 to 6
- old_nodes: float32 [8, 3, 96, 512, 256], P('tm', None, 'space'), may hold values from -6 to 6
- diffusivity: float32 [96, 512, 256], P('space'), may hold values from 0.2 to 2
Outputs:
- fine_nodes: float32 [8, 3, 96, 512, 256], P('tm', None, 'space')
- next_start: float32 [8, 96, 512, 256], P('tm', 'space')
- next_coarse: float32 [8, 96, 512, 256], P('tm', 'space')
The draws below stay inside these ranges and needn't reach their ends.
All inputs are finite; a program needn't handle non-finite values.
Results may differ from the reference program's by a relative error of at most 0.0001.
Values sent between devices are 32-bit elements; how exact they have to be, the bound alone decides.
A program may use at most 64 MiB of HBM per device.

```python
import math
import jax
import jax.numpy as jnp
from jax import lax

NY = 512
NZ = 256
NODES = 3
CG_ITERS = 2
NX = 96
SLICES = 8


def shard_levels(key, extent, split, low, largest):
    factor_of = 1.0
    for dim, parts in split:
        heights = jax.random.uniform(jax.random.fold_in(jax.random.fold_in(key, 6), dim), (parts,), jnp.float32, low / len(split), largest / len(split))
        factor_of = factor_of * jnp.repeat(jnp.exp(heights), extent[dim] // parts).reshape((-1,) + (1,) * (len(extent) - 1 - dim))
    return factor_of


def bell_draw(own_key, shape, scale, most, cuts=(), kind=jnp.bfloat16):
    array = scale * jax.random.normal(own_key, shape, jnp.float32)
    if cuts:
        array = array * shard_levels(own_key, shape, cuts, -0.22, 0.18)
    return jnp.clip(array, -most, most).astype(kind)


def setup_inputs(seed: int = 0) -> dict:
    streams_of = jax.random.split(jax.random.key(seed), 4)
    start_value = bell_draw(streams_of[0], (SLICES, NX, NY, NZ), 1.0, 6.0, ((0, 8), (1, 96)), jnp.float32)
    old_nodes = bell_draw(streams_of[1], (SLICES, NODES, NX, NY, NZ), 1.0, 6.0, ((0, 8), (2, 96)), jnp.float32)
    diffusivity = jnp.clip(jnp.exp(math.log(2.0) - 2.3025851 * jax.random.uniform(streams_of[2], (NX, NY, NZ), jnp.float32) ** shard_levels(streams_of[2], (NX, NY, NZ), ((0, 96),), -0.2, 0.2)), 0.2, 2.0)
    return dict(start_value=start_value, old_nodes=old_nodes, diffusivity=diffusivity)


STEP = 2.0
ROOT_SIX = math.sqrt(6.0)
NODE_TIMES = [(4.0 - ROOT_SIX) / 10.0, (4.0 + ROOT_SIX) / 10.0, 1.0]
COLLOC = [[(88.0 - 7.0 * ROOT_SIX) / 360.0, (296.0 - 169.0 * ROOT_SIX) / 1800.0, (-2.0 + 3.0 * ROOT_SIX) / 225.0], [(296.0 + 169.0 * ROOT_SIX) / 1800.0, (88.0 + 7.0 * ROOT_SIX) / 360.0, (-2.0 - 3.0 * ROOT_SIX) / 225.0], [(16.0 - ROOT_SIX) / 36.0, (16.0 + ROOT_SIX) / 36.0, 1.0 / 9.0]]

def sweep_weight(row, column):
    below = COLLOC[row - 1][column] if row > 0 else 0.0
    return COLLOC[row][column] - below

def node_width(row):
    below = NODE_TIMES[row - 1] if row > 0 else 0.0
    return NODE_TIMES[row] - below

def neighbour(field, dim, forward):
    length = field.shape[dim]
    edge = jnp.zeros_like(lax.slice_in_dim(field, 0, 1, axis=dim))
    if forward:
        return jnp.concatenate([lax.slice_in_dim(field, 1, length, axis=dim), edge], axis=dim)
    return jnp.concatenate([edge, lax.slice_in_dim(field, 0, length - 1, axis=dim)], axis=dim)

def face_table(kappa):
    faces = []
    for dim in range(3):
        for forward in (True, False):
            faces.append(0.5 * (kappa + neighbour(kappa, dim, forward)))
    total = faces[0] + faces[1] + faces[2] + faces[3] + faces[4] + faces[5]
    return (faces, total)

def apply_heat(field, faces, total):
    result = faces[0] * neighbour(field, 0, True) + faces[1] * neighbour(field, 0, False)
    result = result + faces[2] * neighbour(field, 1, True) + faces[3] * neighbour(field, 1, False)
    result = result + faces[4] * neighbour(field, 2, True) + faces[5] * neighbour(field, 2, False)
    return result - total * field

def combine(weights, images):
    summed = weights[0] * images[0]
    for column in range(1, 3):
        summed = summed + weights[column] * images[column]
    return summed

def solve(guess, residual, width, faces, total):
    iterate = guess
    direction = residual
    norm_now = jnp.sum(residual * residual)
    for sweep in range(CG_ITERS):
        product = direction - width * apply_heat(direction, faces, total)
        step_size = norm_now / jnp.sum(direction * product)
        iterate = iterate + step_size * direction
        if sweep + 1 < CG_ITERS:
            residual = residual - step_size * product
            norm_next = jnp.sum(residual * residual)
            direction = residual + norm_next / norm_now * direction
            norm_now = norm_next
    return iterate

def reference(start_value, old_nodes, diffusivity):
    faces, total = face_table(diffusivity)

    def one_slice(pair):
        begin, previous_nodes = pair
        images = [apply_heat(previous_nodes[column], faces, total) for column in range(3)]
        previous = begin
        fresh = []
        for row in range(3):
            weights = [sweep_weight(row, column) for column in range(3)]
            residual = previous - previous_nodes[row] + STEP * combine(weights, images)
            result = solve(previous_nodes[row], residual, STEP * node_width(row), faces, total)
            fresh.append(result)
            previous = result
        coarse_res = begin - previous_nodes[2] + STEP * combine(COLLOC[2], images)
        coarse_end = solve(previous_nodes[2], coarse_res, STEP, faces, total)
        return (jnp.stack(fresh), coarse_end)
    fine_nodes, coarse_ends = lax.map(one_slice, (start_value, old_nodes))
    next_start = jnp.concatenate([start_value[:1], fine_nodes[:-1, 2]], axis=0)
    next_coarse = jnp.concatenate([start_value[:1], coarse_ends[:-1]], axis=0)
    return (fine_nodes, next_start, next_coarse)
```

```python
import functools
import math

import jax
import jax.numpy as jnp
from jax import lax
from jax.experimental import pallas as pl
from jax.experimental.pallas import tpu as pltpu
from jax.sharding import Mesh
from jax.sharding import PartitionSpec as P

MESH = pl.DeviceIdType.MESH
SPACE = ("y", "z")
ROWS_Y = 8
STEP = 2.0
ROOT_SIX = math.sqrt(6.0)
NODE_TIMES = [(4.0 - ROOT_SIX) / 10.0, (4.0 + ROOT_SIX) / 10.0, 1.0]
COLLOC = [
    [
        (88.0 - 7.0 * ROOT_SIX) / 360.0,
        (296.0 - 169.0 * ROOT_SIX) / 1800.0,
        (-2.0 + 3.0 * ROOT_SIX) / 225.0,
    ],
    [
        (296.0 + 169.0 * ROOT_SIX) / 1800.0,
        (88.0 + 7.0 * ROOT_SIX) / 360.0,
        (-2.0 - 3.0 * ROOT_SIX) / 225.0,
    ],
    [(16.0 - ROOT_SIX) / 36.0, (16.0 + ROOT_SIX) / 36.0, 1.0 / 9.0],
]
WEIGHT = [
    [STEP * (COLLOC[m][j] - (COLLOC[m - 1][j] if m else 0.0)) for j in range(3)] for m in range(3)
]
WIDTH = [STEP * (NODE_TIMES[m] - (NODE_TIMES[m - 1] if m else 0.0)) for m in range(3)]
PAD = 8
BLOCK = 32
CHUNKS = 4

PADDED = ["k", "u0", "u1", "u2", "a", "b", "d", "la", "v2", "v3", "vc"]
PLANES = ["s", "wxm", "wxp", "wym", "wyp", "wzm", "wzp", "dg", "lb", "ld", "lla", "lv2"]
PLANES += ["r2", "r3", "rc", "hv3", "hvc", "xu", "xrc", "xvc", "xr3", "xv3"]
PLANES += ["o0", "o1", "o2", "ons", "onc"]
SIDES = ["k", "u0", "u1", "u2", "a", "b", "d", "la", "v2"]


def kernel(dims, start_hbm, old_hbm, kappa_hbm, fine_hbm, ns_hbm, nc_hbm, padded, planes, sides,
           tiles, ztiles, zslots, yslots, xslots, send, recv, gsend, grecv, local):
    nt, ny, nz, rows, cols = dims
    chunk = rows // CHUNKS
    me_t, me_y, me_z = lax.axis_index("tm"), lax.axis_index("y"), lax.axis_index("z")
    place = me_y * nz + me_z
    slabs = ny * nz

    def chain(shift):
        other = lax.rem(place + (slabs + shift), slabs)
        return (me_t, lax.div(other, nz), lax.rem(other, nz))

    after, before = chain(1), chain(-1)
    next_t = lax.rem(me_t + 1, nt)
    last_t = lax.rem(me_t + (nt - 1), nt)

    def z_peer(k):
        return (me_t, me_y, lax.rem(me_z + k, nz))

    def y_peer(k, t=me_t):
        return (t, lax.rem(me_y + k, ny), me_z)

    def t_peer(k):
        return (lax.rem(me_t + k, nt), me_y, me_z)

    pad = {name: padded.at[i] for i, name in enumerate(PADDED)}
    plane = {name: planes.at[i] for i, name in enumerate(PLANES)}
    side = {name: sides.at[i] for i, name in enumerate(SIDES)}

    def inner(name, first=0, count=rows):
        return pad[name].at[pl.ds(PAD + first, count), :]

    loads = [(kappa_hbm, "k"), (old_hbm.at[0], "u0"), (old_hbm.at[1], "u1"), (old_hbm.at[2], "u2")]
    copies = [pltpu.make_async_copy(src, inner(name), local.at[i]) for i, (src, name) in enumerate(loads)]
    copies.append(pltpu.make_async_copy(start_hbm, plane["s"], local.at[4]))
    for copy in copies:
        copy.start()
    barrier = pltpu.get_barrier_semaphore()
    greeted = [after, before]
    greeted += [z_peer(k) for k in range(1, nz)]
    greeted += [y_peer(k) for k in range(1, ny)]
    greeted += [t_peer(k) for k in range(1, nt)]
    greeted += [y_peer(k, last_t) for k in range(ny)]
    for device in greeted:
        pl.semaphore_signal(barrier, inc=1, device_id=device, device_id_type=MESH)
    edge = jnp.zeros((PAD, cols), jnp.float32)
    for name in PADDED:
        pad[name][pl.ds(0, PAD), :] = edge
        pad[name][pl.ds(PAD + rows, PAD), :] = edge
    for copy in copies:
        copy.wait()
    pl.semaphore_wait(barrier, len(greeted))

    started = []

    def put(src, dst, device):
        i = len(started)
        copy = pltpu.make_async_remote_copy(
            src_ref=src, dst_ref=dst, send_sem=send.at[i], recv_sem=recv.at[i],
            device_id=device, device_id_type=MESH,
        )
        copy.start()
        started.append(copy)
        return copy

    def swap(name, c):
        here = inner(name, c * chunk, chunk)
        there = pl.ds(c * chunk, chunk)
        return [
            put(here, side[name].at[0, there, :], after),
            put(here, side[name].at[1, there, :], before),
        ]

    def swap_half(name, c, second):
        here = inner(name, c * chunk, chunk)
        there = pl.ds(c * chunk, chunk)
        up = (c < CHUNKS // 2) != second
        return [put(here, side[name].at[0 if up else 1, there, :], after if up else before)]

    def give_half(name, c):
        up = c < CHUNKS // 2
        here = inner(name, c * chunk, chunk)
        there = plane["h" + name].at[pl.ds(c * chunk, chunk), :]
        return [put(here, there, after if up else before)]

    def arrive(batch):
        for copy in batch:
            copy.wait_recv()

    share = rows // nt
    own = pl.multiple_of(me_t * share, share)
    mine = pl.ds(own, share)
    k_src = pad["k"].at[pl.ds(pl.multiple_of(PAD + own, PAD), share), :]
    k_in = [put(k_src, side["k"].at[0, mine, :], after), put(k_src, side["k"].at[1, mine, :], before)]
    u_in = []
    for c in range(CHUNKS):
        u_in.append([swap("u%d" % j, c) for j in range(3)])
    put_u = put(inner("u2"), plane["xu"], (next_t, me_y, me_z))
    arrive(k_in)
    for s in range(2):
        block = side["k"].at[s, mine, :]
        for k in range(1, nt):
            pltpu.make_async_remote_copy(
                src_ref=block, dst_ref=block, send_sem=gsend.at[0], recv_sem=grecv.at[0],
                device_id=t_peer(k), device_id_type=MESH,
            ).start()
    spread = side["k"].at[:, pl.ds(0, share * (nt - 1)), :]
    shared = pltpu.make_async_remote_copy(
        src_ref=spread, dst_ref=spread, send_sem=gsend.at[0], recv_sem=grecv.at[0],
        device_id=after, device_id_type=MESH,
    )
    shared.wait_recv()

    lane = lax.broadcasted_iota(jnp.int32, (BLOCK, cols), 1)
    first_lane, last_lane = lane == 0, lane == cols - 1
    zero = jnp.zeros((BLOCK, cols), jnp.float32)

    def to_right(x):
        return pltpu.roll(x, cols - 1, 1)

    def to_left(x):
        return pltpu.roll(x, 1, 1)

    def at(r):
        return pl.ds(r, BLOCK)

    def column(name, r):
        x = pad[name][pl.ds(r, BLOCK + 2 * PAD), :]
        return x[PAD:PAD + BLOCK], x[PAD - 1:PAD + BLOCK - 1], x[PAD + 1:PAD + BLOCK + 1]

    def sweep(first, count, body, carry):
        def step(i, carry):
            return body(pl.multiple_of(first + i * BLOCK, BLOCK), carry)

        return lax.fori_loop(0, count // BLOCK, step, carry)

    def weights(r, carry):
        k, k_down, k_up = column("k", r)
        row = lax.broadcasted_iota(jnp.int32, (BLOCK, cols), 0) + r
        k_before = jnp.where(place == 0, zero, side["k"][0, at(r), :])
        k_after = jnp.where(place == slabs - 1, zero, side["k"][1, at(r), :])
        faces = [
            0.5 * (k + k_before),
            0.5 * (k + k_after),
            0.5 * (k + k_down),
            0.5 * (k + k_up),
            0.5 * (k + jnp.where(first_lane, zero, to_left(k))),
            0.5 * (k + jnp.where(last_lane, zero, to_right(k))),
        ]
        total = faces[1] + faces[0] + faces[3] + faces[2] + faces[5] + faces[4]
        plane["dg"][at(r), :] = -total
        plane["wxm"][at(r), :] = jnp.where(place == 0, zero, faces[0])
        plane["wxp"][at(r), :] = jnp.where(place == slabs - 1, zero, faces[1])
        plane["wym"][at(r), :] = jnp.where(row == 0, zero, faces[2])
        plane["wyp"][at(r), :] = jnp.where(row == rows - 1, zero, faces[3])
        plane["wzm"][at(r), :] = jnp.where(first_lane, zero, faces[4])
        plane["wzp"][at(r), :] = jnp.where(last_lane, zero, faces[5])
        return carry

    sweep(0, rows, weights, 0)

    def heat(name, r):
        mid, down, up = column(name, r)
        out = plane["wxp"][at(r), :] * side[name][1, at(r), :]
        out = out + plane["wxm"][at(r), :] * side[name][0, at(r), :]
        out = out + plane["wyp"][at(r), :] * up + plane["wym"][at(r), :] * down
        out = out + plane["wzp"][at(r), :] * to_right(mid) + plane["wzm"][at(r), :] * to_left(mid)
        return mid, out + plane["dg"][at(r), :] * mid

    def fold(x):
        return jnp.sum(x.reshape(BLOCK // 8, 8, cols), axis=0)

    nothing = jnp.zeros((8, cols), jnp.float32)

    def quadratic(name, beside, weight, r):
        mid, _, up = column(name, r)
        twice = plane[weight][at(r), :] * beside[at(r), :]
        twice = twice + plane["wyp"][at(r), :] * up + plane["wzp"][at(r), :] * to_right(mid)
        return fold(mid * (twice + twice + plane["dg"][at(r), :] * mid))

    def moments(name, beside, c):
        weight = "wxm" if c < CHUNKS // 2 else "wxp"
        beside = beside(0 if c < CHUNKS // 2 else 1)
        return sweep(c * chunk, chunk, lambda r, acc: acc + quadratic(name, beside, weight, r), nothing)

    def lanes(acc):
        both = acc[:, 0:128]
        for i in range(1, cols // 128):
            both = both + acc[:, i * 128:(i + 1) * 128]
        return jnp.sum(both, axis=0, keepdims=True)

    def burst(src, slots, base, devices, sem):
        for k, device in enumerate(devices):
            pltpu.make_async_remote_copy(
                src_ref=src, dst_ref=slots.at[base + k], send_sem=gsend.at[sem], recv_sem=grecv.at[sem],
                device_id=device, device_id_type=MESH,
            ).start()
        whole = slots.at[pl.ds(base, len(devices))]
        return pltpu.make_async_remote_copy(
            src_ref=whole, dst_ref=whole, send_sem=gsend.at[sem], recv_sem=grecv.at[sem],
            device_id=after, device_id_type=MESH,
        )

    bursts = [shared]

    def reduce_z(n, accs):
        accs = accs + [nothing] * (8 - len(accs))
        tiles[n] = jnp.concatenate([lanes(acc) for acc in accs], axis=0)
        waits = burst(tiles.at[n], zslots.at[n], 0, [z_peer(k) for k in range(1, nz)], 1 + 3 * n)
        bursts.append(waits)
        return waits

    def reduce_y(n, waits, onward=False):
        waits.wait_recv()
        total = tiles[n]
        for k in range(nz - 1):
            total = total + zslots[n, k]
        ztiles[n] = total
        out = [burst(ztiles.at[n], yslots.at[n], 0, [y_peer(k) for k in range(1, ny)], 2 + 3 * n)]
        if onward:
            out.append(burst(ztiles.at[n], xslots, 0, [y_peer(k, next_t) for k in range(ny)], 3 + 3 * n))
        bursts.extend(out)
        return out

    def total_own(n, waits):
        waits.wait_recv()
        total = ztiles[n]
        for k in range(ny - 1):
            total = total + yslots[n, k]
        return jnp.sum(total, axis=1, keepdims=True)

    def total_last(waits):
        waits.wait_recv()
        total = xslots[0]
        for k in range(1, ny):
            total = total + xslots[k]
        return jnp.sum(total, axis=1, keepdims=True)

    def factors(sums, first, h):
        s0, s1, s2, s3 = [sums[first + i:first + i + 1, :] for i in range(4)]
        sigma = s1 / s0
        spread = jnp.maximum(s2 - s1 * sigma, 1e-30)
        bent = s3 - sigma * (s2 + s2) + sigma * sigma * s1
        one = s0 / (s0 - h * s1)
        part = spread / s0
        two = 1.0 / jnp.maximum(1.0 - h * bent / spread - one * (h * h) * part, 1.0)
        slope = (one * h) * (one * h) * part
        c1 = one * two * h
        c0 = one + two * slope - c1 * sigma
        return c0, c1

    def first_fields(r, carry):
        mids, images = zip(*[heat("u%d" % j, r) for j in range(3)])
        begin = plane["s"][at(r), :]
        leads = [begin - mids[0], mids[0] - mids[1], mids[1] - mids[2]]
        rc = None
        for m, name in enumerate(["a", "b", "d"]):
            value = leads[m]
            for j in range(3):
                value = value + WEIGHT[m][j] * images[j]
            pad[name][pl.ds(PAD + r, BLOCK), :] = value
            rc = value if rc is None else rc + value
        plane["rc"][at(r), :] = rc
        return carry

    a_in, b_in, d_in, la_in = [], [], [], []
    for c in range(CHUNKS):
        for j in range(3):
            arrive(u_in[c][j])
        sweep(c * chunk, chunk, first_fields, 0)
        a_in.append(swap("a", c))
    put_rc = put(plane["rc"], plane["xrc"], (next_t, me_y, me_z))
    for c in range(CHUNKS):
        b_in.append(swap("b", c))

    def first_heat(r, carry):
        s0, s1, s2 = carry
        mid, out = heat("a", r)
        pad["la"][pl.ds(PAD + r, BLOCK), :] = out
        return s0 + fold(mid * mid), s1 + fold(mid * out), s2 + fold(out * out)

    sums = (nothing,) * 3
    for c in range(CHUNKS):
        arrive(a_in[c])
        sums = sweep(c * chunk, chunk, first_heat, sums)
        la_in.append(swap("la", c))
    d_in.append(swap("d", 0))

    def second_field(r, carry):
        plane["lb"][at(r), :] = heat("b", r)[1]
        return carry

    for c in range(CHUNKS):
        arrive(b_in[c])
        sweep(c * chunk, chunk, second_field, 0)

    def second_heat(r, carry):
        mid, out = heat("la", r)
        plane["lla"][at(r), :] = out
        return carry + fold(mid * out)

    s3 = nothing
    for c in range(CHUNKS):
        arrive(la_in[c])
        s3 = sweep(c * chunk, chunk, second_heat, s3)
    z_wait = reduce_z(0, list(sums) + [s3])
    for c in range(1, CHUNKS):
        d_in.append(swap("d", c))

    def third_field(r, carry):
        s0, s1, s2 = carry
        ld = heat("d", r)[1]
        rc = plane["rc"][at(r), :]
        vc = pad["la"][pl.ds(PAD + r, BLOCK), :] + plane["lb"][at(r), :] + ld
        plane["ld"][at(r), :] = ld
        pad["vc"][pl.ds(PAD + r, BLOCK), :] = vc
        return s0 + fold(rc * rc), s1 + fold(rc * vc), s2 + fold(vc * vc)

    coarse = (nothing,) * 3
    arrive(d_in[0])
    coarse = sweep(0, chunk, third_field, coarse)
    (y_wait,) = reduce_y(0, z_wait)
    if CHUNKS > 2:
        arrive(d_in[1])
        coarse = sweep(chunk, chunk, third_field, coarse)
    c0, c1 = factors(total_own(0, y_wait), 0, WIDTH[0])

    def second_node(r, carry):
        s0, s1, s2 = carry
        at_pad = pl.ds(PAD + r, BLOCK)
        a, la, lla = pad["a"][at_pad, :], pad["la"][at_pad, :], plane["lla"][at(r), :]
        move = c0 * a + c1 * la
        plane["o0"][at(r), :] = pad["u0"][at_pad, :] + move
        r2 = pad["b"][at_pad, :] + move
        v2 = plane["lb"][at(r), :] + c0 * la + c1 * lla
        plane["r2"][at(r), :] = r2
        pad["v2"][at_pad, :] = v2
        return s0 + fold(r2 * r2), s1 + fold(r2 * v2), s2 + fold(v2 * v2)

    sums = (nothing,) * 3
    v_in = {}
    order = [i // 2 + (i % 2) * (CHUNKS // 2) for i in range(CHUNKS)]
    for c in order:
        sums = sweep(c * chunk, chunk, second_node, sums)
        v_in[c] = swap_half("v2", c, False)
    w_in = {}
    for c in order[:2]:
        w_in[c] = swap_half("v2", c, True)
    outs = [pltpu.make_async_copy(plane["o0"], fine_hbm.at[0], local.at[5])]
    outs[0].start()
    for c in range(2 if CHUNKS > 2 else 1, CHUNKS):
        arrive(d_in[c])
        coarse = sweep(c * chunk, chunk, third_field, coarse)
    put_vc = put(inner("vc"), plane["xvc"], (next_t, me_y, me_z))
    s3 = nothing
    for c in order:
        arrive(v_in[c])
        s3 = s3 + moments("v2", lambda s: side["v2"].at[s], c)
    z_wait = reduce_z(1, list(sums) + [s3])
    for c in order[2:]:
        w_in[c] = swap_half("v2", c, True)
    vc_in = {c: give_half("vc", c) for c in order}

    def third_heat(r, carry):
        plane["lv2"][at(r), :] = heat("v2", r)[1]
        return carry

    for c in order[:2]:
        arrive(w_in[c])
        sweep(c * chunk, chunk, third_heat, 0)
    (y_wait,) = reduce_y(1, z_wait)
    for c in order[2:]:
        arrive(w_in[c])
        sweep(c * chunk, chunk, third_heat, 0)
    e0, e1 = factors(total_own(1, y_wait), 0, WIDTH[1])

    def third_node(r, carry):
        s0, s1, s2 = carry
        at_pad = pl.ds(PAD + r, BLOCK)
        r2, v2, lv2 = plane["r2"][at(r), :], pad["v2"][at_pad, :], plane["lv2"][at(r), :]
        move = e0 * r2 + e1 * v2
        plane["o1"][at(r), :] = pad["u1"][at_pad, :] + move
        r3 = pad["d"][at_pad, :] + move
        v3 = plane["ld"][at(r), :] + e0 * v2 + e1 * lv2
        plane["r3"][at(r), :] = r3
        pad["v3"][at_pad, :] = v3
        return s0 + fold(r3 * r3), s1 + fold(r3 * v3), s2 + fold(v3 * v3)

    sums = (nothing,) * 3
    v3_in = {}
    for c in order:
        sums = sweep(c * chunk, chunk, third_node, sums)
        v3_in[c] = give_half("v3", c)
    put_r3 = put(plane["r3"], plane["xr3"], (next_t, me_y, me_z))
    put_v3 = put(inner("v3"), plane["xv3"], (next_t, me_y, me_z))
    outs.append(pltpu.make_async_copy(plane["o1"], fine_hbm.at[1], local.at[6]))
    outs[1].start()
    coarse3 = nothing
    for c in order:
        arrive(vc_in[c])
        coarse3 = coarse3 + moments("vc", lambda s: plane["hvc"], c)
    s3 = nothing
    for c in order:
        arrive(v3_in[c])
        s3 = s3 + moments("v3", lambda s: plane["hv3"], c)
    z_wait = reduce_z(2, list(sums) + [s3] + list(coarse) + [coarse3])
    y_wait, x_wait = reduce_y(2, z_wait, onward=True)
    for copy in (put_u, put_rc, put_vc, put_r3, put_v3):
        copy.wait_recv()
    g0, g1 = factors(total_own(2, y_wait), 0, WIDTH[2])

    def last_node(r, carry):
        at_pad = pl.ds(PAD + r, BLOCK)
        move = g0 * plane["r3"][at(r), :] + g1 * pad["v3"][at_pad, :]
        plane["o2"][at(r), :] = pad["u2"][at_pad, :] + move
        return carry

    sweep(0, rows, last_node, 0)
    outs.append(pltpu.make_async_copy(plane["o2"], fine_hbm.at[2], local.at[7]))
    outs[2].start()
    sums = total_last(x_wait)
    p0, p1 = factors(sums, 0, WIDTH[2])
    q0, q1 = factors(sums, 4, STEP)

    def next_slice(r, carry):
        begin, guess = plane["s"][at(r), :], plane["xu"][at(r), :]
        fine = guess + (p0 * plane["xr3"][at(r), :] + p1 * plane["xv3"][at(r), :])
        coarse = guess + (q0 * plane["xrc"][at(r), :] + q1 * plane["xvc"][at(r), :])
        plane["ons"][at(r), :] = jnp.where(me_t == 0, begin, fine)
        plane["onc"][at(r), :] = jnp.where(me_t == 0, begin, coarse)
        return carry

    sweep(0, rows, next_slice, 0)
    outs.append(pltpu.make_async_copy(plane["ons"], ns_hbm, local.at[8]))
    outs.append(pltpu.make_async_copy(plane["onc"], nc_hbm, local.at[9]))
    for copy in outs[3:]:
        copy.start()
    for copy in started:
        copy.wait_send()
    for waits in bursts:
        waits.wait_send()
    for copy in outs:
        copy.wait()


def copies_needed():
    return 2 + 6 * CHUNKS + 5 * 2 * CHUNKS + 2 * CHUNKS + 5


def on_device(dims, start_value, old_nodes, diffusivity):
    nt, ny, nz, rows, cols = dims
    anywhere = pl.BlockSpec(memory_space=pl.ANY)
    plane = jax.ShapeDtypeStruct((rows, cols), jnp.float32)
    fine, following, coarse = pl.pallas_call(
        functools.partial(kernel, dims),
        out_shape=(jax.ShapeDtypeStruct((3, rows, cols), jnp.float32), plane, plane),
        in_specs=[anywhere] * 3,
        out_specs=(anywhere,) * 3,
        scratch_shapes=[
            pltpu.VMEM((len(PADDED), rows + 2 * PAD, cols), jnp.float32),
            pltpu.VMEM((len(PLANES), rows, cols), jnp.float32),
            pltpu.VMEM((len(SIDES), 2, rows, cols), jnp.float32),
            pltpu.VMEM((3, 8, 128), jnp.float32),
            pltpu.VMEM((3, 8, 128), jnp.float32),
            pltpu.VMEM((3, nz - 1, 8, 128), jnp.float32),
            pltpu.VMEM((3, ny - 1, 8, 128), jnp.float32),
            pltpu.VMEM((ny, 8, 128), jnp.float32),
            pltpu.SemaphoreType.DMA((copies_needed(),)),
            pltpu.SemaphoreType.DMA((copies_needed(),)),
            pltpu.SemaphoreType.DMA((10,)),
            pltpu.SemaphoreType.DMA((10,)),
            pltpu.SemaphoreType.DMA((10,)),
        ],
        compiler_params=pltpu.CompilerParams(
            collective_id=0, has_side_effects=True, vmem_limit_bytes=60 * 1024 * 1024
        ),
    )(start_value.reshape(rows, cols), old_nodes.reshape(3, rows, cols), diffusivity.reshape(rows, cols))
    return (
        fine.reshape(1, 3, 1, rows, cols),
        following.reshape(1, 1, rows, cols),
        coarse.reshape(1, 1, rows, cols),
    )


def build(split, rows, cols):
    dims = (split.shape["tm"], split.shape["y"], split.shape["z"], rows, cols)
    in_specs = (P("tm", SPACE, None, None), P("tm", None, SPACE, None, None), P(SPACE, None, None))
    out_specs = (
        P("tm", None, SPACE, None, None),
        P("tm", SPACE, None, None),
        P("tm", SPACE, None, None),
    )
    return jax.shard_map(
        functools.partial(on_device, dims), mesh=split, in_specs=in_specs, out_specs=out_specs,
        check_vma=False,
    )


def solution(mesh):
    split = Mesh(
        mesh.devices.reshape(mesh.shape["tm"], ROWS_Y, mesh.shape["space"] // ROWS_Y), ("tm",) + SPACE
    )
    return build(split, 512, 256)
```

```python
import functools
import math

import jax
import jax.numpy as jnp
from jax import lax
from jax.experimental import pallas as pl
from jax.experimental.pallas import tpu as pltpu
from jax.sharding import Mesh
from jax.sharding import PartitionSpec as P

MESH = pl.DeviceIdType.MESH
SPACE = ("y", "z")
ROWS_Y = 8
STEP = 2.0
ROOT_SIX = math.sqrt(6.0)
NODE_TIMES = [(4.0 - ROOT_SIX) / 10.0, (4.0 + ROOT_SIX) / 10.0, 1.0]
COLLOC = [
    [
        (88.0 - 7.0 * ROOT_SIX) / 360.0,
        (296.0 - 169.0 * ROOT_SIX) / 1800.0,
        (-2.0 + 3.0 * ROOT_SIX) / 225.0,
    ],
    [
        (296.0 + 169.0 * ROOT_SIX) / 1800.0,
        (88.0 + 7.0 * ROOT_SIX) / 360.0,
        (-2.0 - 3.0 * ROOT_SIX) / 225.0,
    ],
    [(16.0 - ROOT_SIX) / 36.0, (16.0 + ROOT_SIX) / 36.0, 1.0 / 9.0],
]
WEIGHT = [
    [STEP * (COLLOC[m][j] - (COLLOC[m - 1][j] if m else 0.0)) for j in range(3)] for m in range(3)
]
WIDTH = [STEP * (NODE_TIMES[m] - (NODE_TIMES[m - 1] if m else 0.0)) for m in range(3)]
PAD = 8
BLOCK = 32
CHUNKS = 8

PADDED = ["k", "u0", "u1", "u2", "a", "b", "d", "la", "v2", "v3", "vc"]
PLANES = ["s", "wxm", "wxp", "wym", "wyp", "wzm", "wzp", "dg", "lb", "ld", "lla", "lv2"]
PLANES += ["r2", "r3", "rc", "hv3", "hvc", "xu", "xrc", "xvc", "xr3", "xv3"]
SIDES = ["k", "u0", "u1", "u2", "a", "b", "d", "la", "v2"]


def kernel(dims, start_hbm, old_hbm, kappa_hbm, fine, following, coarse_next, padded, planes, sides,
           tiles, ztiles, zslots, yslots, xslots, send, recv, gsend, grecv, local):
    nt, ny, nz, rows, cols = dims
    chunk = rows // CHUNKS
    me_t, me_y, me_z = lax.axis_index("tm"), lax.axis_index("y"), lax.axis_index("z")
    place = me_y * nz + me_z
    slabs = ny * nz

    def chain(shift):
        other = lax.rem(place + (slabs + shift), slabs)
        return (me_t, lax.div(other, nz), lax.rem(other, nz))

    after, before = chain(1), chain(-1)
    next_t = lax.rem(me_t + 1, nt)
    last_t = lax.rem(me_t + (nt - 1), nt)

    def z_peer(k):
        return (me_t, me_y, lax.rem(me_z + k, nz))

    def y_peer(k, t=me_t):
        return (t, lax.rem(me_y + k, ny), me_z)

    def t_peer(k):
        return (lax.rem(me_t + k, nt), me_y, me_z)

    pad = {name: padded.at[i] for i, name in enumerate(PADDED)}
    plane = {name: planes.at[i] for i, name in enumerate(PLANES)}
    side = {name: sides.at[i] for i, name in enumerate(SIDES)}

    def inner(name, first=0, count=rows):
        return pad[name].at[pl.ds(PAD + first, count), :]

    loads = [(kappa_hbm, "k"), (old_hbm.at[0], "u0"), (old_hbm.at[1], "u1"), (old_hbm.at[2], "u2")]
    copies = [pltpu.make_async_copy(src, inner(name), local.at[i]) for i, (src, name) in enumerate(loads)]
    copies.append(pltpu.make_async_copy(start_hbm, plane["s"], local.at[4]))
    for copy in copies:
        copy.start()
    barrier = pltpu.get_barrier_semaphore()
    greeted = [after, before]
    greeted += [z_peer(k) for k in range(1, nz)]
    greeted += [y_peer(k) for k in range(1, ny)]
    greeted += [t_peer(k) for k in range(1, nt)]
    greeted += [y_peer(k, last_t) for k in range(ny)]
    for device in greeted:
        pl.semaphore_signal(barrier, inc=1, device_id=device, device_id_type=MESH)
    edge = jnp.zeros((PAD, cols), jnp.float32)
    for name in PADDED:
        pad[name][pl.ds(0, PAD), :] = edge
        pad[name][pl.ds(PAD + rows, PAD), :] = edge
    for copy in copies:
        copy.wait()
    pl.semaphore_wait(barrier, len(greeted))

    started = []

    def put(src, dst, device):
        i = len(started)
        copy = pltpu.make_async_remote_copy(
            src_ref=src, dst_ref=dst, send_sem=send.at[i], recv_sem=recv.at[i],
            device_id=device, device_id_type=MESH,
        )
        copy.start()
        started.append(copy)
        return copy

    def swap(name, c):
        here = inner(name, c * chunk, chunk)
        there = pl.ds(c * chunk, chunk)
        return [
            put(here, side[name].at[0, there, :], after),
            put(here, side[name].at[1, there, :], before),
        ]

    def swap_half(name, c, second):
        here = inner(name, c * chunk, chunk)
        there = pl.ds(c * chunk, chunk)
        up = (c < CHUNKS // 2) != second
        return [put(here, side[name].at[0 if up else 1, there, :], after if up else before)]

    def give_half(name, c):
        up = c < CHUNKS // 2
        here = inner(name, c * chunk, chunk)
        there = plane["h" + name].at[pl.ds(c * chunk, chunk), :]
        return [put(here, there, after if up else before)]

    def arrive(batch):
        for copy in batch:
            copy.wait_recv()

    share = rows // nt
    own = pl.multiple_of(me_t * share, share)
    mine = pl.ds(own, share)
    k_src = pad["k"].at[pl.ds(pl.multiple_of(PAD + own, PAD), share), :]
    k_in = [put(k_src, side["k"].at[0, mine, :], after), put(k_src, side["k"].at[1, mine, :], before)]
    u_in = []
    for c in range(CHUNKS):
        u_in.append([swap("u%d" % j, c) for j in range(3)])
    put_u = put(inner("u2"), plane["xu"], (next_t, me_y, me_z))
    arrive(k_in)
    for s in range(2):
        block = side["k"].at[s, mine, :]
        for k in range(1, nt):
            pltpu.make_async_remote_copy(
                src_ref=block, dst_ref=block, send_sem=gsend.at[0], recv_sem=grecv.at[0],
                device_id=t_peer(k), device_id_type=MESH,
            ).start()
    spread = side["k"].at[:, pl.ds(0, share * (nt - 1)), :]
    shared = pltpu.make_async_remote_copy(
        src_ref=spread, dst_ref=spread, send_sem=gsend.at[0], recv_sem=grecv.at[0],
        device_id=after, device_id_type=MESH,
    )
    shared.wait_recv()

    lane = lax.broadcasted_iota(jnp.int32, (BLOCK, cols), 1)
    first_lane, last_lane = lane == 0, lane == cols - 1
    zero = jnp.zeros((BLOCK, cols), jnp.float32)

    def to_right(x):
        return pltpu.roll(x, cols - 1, 1)

    def to_left(x):
        return pltpu.roll(x, 1, 1)

    def at(r):
        return pl.ds(r, BLOCK)

    def column(name, r):
        x = pad[name][pl.ds(r, BLOCK + 2 * PAD), :]
        return x[PAD:PAD + BLOCK], x[PAD - 1:PAD + BLOCK - 1], x[PAD + 1:PAD + BLOCK + 1]

    def sweep(first, count, body, carry):
        def step(i, carry):
            return body(pl.multiple_of(first + i * BLOCK, BLOCK), carry)

        return lax.fori_loop(0, count // BLOCK, step, carry)

    def weights(r, carry):
        k, k_down, k_up = column("k", r)
        row = lax.broadcasted_iota(jnp.int32, (BLOCK, cols), 0) + r
        k_before = jnp.where(place == 0, zero, side["k"][0, at(r), :])
        k_after = jnp.where(place == slabs - 1, zero, side["k"][1, at(r), :])
        faces = [
            0.5 * (k + k_before),
            0.5 * (k + k_after),
            0.5 * (k + k_down),
            0.5 * (k + k_up),
            0.5 * (k + jnp.where(first_lane, zero, to_left(k))),
            0.5 * (k + jnp.where(last_lane, zero, to_right(k))),
        ]
        total = faces[1] + faces[0] + faces[3] + faces[2] + faces[5] + faces[4]
        plane["dg"][at(r), :] = -total
        plane["wxm"][at(r), :] = jnp.where(place == 0, zero, faces[0])
        plane["wxp"][at(r), :] = jnp.where(place == slabs - 1, zero, faces[1])
        plane["wym"][at(r), :] = jnp.where(row == 0, zero, faces[2])
        plane["wyp"][at(r), :] = jnp.where(row == rows - 1, zero, faces[3])
        plane["wzm"][at(r), :] = jnp.where(first_lane, zero, faces[4])
        plane["wzp"][at(r), :] = jnp.where(last_lane, zero, faces[5])
        return carry

    sweep(0, rows, weights, 0)

    def heat(name, r):
        mid, down, up = column(name, r)
        out = plane["wxp"][at(r), :] * side[name][1, at(r), :]
        out = out + plane["wxm"][at(r), :] * side[name][0, at(r), :]
        out = out + plane["wyp"][at(r), :] * up + plane["wym"][at(r), :] * down
        out = out + plane["wzp"][at(r), :] * to_right(mid) + plane["wzm"][at(r), :] * to_left(mid)
        return mid, out + plane["dg"][at(r), :] * mid

    def fold(x):
        return jnp.sum(x.reshape(BLOCK // 8, 8, cols), axis=0)

    nothing = jnp.zeros((8, cols), jnp.float32)

    def quadratic(name, beside, weight, r):
        mid, _, up = column(name, r)
        twice = plane[weight][at(r), :] * beside[at(r), :]
        twice = twice + plane["wyp"][at(r), :] * up + plane["wzp"][at(r), :] * to_right(mid)
        return fold(mid * (twice + twice + plane["dg"][at(r), :] * mid))

    def moments(name, beside, c):
        weight = "wxm" if c < CHUNKS // 2 else "wxp"
        beside = beside(0 if c < CHUNKS // 2 else 1)
        return sweep(c * chunk, chunk, lambda r, acc: acc + quadratic(name, beside, weight, r), nothing)

    spot = lax.broadcasted_iota(jnp.int32, (1, 128), 1)

    def lanes(acc):
        both = acc[:, 0:128]
        for i in range(1, cols // 128):
            both = both + acc[:, i * 128:(i + 1) * 128]
        return jnp.sum(both, axis=0, keepdims=True)

    def burst(src, slots, devices, sem):
        for k, device in enumerate(devices):
            pltpu.make_async_remote_copy(
                src_ref=src, dst_ref=slots.at[pl.ds(k, 1), :],
                send_sem=gsend.at[sem], recv_sem=grecv.at[sem],
                device_id=device, device_id_type=MESH,
            ).start()
        whole = slots.at[pl.ds(0, len(devices)), :]
        return pltpu.make_async_remote_copy(
            src_ref=whole, dst_ref=whole, send_sem=gsend.at[sem], recv_sem=grecv.at[sem],
            device_id=after, device_id_type=MESH,
        )

    bursts = [shared]

    def reduce_z(n, accs):
        rows_of = jnp.concatenate([lanes(acc) for acc in accs + [nothing] * (8 - len(accs))], axis=0)
        sums = jnp.sum(rows_of, axis=1, keepdims=True)
        row = jnp.zeros((1, 128), jnp.float32)
        for q in range(len(accs)):
            row = jnp.where(spot == q, sums[q:q + 1, :], row)
        tiles[n, 0:1, :] = row
        devices = [z_peer(k) for k in range(1, nz)]
        waits = burst(tiles.at[n, pl.ds(0, 1), :], zslots.at[n], devices, 1 + 3 * n)
        bursts.append(waits)
        return waits

    def reduce_y(n, waits, onward=False):
        waits.wait_recv()
        ztiles[n, 0:1, :] = tiles[n, 0:1, :] + jnp.sum(zslots[n, 0:nz - 1, :], axis=0, keepdims=True)
        src = ztiles.at[n, pl.ds(0, 1), :]
        out = [burst(src, yslots.at[n], [y_peer(k) for k in range(1, ny)], 2 + 3 * n)]
        if onward:
            out.append(burst(src, xslots, [y_peer(k, next_t) for k in range(ny)], 3 + 3 * n))
        bursts.extend(out)
        return out

    def total_own(n, waits):
        waits.wait_recv()
        return ztiles[n, 0:1, :] + jnp.sum(yslots[n, 0:ny - 1, :], axis=0, keepdims=True)

    def total_last(waits):
        waits.wait_recv()
        return jnp.sum(xslots[0:ny, :], axis=0, keepdims=True)

    def factors(sums, first, h):
        s0, s1, s2, s3 = [sums[:, first + i:first + i + 1] for i in range(4)]
        sigma = s1 / s0
        spread = jnp.maximum(s2 - s1 * sigma, 1e-30)
        bent = s3 - sigma * (s2 + s2) + sigma * sigma * s1
        one = s0 / (s0 - h * s1)
        part = spread / s0
        two = 1.0 / jnp.maximum(1.0 - h * bent / spread - one * (h * h) * part, 1.0)
        slope = (one * h) * (one * h) * part
        c1 = one * two * h
        c0 = one + two * slope - c1 * sigma
        return c0, c1

    def first_fields(r, carry):
        mids, images = zip(*[heat("u%d" % j, r) for j in range(3)])
        begin = plane["s"][at(r), :]
        leads = [begin - mids[0], mids[0] - mids[1], mids[1] - mids[2]]
        rc = None
        for m, name in enumerate(["a", "b", "d"]):
            value = leads[m]
            for j in range(3):
                value = value + WEIGHT[m][j] * images[j]
            pad[name][pl.ds(PAD + r, BLOCK), :] = value
            rc = value if rc is None else rc + value
        plane["rc"][at(r), :] = rc
        return carry

    half = CHUNKS // 2
    each = range(CHUNKS)
    order = [i // 2 + (i % 2) * half for i in each]
    a_in, b_in, d_in, la_in = {}, {}, {}, {}
    for c in each:
        for j in range(3):
            arrive(u_in[c][j])
        sweep(c * chunk, chunk, first_fields, 0)
        a_in[c] = swap("a", c)
    put_rc = put(plane["rc"], plane["xrc"], (next_t, me_y, me_z))

    def first_heat(r, carry):
        s0, s1, s2 = carry
        mid, out = heat("a", r)
        pad["la"][pl.ds(PAD + r, BLOCK), :] = out
        return s0 + fold(mid * mid), s1 + fold(mid * out), s2 + fold(out * out)

    sums = (nothing,) * 3
    for c in each:
        arrive(a_in[c])
        sums = sweep(c * chunk, chunk, first_heat, sums)
        la_in[c] = swap("la", c)
    b_in[0] = swap("b", 0)

    def second_field(r, carry):
        plane["lb"][at(r), :] = heat("b", r)[1]
        return carry

    def take_b(chunks):
        for c in chunks:
            arrive(b_in[c])
            sweep(c * chunk, chunk, second_field, 0)

    def second_heat(r, carry):
        mid, out = heat("la", r)
        plane["lla"][at(r), :] = out
        return carry + fold(mid * out)

    s3 = nothing
    for c in each:
        arrive(la_in[c])
        s3 = sweep(c * chunk, chunk, second_heat, s3)
    z_wait = reduce_z(0, list(sums) + [s3])
    for c in each[1:]:
        b_in[c] = swap("b", c)
    for c in each[:2]:
        d_in[c] = swap("d", c)

    def third_field(r, carry):
        s0, s1, s2 = carry
        ld = heat("d", r)[1]
        rc = plane["rc"][at(r), :]
        vc = pad["la"][pl.ds(PAD + r, BLOCK), :] + plane["lb"][at(r), :] + ld
        plane["ld"][at(r), :] = ld
        pad["vc"][pl.ds(PAD + r, BLOCK), :] = vc
        return s0 + fold(rc * rc), s1 + fold(rc * vc), s2 + fold(vc * vc)

    coarse = (nothing,) * 3

    def take_d(chunks, coarse):
        for c in chunks:
            arrive(d_in[c])
            coarse = sweep(c * chunk, chunk, third_field, coarse)
        return coarse

    take_b(each[:4])
    (y_wait,) = reduce_y(0, z_wait)
    take_b(each[4:])
    c0, c1 = factors(total_own(0, y_wait), 0, WIDTH[0])

    def second_node(r, carry):
        s0, s1, s2 = carry
        at_pad = pl.ds(PAD + r, BLOCK)
        a, la, lla = pad["a"][at_pad, :], pad["la"][at_pad, :], plane["lla"][at(r), :]
        move = c0 * a + c1 * la
        fine[0, at(r), :] = pad["u0"][at_pad, :] + move
        r2 = pad["b"][at_pad, :] + move
        v2 = plane["lb"][at(r), :] + c0 * la + c1 * lla
        plane["r2"][at(r), :] = r2
        pad["v2"][at_pad, :] = v2
        return s0 + fold(r2 * r2), s1 + fold(r2 * v2), s2 + fold(v2 * v2)

    sums = (nothing,) * 3
    v_in, w_in = {}, {}
    for c in order:
        sums = sweep(c * chunk, chunk, second_node, sums)
        v_in[c] = swap_half("v2", c, False)
    for c in order[:2]:
        w_in[c] = swap_half("v2", c, True)
    coarse = take_d(each[:2], coarse)
    s3 = nothing
    for c in order:
        arrive(v_in[c])
        s3 = s3 + moments("v2", lambda s: side["v2"].at[s], c)
    z_wait = reduce_z(1, list(sums) + [s3])
    for c in order[2:]:
        w_in[c] = swap_half("v2", c, True)
    for c in each[2:]:
        d_in[c] = swap("d", c)

    def third_heat(r, carry):
        plane["lv2"][at(r), :] = heat("v2", r)[1]
        return carry

    def take_w(chunks):
        for c in chunks:
            arrive(w_in[c])
            sweep(c * chunk, chunk, third_heat, 0)

    take_w(order)
    (y_wait,) = reduce_y(1, z_wait)
    coarse = take_d(each[2:5], coarse)
    e0, e1 = factors(total_own(1, y_wait), 0, WIDTH[1])
    coarse = take_d(each[5:], coarse)

    def third_node(r, carry):
        s0, s1, s2 = carry
        at_pad = pl.ds(PAD + r, BLOCK)
        r2, v2, lv2 = plane["r2"][at(r), :], pad["v2"][at_pad, :], plane["lv2"][at(r), :]
        move = e0 * r2 + e1 * v2
        fine[1, at(r), :] = pad["u1"][at_pad, :] + move
        r3 = pad["d"][at_pad, :] + move
        v3 = plane["ld"][at(r), :] + e0 * v2 + e1 * lv2
        plane["r3"][at(r), :] = r3
        pad["v3"][at_pad, :] = v3
        return s0 + fold(r3 * r3), s1 + fold(r3 * v3), s2 + fold(v3 * v3)

    sums = (nothing,) * 3
    vc_in = {c: give_half("vc", c) for c in order}
    put_vc = put(inner("vc"), plane["xvc"], (next_t, me_y, me_z))
    v3_in = {}
    for c in order:
        sums = sweep(c * chunk, chunk, third_node, sums)
        v3_in[c] = give_half("v3", c)
    put_r3 = put(plane["r3"], plane["xr3"], (next_t, me_y, me_z))
    put_v3 = put(inner("v3"), plane["xv3"], (next_t, me_y, me_z))
    coarse3 = nothing
    for c in order:
        arrive(vc_in[c])
        coarse3 = coarse3 + moments("vc", lambda s: plane["hvc"], c)
    s3 = nothing
    for c in order:
        arrive(v3_in[c])
        s3 = s3 + moments("v3", lambda s: plane["hv3"], c)
    z_wait = reduce_z(2, list(sums) + [s3] + list(coarse) + [coarse3])
    y_wait, x_wait = reduce_y(2, z_wait, onward=True)
    for copy in (put_u, put_rc, put_vc, put_r3, put_v3):
        copy.wait_recv()
    for copy in started:
        copy.wait_send()
    for waits in bursts[:-2]:
        waits.wait_send()
    g0, g1 = factors(total_own(2, y_wait), 0, WIDTH[2])

    def last_node(r, carry):
        at_pad = pl.ds(PAD + r, BLOCK)
        move = g0 * plane["r3"][at(r), :] + g1 * pad["v3"][at_pad, :]
        fine[2, at(r), :] = pad["u2"][at_pad, :] + move
        return carry

    sweep(0, rows, last_node, 0)
    sums = total_last(x_wait)
    p0, p1 = factors(sums, 0, WIDTH[2])
    q0, q1 = factors(sums, 4, STEP)

    def next_slice(r, carry):
        begin, guess = plane["s"][at(r), :], plane["xu"][at(r), :]
        fine_end = guess + (p0 * plane["xr3"][at(r), :] + p1 * plane["xv3"][at(r), :])
        coarse_end = guess + (q0 * plane["xrc"][at(r), :] + q1 * plane["xvc"][at(r), :])
        following[at(r), :] = jnp.where(me_t == 0, begin, fine_end)
        coarse_next[at(r), :] = jnp.where(me_t == 0, begin, coarse_end)
        return carry

    sweep(0, rows, next_slice, 0)
    for waits in bursts[-2:]:
        waits.wait_send()


def copies_needed():
    return 2 + 6 * CHUNKS + 5 * 2 * CHUNKS + 2 * CHUNKS + 5


def on_device(dims, start_value, old_nodes, diffusivity):
    nt, ny, nz, rows, cols = dims
    anywhere = pl.BlockSpec(memory_space=pl.ANY)
    near = pl.BlockSpec(memory_space=pltpu.VMEM)
    plane = jax.ShapeDtypeStruct((rows, cols), jnp.float32)
    inputs = [
        pltpu.with_memory_space_constraint(value, pltpu.MemorySpace.HBM)
        for value in (
            start_value.reshape(rows, cols),
            old_nodes.reshape(3, rows, cols),
            diffusivity.reshape(rows, cols),
        )
    ]
    fine, following, coarse = pl.pallas_call(
        functools.partial(kernel, dims),
        out_shape=(jax.ShapeDtypeStruct((3, rows, cols), jnp.float32), plane, plane),
        in_specs=[anywhere] * 3,
        out_specs=(near,) * 3,
        scratch_shapes=[
            pltpu.VMEM((len(PADDED), rows + 2 * PAD, cols), jnp.float32),
            pltpu.VMEM((len(PLANES), rows, cols), jnp.float32),
            pltpu.VMEM((len(SIDES), 2, rows, cols), jnp.float32),
            pltpu.VMEM((3, 8, 128), jnp.float32),
            pltpu.VMEM((3, 8, 128), jnp.float32),
            pltpu.VMEM((3, 16, 128), jnp.float32),
            pltpu.VMEM((3, 8, 128), jnp.float32),
            pltpu.VMEM((8, 128), jnp.float32),
            pltpu.SemaphoreType.DMA((copies_needed(),)),
            pltpu.SemaphoreType.DMA((copies_needed(),)),
            pltpu.SemaphoreType.DMA((10,)),
            pltpu.SemaphoreType.DMA((10,)),
            pltpu.SemaphoreType.DMA((5,)),
        ],
        compiler_params=pltpu.CompilerParams(
            collective_id=0, has_side_effects=True, vmem_limit_bytes=40 * 1024 * 1024
        ),
    )(*inputs)
    return (
        fine.reshape(1, 3, 1, rows, cols),
        following.reshape(1, 1, rows, cols),
        coarse.reshape(1, 1, rows, cols),
    )


def build(split, rows, cols):
    dims = (split.shape["tm"], split.shape["y"], split.shape["z"], rows, cols)
    in_specs = (P("tm", SPACE, None, None), P("tm", None, SPACE, None, None), P(SPACE, None, None))
    out_specs = (
        P("tm", None, SPACE, None, None),
        P("tm", SPACE, None, None),
        P("tm", SPACE, None, None),
    )
    return jax.shard_map(
        functools.partial(on_device, dims), mesh=split, in_specs=in_specs, out_specs=out_specs,
        check_vma=False,
    )


def solution(mesh):
    split = Mesh(
        mesh.devices.reshape(mesh.shape["tm"], ROWS_Y, mesh.shape["space"] // ROWS_Y), ("tm",) + SPACE
    )
    return build(split, 512, 256)
```

```python
import functools
import math

import jax
import jax.numpy as jnp
from jax import lax
from jax.experimental import pallas as pl
from jax.experimental.pallas import tpu as pltpu
from jax.sharding import Mesh
from jax.sharding import PartitionSpec as P

MESH = pl.DeviceIdType.MESH
SPACE = ("y", "z")
ROWS_Y = 8
STEP = 2.0
ROOT_SIX = math.sqrt(6.0)
NODE_TIMES = [(4.0 - ROOT_SIX) / 10.0, (4.0 + ROOT_SIX) / 10.0, 1.0]
COLLOC = [
    [
        (88.0 - 7.0 * ROOT_SIX) / 360.0,
        (296.0 - 169.0 * ROOT_SIX) / 1800.0,
        (-2.0 + 3.0 * ROOT_SIX) / 225.0,
    ],
    [
        (296.0 + 169.0 * ROOT_SIX) / 1800.0,
        (88.0 + 7.0 * ROOT_SIX) / 360.0,
        (-2.0 - 3.0 * ROOT_SIX) / 225.0,
    ],
    [(16.0 - ROOT_SIX) / 36.0, (16.0 + ROOT_SIX) / 36.0, 1.0 / 9.0],
]
WEIGHT = [
    [STEP * (COLLOC[m][j] - (COLLOC[m - 1][j] if m else 0.0)) for j in range(3)] for m in range(3)
]
WIDTH = [STEP * (NODE_TIMES[m] - (NODE_TIMES[m - 1] if m else 0.0)) for m in range(3)]
PAD = 8
BLOCK = 32
CHUNKS = 8

PADDED = ["k", "u0", "u1", "u2", "a", "b", "d", "la", "v2", "v3", "vc"]
PLANES = ["s", "wxm", "wxp", "wym", "wyp", "wzm", "wzp", "dg", "lb", "ld", "lla", "lv2"]
PLANES += ["r2", "r3", "rc", "hv3", "hvc", "xu", "xrc", "xvc", "xr3", "xv3"]
SIDES = ["k", "u0", "u1", "u2", "a", "b", "d", "la", "v2"]


def kernel(dims, start_hbm, old_hbm, kappa_hbm, fine, following, coarse_next, padded, planes, sides,
           tiles, ztiles, zslots, yslots, xslots, send, recv, gsend, grecv, local):
    nt, ny, nz, rows, cols = dims
    chunk = rows // CHUNKS
    half = CHUNKS // 2
    each = range(CHUNKS)
    order = [i // 2 + (i % 2) * half for i in each]
    me_t, me_y, me_z = lax.axis_index("tm"), lax.axis_index("y"), lax.axis_index("z")
    place = me_y * nz + me_z
    slabs = ny * nz

    def chain(shift):
        other = lax.rem(place + (slabs + shift), slabs)
        return (me_t, lax.div(other, nz), lax.rem(other, nz))

    after, before = chain(1), chain(-1)
    next_t = lax.rem(me_t + 1, nt)
    last_t = lax.rem(me_t + (nt - 1), nt)

    def z_peer(k):
        return (me_t, me_y, lax.rem(me_z + k, nz))

    def y_peer(k, t=me_t):
        return (t, lax.rem(me_y + k, ny), me_z)

    def t_peer(k):
        return (lax.rem(me_t + k, nt), me_y, me_z)

    pad = {name: padded.at[i] for i, name in enumerate(PADDED)}
    plane = {name: planes.at[i] for i, name in enumerate(PLANES)}
    side = {name: sides.at[i] for i, name in enumerate(SIDES)}

    def inner(name, first=0, count=rows):
        return pad[name].at[pl.ds(PAD + first, count), :]

    loads = [(kappa_hbm, "k"), (old_hbm.at[0], "u0"), (old_hbm.at[1], "u1"), (old_hbm.at[2], "u2")]
    copies = [pltpu.make_async_copy(src, inner(name), local.at[i]) for i, (src, name) in enumerate(loads)]
    copies.append(pltpu.make_async_copy(start_hbm, plane["s"], local.at[4]))
    for copy in copies:
        copy.start()
    barrier = pltpu.get_barrier_semaphore()
    greeted = [after, before]
    greeted += [z_peer(k) for k in range(1, nz)]
    greeted += [y_peer(k) for k in range(1, ny)]
    greeted += [t_peer(k) for k in range(1, nt)]
    greeted += [y_peer(k, last_t) for k in range(ny)]
    for device in greeted:
        pl.semaphore_signal(barrier, inc=1, device_id=device, device_id_type=MESH)
    edge = jnp.zeros((PAD, cols), jnp.float32)
    for name in PADDED:
        pad[name][pl.ds(0, PAD), :] = edge
        pad[name][pl.ds(PAD + rows, PAD), :] = edge
    for copy in copies:
        copy.wait()
    pl.semaphore_wait(barrier, len(greeted))

    taken = []

    def put(src, dst, device, group, slot):
        pltpu.make_async_remote_copy(
            src_ref=src, dst_ref=dst, send_sem=send.at[group], recv_sem=recv.at[slot],
            device_id=device, device_id_type=MESH,
        ).start()

    def expect(region, group, slot):
        return pltpu.make_async_remote_copy(
            src_ref=region, dst_ref=region, send_sem=send.at[group], recv_sem=recv.at[slot],
            device_id=after, device_id_type=MESH,
        )

    def fresh_slot():
        taken.append(0)
        return len(taken) - 1

    def swap_all(names, c):
        slot = fresh_slot()
        there = pl.ds(c * chunk, chunk)
        for name in names:
            here = inner(name, c * chunk, chunk)
            put(here, side[name].at[0, there, :], after, 0, slot)
            put(here, side[name].at[1, there, :], before, 0, slot)
        first = SIDES.index(names[0])
        return expect(sides.at[pl.ds(first, len(names)), :, there, :], 0, slot)

    def swap(name, c):
        return swap_all([name], c)

    def swap_half(name, i, second):
        slot = fresh_slot()
        for c, up in ((i, not second), (i + half, second)):
            there = pl.ds(c * chunk, chunk)
            dst = side[name].at[0 if up else 1, there, :]
            put(inner(name, c * chunk, chunk), dst, after if up else before, 0, slot)
        return expect(side[name].at[:, pl.ds(0, chunk), :], 0, slot)

    def give_half(name, i):
        slot = fresh_slot()
        for c, up in ((i, True), (i + half, False)):
            dst = plane["h" + name].at[pl.ds(c * chunk, chunk), :]
            put(inner(name, c * chunk, chunk), dst, after if up else before, 1, slot)
        return expect(side["v2"].at[:, pl.ds(0, chunk), :], 1, slot)

    def arrive(waiter):
        waiter.wait_recv()

    share = rows // nt
    own = pl.multiple_of(me_t * share, share)
    mine = pl.ds(own, share)
    k_src = pad["k"].at[pl.ds(pl.multiple_of(PAD + own, PAD), share), :]
    k_slot = fresh_slot()
    put(k_src, side["k"].at[0, mine, :], after, 3, k_slot)
    put(k_src, side["k"].at[1, mine, :], before, 3, k_slot)
    k_in = expect(side["k"].at[:, mine, :], 3, k_slot)
    u_in = [swap_all(["u0", "u1", "u2"], c) for c in range(CHUNKS)]
    next_device = (next_t, me_y, me_z)
    early, late = fresh_slot(), fresh_slot()
    put(inner("u2"), plane["xu"], next_device, 2, early)
    arrive(k_in)
    for s in range(2):
        block = side["k"].at[s, mine, :]
        for k in range(1, nt):
            pltpu.make_async_remote_copy(
                src_ref=block, dst_ref=block, send_sem=gsend.at[0], recv_sem=grecv.at[0],
                device_id=t_peer(k), device_id_type=MESH,
            ).start()
    spread = side["k"].at[:, pl.ds(0, share * (nt - 1)), :]
    shared = pltpu.make_async_remote_copy(
        src_ref=spread, dst_ref=spread, send_sem=gsend.at[0], recv_sem=grecv.at[0],
        device_id=after, device_id_type=MESH,
    )
    shared.wait_recv()

    lane = lax.broadcasted_iota(jnp.int32, (BLOCK, cols), 1)
    first_lane, last_lane = lane == 0, lane == cols - 1
    zero = jnp.zeros((BLOCK, cols), jnp.float32)

    def to_right(x):
        return pltpu.roll(x, cols - 1, 1)

    def to_left(x):
        return pltpu.roll(x, 1, 1)

    def at(r):
        return pl.ds(r, BLOCK)

    def column(name, r):
        x = pad[name][pl.ds(r, BLOCK + 2 * PAD), :]
        return x[PAD:PAD + BLOCK], x[PAD - 1:PAD + BLOCK - 1], x[PAD + 1:PAD + BLOCK + 1]

    def sweep(first, count, body, carry):
        def step(i, carry):
            return body(pl.multiple_of(first + i * BLOCK, BLOCK), carry)

        return lax.fori_loop(0, count // BLOCK, step, carry)

    def weights(r, carry):
        k, k_down, k_up = column("k", r)
        row = lax.broadcasted_iota(jnp.int32, (BLOCK, cols), 0) + r
        k_before = jnp.where(place == 0, zero, side["k"][0, at(r), :])
        k_after = jnp.where(place == slabs - 1, zero, side["k"][1, at(r), :])
        faces = [
            0.5 * (k + k_before),
            0.5 * (k + k_after),
            0.5 * (k + k_down),
            0.5 * (k + k_up),
            0.5 * (k + jnp.where(first_lane, zero, to_left(k))),
            0.5 * (k + jnp.where(last_lane, zero, to_right(k))),
        ]
        total = faces[1] + faces[0] + faces[3] + faces[2] + faces[5] + faces[4]
        plane["dg"][at(r), :] = -total
        plane["wxm"][at(r), :] = jnp.where(place == 0, zero, faces[0])
        plane["wxp"][at(r), :] = jnp.where(place == slabs - 1, zero, faces[1])
        plane["wym"][at(r), :] = jnp.where(row == 0, zero, faces[2])
        plane["wyp"][at(r), :] = jnp.where(row == rows - 1, zero, faces[3])
        plane["wzm"][at(r), :] = jnp.where(first_lane, zero, faces[4])
        plane["wzp"][at(r), :] = jnp.where(last_lane, zero, faces[5])
        return carry

    sweep(0, rows, weights, 0)

    def heat(name, r):
        mid, down, up = column(name, r)
        out = plane["wxp"][at(r), :] * side[name][1, at(r), :]
        out = out + plane["wxm"][at(r), :] * side[name][0, at(r), :]
        out = out + plane["wyp"][at(r), :] * up + plane["wym"][at(r), :] * down
        out = out + plane["wzp"][at(r), :] * to_right(mid) + plane["wzm"][at(r), :] * to_left(mid)
        return mid, out + plane["dg"][at(r), :] * mid

    def fold(x):
        return jnp.sum(x.reshape(BLOCK // 8, 8, cols), axis=0)

    nothing = jnp.zeros((8, cols), jnp.float32)

    def quadratic(name, beside, weight, r):
        mid, _, up = column(name, r)
        twice = plane[weight][at(r), :] * beside[at(r), :]
        twice = twice + plane["wyp"][at(r), :] * up + plane["wzp"][at(r), :] * to_right(mid)
        return fold(mid * (twice + twice + plane["dg"][at(r), :] * mid))

    def moments(name, beside, c):
        weight = "wxm" if c < CHUNKS // 2 else "wxp"
        beside = beside(0 if c < CHUNKS // 2 else 1)
        return sweep(c * chunk, chunk, lambda r, acc: acc + quadratic(name, beside, weight, r), nothing)

    spot = lax.broadcasted_iota(jnp.int32, (1, 128), 1)

    def lanes(acc):
        both = acc[:, 0:128]
        for i in range(1, cols // 128):
            both = both + acc[:, i * 128:(i + 1) * 128]
        return jnp.sum(both, axis=0, keepdims=True)

    def burst(src, slots, devices, sem):
        for k, device in enumerate(devices):
            pltpu.make_async_remote_copy(
                src_ref=src, dst_ref=slots.at[pl.ds(k, 1), :],
                send_sem=gsend.at[sem], recv_sem=grecv.at[sem],
                device_id=device, device_id_type=MESH,
            ).start()
        whole = slots.at[pl.ds(0, len(devices)), :]
        return pltpu.make_async_remote_copy(
            src_ref=whole, dst_ref=whole, send_sem=gsend.at[sem], recv_sem=grecv.at[sem],
            device_id=after, device_id_type=MESH,
        )

    bursts = [shared]

    def reduce_z(n, accs):
        rows_of = jnp.concatenate([lanes(acc) for acc in accs + [nothing] * (8 - len(accs))], axis=0)
        sums = jnp.sum(rows_of, axis=1, keepdims=True)
        row = jnp.zeros((1, 128), jnp.float32)
        for q in range(len(accs)):
            row = jnp.where(spot == q, sums[q:q + 1, :], row)
        tiles[n, 0:1, :] = row
        devices = [z_peer(k) for k in range(1, nz)]
        waits = burst(tiles.at[n, pl.ds(0, 1), :], zslots.at[n], devices, 1 + 3 * n)
        bursts.append(waits)
        return waits

    def reduce_y(n, waits, onward=False):
        waits.wait_recv()
        ztiles[n, 0:1, :] = tiles[n, 0:1, :] + jnp.sum(zslots[n, 0:nz - 1, :], axis=0, keepdims=True)
        src = ztiles.at[n, pl.ds(0, 1), :]
        out = [burst(src, yslots.at[n], [y_peer(k) for k in range(1, ny)], 2 + 3 * n)]
        if onward:
            out.append(burst(src, xslots, [y_peer(k, next_t) for k in range(ny)], 3 + 3 * n))
        bursts.extend(out)
        return out

    def total_own(n, waits):
        waits.wait_recv()
        return ztiles[n, 0:1, :] + jnp.sum(yslots[n, 0:ny - 1, :], axis=0, keepdims=True)

    def total_last(waits):
        waits.wait_recv()
        return jnp.sum(xslots[0:ny, :], axis=0, keepdims=True)

    def factors(sums, first, h):
        s0, s1, s2, s3 = [sums[:, first + i:first + i + 1] for i in range(4)]
        sigma = s1 / s0
        spread = jnp.maximum(s2 - s1 * sigma, 1e-30)
        bent = s3 - sigma * (s2 + s2) + sigma * sigma * s1
        one = s0 / (s0 - h * s1)
        part = spread / s0
        two = 1.0 / jnp.maximum(1.0 - h * bent / spread - one * (h * h) * part, 1.0)
        slope = (one * h) * (one * h) * part
        c1 = one * two * h
        c0 = one + two * slope - c1 * sigma
        return c0, c1

    def whole(x):
        return jnp.concatenate([jnp.broadcast_to(x, (8, cols))] * (BLOCK // 8), axis=0)

    def first_fields(r, carry):
        mids, images = zip(*[heat("u%d" % j, r) for j in range(3)])
        begin = plane["s"][at(r), :]
        leads = [begin - mids[0], mids[0] - mids[1], mids[1] - mids[2]]
        rc = None
        for m, name in enumerate(["a", "b", "d"]):
            value = leads[m]
            for j in range(3):
                value = value + WEIGHT[m][j] * images[j]
            pad[name][pl.ds(PAD + r, BLOCK), :] = value
            rc = value if rc is None else rc + value
        plane["rc"][at(r), :] = rc
        return carry

    a_in, b_in, d_in, la_in = {}, {}, {}, {}
    for c in each:
        arrive(u_in[c])
        sweep(c * chunk, chunk, first_fields, 0)
        a_in[c] = swap("a", c)
    put(plane["rc"], plane["xrc"], next_device, 2, early)

    def first_heat(r, carry):
        s0, s1, s2 = carry
        mid, out = heat("a", r)
        pad["la"][pl.ds(PAD + r, BLOCK), :] = out
        return s0 + fold(mid * mid), s1 + fold(mid * out), s2 + fold(out * out)

    sums = (nothing,) * 3
    for c in each:
        arrive(a_in[c])
        sums = sweep(c * chunk, chunk, first_heat, sums)
        la_in[c] = swap("la", c)
    b_in[0] = swap("b", 0)

    def second_field(r, carry):
        plane["lb"][at(r), :] = heat("b", r)[1]
        return carry

    def take_b(chunks):
        for c in chunks:
            arrive(b_in[c])
            sweep(c * chunk, chunk, second_field, 0)

    def second_heat(r, carry):
        mid, out = heat("la", r)
        plane["lla"][at(r), :] = out
        return carry + fold(mid * out)

    s3 = nothing
    for c in each:
        arrive(la_in[c])
        s3 = sweep(c * chunk, chunk, second_heat, s3)
    z_wait = reduce_z(0, list(sums) + [s3])
    for c in each[1:]:
        b_in[c] = swap("b", c)
    for c in order[:2]:
        d_in[c] = swap("d", c)

    def third_field(r, carry):
        s0, s1, s2 = carry
        ld = heat("d", r)[1]
        rc = plane["rc"][at(r), :]
        vc = pad["la"][pl.ds(PAD + r, BLOCK), :] + plane["lb"][at(r), :] + ld
        plane["ld"][at(r), :] = ld
        pad["vc"][pl.ds(PAD + r, BLOCK), :] = vc
        return s0 + fold(rc * rc), s1 + fold(rc * vc), s2 + fold(vc * vc)

    coarse = (nothing,) * 3
    vc_in = {}

    def take_d(chunks, coarse):
        for c in chunks:
            arrive(d_in[c])
            coarse = sweep(c * chunk, chunk, third_field, coarse)
            if c >= half:
                vc_in[c - half] = give_half("vc", c - half)
        return coarse

    take_b(each[:4])
    (y_wait,) = reduce_y(0, z_wait)
    take_b(each[4:])
    c0, c1 = [whole(x) for x in factors(total_own(0, y_wait), 0, WIDTH[0])]

    def second_node(r, carry):
        s0, s1, s2 = carry
        at_pad = pl.ds(PAD + r, BLOCK)
        a, la, lla = pad["a"][at_pad, :], pad["la"][at_pad, :], plane["lla"][at(r), :]
        move = c0 * a + c1 * la
        fine[0, at(r), :] = pad["u0"][at_pad, :] + move
        r2 = pad["b"][at_pad, :] + move
        v2 = plane["lb"][at(r), :] + c0 * la + c1 * lla
        plane["r2"][at(r), :] = r2
        pad["v2"][at_pad, :] = v2
        return s0 + fold(r2 * r2), s1 + fold(r2 * v2), s2 + fold(v2 * v2)

    sums = (nothing,) * 3
    v_in, w_in = {}, {}
    for c in order:
        sums = sweep(c * chunk, chunk, second_node, sums)
        if c >= half:
            v_in[c - half] = swap_half("v2", c - half, False)
    w_in[0] = swap_half("v2", 0, True)
    s3 = nothing
    for i in range(half):
        arrive(v_in[i])
        for c in (i, i + half):
            s3 = s3 + moments("v2", lambda s: side["v2"].at[s], c)
    z_wait = reduce_z(1, list(sums) + [s3])
    for i in range(1, half):
        w_in[i] = swap_half("v2", i, True)
    for c in order[2:]:
        d_in[c] = swap("d", c)

    def third_heat(r, carry):
        plane["lv2"][at(r), :] = heat("v2", r)[1]
        return carry

    def take_w(pairs):
        for i in pairs:
            arrive(w_in[i])
            for c in (i, i + half):
                sweep(c * chunk, chunk, third_heat, 0)

    take_w(range(2))
    (y_wait,) = reduce_y(1, z_wait)
    take_w(range(2, half))
    coarse = take_d(order[:5], coarse)
    e0, e1 = [whole(x) for x in factors(total_own(1, y_wait), 0, WIDTH[1])]
    coarse = take_d(order[5:], coarse)

    def third_node(r, carry):
        s0, s1, s2 = carry
        at_pad = pl.ds(PAD + r, BLOCK)
        r2, v2, lv2 = plane["r2"][at(r), :], pad["v2"][at_pad, :], plane["lv2"][at(r), :]
        move = e0 * r2 + e1 * v2
        fine[1, at(r), :] = pad["u1"][at_pad, :] + move
        r3 = pad["d"][at_pad, :] + move
        v3 = plane["ld"][at(r), :] + e0 * v2 + e1 * lv2
        plane["r3"][at(r), :] = r3
        pad["v3"][at_pad, :] = v3
        return s0 + fold(r3 * r3), s1 + fold(r3 * v3), s2 + fold(v3 * v3)

    sums = (nothing,) * 3
    put(inner("vc"), plane["xvc"], next_device, 2, early)
    v3_in = {}
    for c in order:
        sums = sweep(c * chunk, chunk, third_node, sums)
        if c >= half:
            v3_in[c - half] = give_half("v3", c - half)
    put(plane["r3"], plane["xr3"], next_device, 2, late)
    put(inner("v3"), plane["xv3"], next_device, 2, late)
    coarse3 = nothing
    for i in range(half):
        arrive(vc_in[i])
        for c in (i, i + half):
            coarse3 = coarse3 + moments("vc", lambda s: plane["hvc"], c)
    s3 = nothing
    for i in range(half):
        arrive(v3_in[i])
        for c in (i, i + half):
            s3 = s3 + moments("v3", lambda s: plane["hv3"], c)
    z_wait = reduce_z(2, list(sums) + [s3] + list(coarse) + [coarse3])
    expect(planes.at[pl.ds(0, 3)], 2, early).wait_recv()

    def first_slice(r, carry):
        plane["xu"][at(r), :] = jnp.where(me_t == 0, plane["s"][at(r), :], plane["xu"][at(r), :])
        return carry

    sweep(0, rows, first_slice, 0)
    y_wait, x_wait = reduce_y(2, z_wait, onward=True)
    expect(planes.at[pl.ds(0, 2)], 2, late).wait_recv()
    expect(sides.at[pl.ds(1, len(SIDES) - 1)], 0, 0).wait_send()
    expect(planes.at[pl.ds(0, 2)], 1, 0).wait_send()
    expect(planes.at[pl.ds(0, 5)], 2, 0).wait_send()
    k_in.wait_send()
    for waits in bursts[:-2]:
        waits.wait_send()
    g0, g1 = [whole(x) for x in factors(total_own(2, y_wait), 0, WIDTH[2])]

    def last_node(r, carry):
        at_pad = pl.ds(PAD + r, BLOCK)
        move = g0 * plane["r3"][at(r), :] + g1 * pad["v3"][at_pad, :]
        fine[2, at(r), :] = pad["u2"][at_pad, :] + move
        return carry

    sweep(0, rows, last_node, 0)
    sums = total_last(x_wait)
    passed = [jnp.where(me_t == 0, 0.0, x) for x in factors(sums, 0, WIDTH[2]) + factors(sums, 4, STEP)]
    p0, p1, q0, q1 = [whole(x) for x in passed]

    def next_slice(r, carry):
        guess = plane["xu"][at(r), :]
        following[at(r), :] = guess + (p0 * plane["xr3"][at(r), :] + p1 * plane["xv3"][at(r), :])
        coarse_next[at(r), :] = guess + (q0 * plane["xrc"][at(r), :] + q1 * plane["xvc"][at(r), :])
        return carry

    sweep(0, rows, next_slice, 0)
    for waits in bursts[-2:]:
        waits.wait_send()


def slots_needed():
    return 1 + 2 + 5 * CHUNKS + 4 * (CHUNKS // 2)


def leave(fine, following, coarse, fine_hbm, following_hbm, coarse_hbm, sem):
    copies = [
        pltpu.make_async_copy(src, dst, sem.at[i])
        for i, (src, dst) in enumerate(
            [(fine, fine_hbm), (following, following_hbm), (coarse, coarse_hbm)]
        )
    ]
    for copy in copies:
        copy.start()
    for copy in copies:
        copy.wait()


def on_device(dims, start_value, old_nodes, diffusivity):
    nt, ny, nz, rows, cols = dims
    anywhere = pl.BlockSpec(memory_space=pl.ANY)
    near = pl.BlockSpec(memory_space=pltpu.VMEM)
    plane = jax.ShapeDtypeStruct((rows, cols), jnp.float32)
    inputs = [
        pltpu.with_memory_space_constraint(value, pltpu.MemorySpace.HBM)
        for value in (
            start_value.reshape(rows, cols),
            old_nodes.reshape(3, rows, cols),
            diffusivity.reshape(rows, cols),
        )
    ]
    fine, following, coarse = pl.pallas_call(
        functools.partial(kernel, dims),
        out_shape=(jax.ShapeDtypeStruct((3, rows, cols), jnp.float32), plane, plane),
        in_specs=[anywhere] * 3,
        out_specs=(near,) * 3,
        scratch_shapes=[
            pltpu.VMEM((len(PADDED), rows + 2 * PAD, cols), jnp.float32),
            pltpu.VMEM((len(PLANES), rows, cols), jnp.float32),
            pltpu.VMEM((len(SIDES), 2, rows, cols), jnp.float32),
            pltpu.VMEM((3, 8, 128), jnp.float32),
            pltpu.VMEM((3, 8, 128), jnp.float32),
            pltpu.VMEM((3, 16, 128), jnp.float32),
            pltpu.VMEM((3, 8, 128), jnp.float32),
            pltpu.VMEM((8, 128), jnp.float32),
            pltpu.SemaphoreType.DMA((4,)),
            pltpu.SemaphoreType.DMA((slots_needed(),)),
            pltpu.SemaphoreType.DMA((10,)),
            pltpu.SemaphoreType.DMA((10,)),
            pltpu.SemaphoreType.DMA((5,)),
        ],
        compiler_params=pltpu.CompilerParams(
            collective_id=0, has_side_effects=True, vmem_limit_bytes=40 * 1024 * 1024
        ),
    )(*inputs)
    fine, following, coarse = pl.pallas_call(
        leave,
        out_shape=(jax.ShapeDtypeStruct((3, rows, cols), jnp.float32), plane, plane),
        in_specs=[anywhere] * 3,
        out_specs=(anywhere,) * 3,
        scratch_shapes=[pltpu.SemaphoreType.DMA((3,))],
        compiler_params=pltpu.CompilerParams(vmem_limit_bytes=40 * 1024 * 1024),
    )(fine, following, coarse)
    return (
        fine.reshape(1, 3, 1, rows, cols),
        following.reshape(1, 1, rows, cols),
        coarse.reshape(1, 1, rows, cols),
    )


def build(split, rows, cols):
    dims = (split.shape["tm"], split.shape["y"], split.shape["z"], rows, cols)
    in_specs = (P("tm", SPACE, None, None), P("tm", None, SPACE, None, None), P(SPACE, None, None))
    out_specs = (
        P("tm", None, SPACE, None, None),
        P("tm", SPACE, None, None),
        P("tm", SPACE, None, None),
    )
    return jax.shard_map(
        functools.partial(on_device, dims), mesh=split, in_specs=in_specs, out_specs=out_specs,
        check_vma=False,
    )


def solution(mesh):
    split = Mesh(
        mesh.devices.reshape(mesh.shape["tm"], ROWS_Y, mesh.shape["space"] // ROWS_Y), ("tm",) + SPACE
    )
    return build(split, 512, 256)
```

```python
import functools
import math

import jax
import jax.numpy as jnp
from jax import lax
from jax.experimental import pallas as pl
from jax.experimental.pallas import tpu as pltpu
from jax.sharding import Mesh
from jax.sharding import PartitionSpec as P

MESH = pl.DeviceIdType.MESH
SPACE = ("y", "z")
ROWS_Y = 8
STEP = 2.0
ROOT_SIX = math.sqrt(6.0)
NODE_TIMES = [(4.0 - ROOT_SIX) / 10.0, (4.0 + ROOT_SIX) / 10.0, 1.0]
COLLOC = [
    [
        (88.0 - 7.0 * ROOT_SIX) / 360.0,
        (296.0 - 169.0 * ROOT_SIX) / 1800.0,
        (-2.0 + 3.0 * ROOT_SIX) / 225.0,
    ],
    [
        (296.0 + 169.0 * ROOT_SIX) / 1800.0,
        (88.0 + 7.0 * ROOT_SIX) / 360.0,
        (-2.0 - 3.0 * ROOT_SIX) / 225.0,
    ],
    [(16.0 - ROOT_SIX) / 36.0, (16.0 + ROOT_SIX) / 36.0, 1.0 / 9.0],
]
WEIGHT = [
    [STEP * (COLLOC[m][j] - (COLLOC[m - 1][j] if m else 0.0)) for j in range(3)] for m in range(3)
]
WIDTH = [STEP * (NODE_TIMES[m] - (NODE_TIMES[m - 1] if m else 0.0)) for m in range(3)]
PAD = 8
BLOCK = 32
CHUNKS = 8

PADDED = ["k", "u0", "u1", "u2", "a", "b", "d", "la", "v2", "v3", "vc"]
PLANES = ["s", "wxm", "wxp", "wym", "wyp", "wzm", "wzp", "dg", "lb", "ld", "lla", "lv2"]
PLANES += ["r2", "r3", "rc", "hv3", "hvc", "xu", "xrc", "xvc", "xr3", "xv3"]
SIDES = ["k", "u0", "u1", "u2", "a", "b", "d", "la", "v2"]


def kernel(dims, start_hbm, old_hbm, kappa_hbm, fine, following, coarse_next, padded, planes, sides,
           tiles, ztiles, zslots, yslots, xslots, send, recv, gsend, grecv, local):
    nt, ny, nz, rows, cols = dims
    chunk = rows // CHUNKS
    half = CHUNKS // 2
    each = range(CHUNKS)
    order = [i // 2 + (i % 2) * half for i in each]
    me_t, me_y, me_z = lax.axis_index("tm"), lax.axis_index("y"), lax.axis_index("z")
    place = me_y * nz + me_z
    slabs = ny * nz

    def chain(shift):
        other = lax.rem(place + (slabs + shift), slabs)
        return (me_t, lax.div(other, nz), lax.rem(other, nz))

    after, before = chain(1), chain(-1)
    next_t = lax.rem(me_t + 1, nt)
    last_t = lax.rem(me_t + (nt - 1), nt)

    def z_peer(k):
        return (me_t, me_y, lax.rem(me_z + k, nz))

    def y_peer(k, t=me_t):
        return (t, lax.rem(me_y + k, ny), me_z)

    def t_peer(k):
        return (lax.rem(me_t + k, nt), me_y, me_z)

    pad = {name: padded.at[i] for i, name in enumerate(PADDED)}
    plane = {name: planes.at[i] for i, name in enumerate(PLANES)}
    side = {name: sides.at[i] for i, name in enumerate(SIDES)}

    def inner(name, first=0, count=rows):
        return pad[name].at[pl.ds(PAD + first, count), :]

    loads = [(kappa_hbm, "k"), (old_hbm.at[0], "u0"), (old_hbm.at[1], "u1"), (old_hbm.at[2], "u2")]
    copies = [pltpu.make_async_copy(src, inner(name), local.at[i]) for i, (src, name) in enumerate(loads)]
    copies.append(pltpu.make_async_copy(start_hbm, plane["s"], local.at[4]))
    for copy in copies:
        copy.start()
    barrier = pltpu.get_barrier_semaphore()
    greeted = [after, before]
    greeted += [z_peer(k) for k in range(1, nz)]
    greeted += [y_peer(k) for k in range(1, ny)]
    greeted += [t_peer(k) for k in range(1, nt)]
    greeted += [y_peer(k, last_t) for k in range(ny)]
    for device in greeted:
        pl.semaphore_signal(barrier, inc=1, device_id=device, device_id_type=MESH)
    edge = jnp.zeros((PAD, cols), jnp.float32)
    for name in PADDED:
        pad[name][pl.ds(0, PAD), :] = edge
        pad[name][pl.ds(PAD + rows, PAD), :] = edge
    for copy in copies:
        copy.wait()
    pl.semaphore_wait(barrier, len(greeted))

    taken = []

    def put(src, dst, device, group, slot):
        pltpu.make_async_remote_copy(
            src_ref=src, dst_ref=dst, send_sem=send.at[group], recv_sem=recv.at[slot],
            device_id=device, device_id_type=MESH,
        ).start()

    def expect(region, group, slot):
        return pltpu.make_async_remote_copy(
            src_ref=region, dst_ref=region, send_sem=send.at[group], recv_sem=recv.at[slot],
            device_id=after, device_id_type=MESH,
        )

    def fresh_slot():
        taken.append(0)
        return len(taken) - 1

    def swap_all(names, c):
        slot = fresh_slot()
        there = pl.ds(c * chunk, chunk)
        for name in names:
            here = inner(name, c * chunk, chunk)
            put(here, side[name].at[0, there, :], after, 0, slot)
            put(here, side[name].at[1, there, :], before, 0, slot)
        first = SIDES.index(names[0])
        return expect(sides.at[pl.ds(first, len(names)), :, there, :], 0, slot)

    def swap(name, c):
        return swap_all([name], c)

    def swap_half(name, i, second):
        slot = fresh_slot()
        for c, up in ((i, not second), (i + half, second)):
            there = pl.ds(c * chunk, chunk)
            dst = side[name].at[0 if up else 1, there, :]
            put(inner(name, c * chunk, chunk), dst, after if up else before, 0, slot)
        return expect(side[name].at[:, pl.ds(0, chunk), :], 0, slot)

    def give_half(name, i):
        slot = fresh_slot()
        for c, up in ((i, True), (i + half, False)):
            dst = plane["h" + name].at[pl.ds(c * chunk, chunk), :]
            put(inner(name, c * chunk, chunk), dst, after if up else before, 1, slot)
        return expect(side["v2"].at[:, pl.ds(0, chunk), :], 1, slot)

    next_device = (next_t, me_y, me_z)
    early, late = fresh_slot(), fresh_slot()

    def onward(src, name, c, slot):
        put(src, plane[name].at[pl.ds(c * chunk, chunk), :], next_device, 2, slot)

    def arrive(waiter):
        waiter.wait_recv()

    share = rows // nt
    own = pl.multiple_of(me_t * share, share)
    mine = pl.ds(own, share)
    k_src = pad["k"].at[pl.ds(pl.multiple_of(PAD + own, PAD), share), :]
    k_slot = fresh_slot()
    put(k_src, side["k"].at[0, mine, :], after, 3, k_slot)
    put(k_src, side["k"].at[1, mine, :], before, 3, k_slot)
    k_in = expect(side["k"].at[:, mine, :], 3, k_slot)
    u_in = [swap_all(["u0", "u1", "u2"], c) for c in range(CHUNKS)]
    put(inner("u2"), plane["xu"], next_device, 2, early)
    arrive(k_in)
    for s in range(2):
        block = side["k"].at[s, mine, :]
        for k in range(1, nt):
            pltpu.make_async_remote_copy(
                src_ref=block, dst_ref=block, send_sem=gsend.at[0], recv_sem=grecv.at[0],
                device_id=t_peer(k), device_id_type=MESH,
            ).start()
    spread = side["k"].at[:, pl.ds(0, share * (nt - 1)), :]
    shared = pltpu.make_async_remote_copy(
        src_ref=spread, dst_ref=spread, send_sem=gsend.at[0], recv_sem=grecv.at[0],
        device_id=after, device_id_type=MESH,
    )
    shared.wait_recv()

    lane = lax.broadcasted_iota(jnp.int32, (BLOCK, cols), 1)
    first_lane, last_lane = lane == 0, lane == cols - 1
    zero = jnp.zeros((BLOCK, cols), jnp.float32)

    def to_right(x):
        return pltpu.roll(x, cols - 1, 1)

    def to_left(x):
        return pltpu.roll(x, 1, 1)

    def at(r):
        return pl.ds(r, BLOCK)

    def column(name, r):
        x = pad[name][pl.ds(r, BLOCK + 2 * PAD), :]
        return x[PAD:PAD + BLOCK], x[PAD - 1:PAD + BLOCK - 1], x[PAD + 1:PAD + BLOCK + 1]

    def sweep(first, count, body, carry):
        def step(i, carry):
            return body(pl.multiple_of(first + i * BLOCK, BLOCK), carry)

        return lax.fori_loop(0, count // BLOCK, step, carry)

    def weights(r, carry):
        k, k_down, k_up = column("k", r)
        row = lax.broadcasted_iota(jnp.int32, (BLOCK, cols), 0) + r
        k_before = jnp.where(place == 0, zero, side["k"][0, at(r), :])
        k_after = jnp.where(place == slabs - 1, zero, side["k"][1, at(r), :])
        faces = [
            0.5 * (k + k_before),
            0.5 * (k + k_after),
            0.5 * (k + k_down),
            0.5 * (k + k_up),
            0.5 * (k + jnp.where(first_lane, zero, to_left(k))),
            0.5 * (k + jnp.where(last_lane, zero, to_right(k))),
        ]
        total = faces[1] + faces[0] + faces[3] + faces[2] + faces[5] + faces[4]
        plane["dg"][at(r), :] = -total
        plane["wxm"][at(r), :] = jnp.where(place == 0, zero, faces[0])
        plane["wxp"][at(r), :] = jnp.where(place == slabs - 1, zero, faces[1])
        plane["wym"][at(r), :] = jnp.where(row == 0, zero, faces[2])
        plane["wyp"][at(r), :] = jnp.where(row == rows - 1, zero, faces[3])
        plane["wzm"][at(r), :] = jnp.where(first_lane, zero, faces[4])
        plane["wzp"][at(r), :] = jnp.where(last_lane, zero, faces[5])
        return carry

    sweep(0, rows, weights, 0)

    def heat(name, r):
        mid, down, up = column(name, r)
        out = plane["wxp"][at(r), :] * side[name][1, at(r), :]
        out = out + plane["wxm"][at(r), :] * side[name][0, at(r), :]
        out = out + plane["wyp"][at(r), :] * up + plane["wym"][at(r), :] * down
        out = out + plane["wzp"][at(r), :] * to_right(mid) + plane["wzm"][at(r), :] * to_left(mid)
        return mid, out + plane["dg"][at(r), :] * mid

    def fold(x):
        return jnp.sum(x.reshape(BLOCK // 8, 8, cols), axis=0)

    nothing = jnp.zeros((8, cols), jnp.float32)

    def quadratic(name, beside, weight, r):
        mid, _, up = column(name, r)
        twice = plane[weight][at(r), :] * beside[at(r), :]
        twice = twice + plane["wyp"][at(r), :] * up + plane["wzp"][at(r), :] * to_right(mid)
        return fold(mid * (twice + twice + plane["dg"][at(r), :] * mid))

    def moments(name, beside, c):
        weight = "wxm" if c < CHUNKS // 2 else "wxp"
        beside = beside(0 if c < CHUNKS // 2 else 1)
        return sweep(c * chunk, chunk, lambda r, acc: acc + quadratic(name, beside, weight, r), nothing)

    spot = lax.broadcasted_iota(jnp.int32, (1, 128), 1)

    def lanes(acc):
        both = acc[:, 0:128]
        for i in range(1, cols // 128):
            both = both + acc[:, i * 128:(i + 1) * 128]
        return jnp.sum(both, axis=0, keepdims=True)

    def burst(src, slots, devices, sem):
        for k, device in enumerate(devices):
            pltpu.make_async_remote_copy(
                src_ref=src, dst_ref=slots.at[pl.ds(k, 1), :],
                send_sem=gsend.at[sem], recv_sem=grecv.at[sem],
                device_id=device, device_id_type=MESH,
            ).start()
        whole = slots.at[pl.ds(0, len(devices)), :]
        return pltpu.make_async_remote_copy(
            src_ref=whole, dst_ref=whole, send_sem=gsend.at[sem], recv_sem=grecv.at[sem],
            device_id=after, device_id_type=MESH,
        )

    bursts = [shared]

    def reduce_z(n, accs):
        rows_of = jnp.concatenate([lanes(acc) for acc in accs + [nothing] * (8 - len(accs))], axis=0)
        sums = jnp.sum(rows_of, axis=1, keepdims=True)
        row = jnp.zeros((1, 128), jnp.float32)
        for q in range(len(accs)):
            row = jnp.where(spot == q, sums[q:q + 1, :], row)
        tiles[n, 0:1, :] = row
        devices = [z_peer(k) for k in range(1, nz)]
        waits = burst(tiles.at[n, pl.ds(0, 1), :], zslots.at[n], devices, 1 + 3 * n)
        bursts.append(waits)
        return waits

    def reduce_y(n, waits, also=False):
        waits.wait_recv()
        ztiles[n, 0:1, :] = tiles[n, 0:1, :] + jnp.sum(zslots[n, 0:nz - 1, :], axis=0, keepdims=True)
        src = ztiles.at[n, pl.ds(0, 1), :]
        out = [burst(src, yslots.at[n], [y_peer(k) for k in range(1, ny)], 2 + 3 * n)]
        if also:
            out.append(burst(src, xslots, [y_peer(k, next_t) for k in range(ny)], 3 + 3 * n))
        bursts.extend(out)
        return out

    def total_own(n, waits):
        waits.wait_recv()
        return ztiles[n, 0:1, :] + jnp.sum(yslots[n, 0:ny - 1, :], axis=0, keepdims=True)

    def total_last(waits):
        waits.wait_recv()
        return jnp.sum(xslots[0:ny, :], axis=0, keepdims=True)

    def factors(sums, first, h):
        s0, s1, s2, s3 = [sums[:, first + i:first + i + 1] for i in range(4)]
        sigma = s1 / s0
        spread = jnp.maximum(s2 - s1 * sigma, 1e-30)
        bent = s3 - sigma * (s2 + s2) + sigma * sigma * s1
        one = s0 / (s0 - h * s1)
        part = spread / s0
        two = 1.0 / jnp.maximum(1.0 - h * bent / spread - one * (h * h) * part, 1.0)
        slope = (one * h) * (one * h) * part
        c1 = one * two * h
        c0 = one + two * slope - c1 * sigma
        return c0, c1

    def whole(x):
        return jnp.concatenate([jnp.broadcast_to(x, (8, cols))] * (BLOCK // 8), axis=0)

    def first_fields(r, carry):
        mids, images = zip(*[heat("u%d" % j, r) for j in range(3)])
        begin = plane["s"][at(r), :]
        leads = [begin - mids[0], mids[0] - mids[1], mids[1] - mids[2]]
        rc = None
        for m, name in enumerate(["a", "b", "d"]):
            value = leads[m]
            for j in range(3):
                value = value + WEIGHT[m][j] * images[j]
            pad[name][pl.ds(PAD + r, BLOCK), :] = value
            rc = value if rc is None else rc + value
        plane["rc"][at(r), :] = rc
        return carry

    a_in, b_in, d_in, la_in = {}, {}, {}, {}
    for c in each:
        arrive(u_in[c])
        sweep(c * chunk, chunk, first_fields, 0)
        a_in[c] = swap("a", c)
    put(plane["rc"], plane["xrc"], next_device, 2, early)

    def first_heat(r, carry):
        s0, s1, s2 = carry
        mid, out = heat("a", r)
        pad["la"][pl.ds(PAD + r, BLOCK), :] = out
        return s0 + fold(mid * mid), s1 + fold(mid * out), s2 + fold(out * out)

    sums = (nothing,) * 3
    for c in each:
        arrive(a_in[c])
        sums = sweep(c * chunk, chunk, first_heat, sums)
        la_in[c] = swap("la", c)
    for c in each[:3]:
        b_in[c] = swap("b", c)

    def second_field(r, carry):
        plane["lb"][at(r), :] = heat("b", r)[1]
        return carry

    def take_b(chunks):
        for c in chunks:
            arrive(b_in[c])
            sweep(c * chunk, chunk, second_field, 0)

    def second_heat(r, carry):
        mid, out = heat("la", r)
        plane["lla"][at(r), :] = out
        return carry + fold(mid * out)

    s3 = nothing
    for c in each:
        arrive(la_in[c])
        s3 = sweep(c * chunk, chunk, second_heat, s3)
    z_wait = reduce_z(0, list(sums) + [s3])
    for c in each[3:]:
        b_in[c] = swap("b", c)
    for c in order[:4]:
        d_in[c] = swap("d", c)

    def third_field(r, carry):
        s0, s1, s2 = carry
        ld = heat("d", r)[1]
        rc = plane["rc"][at(r), :]
        vc = pad["la"][pl.ds(PAD + r, BLOCK), :] + plane["lb"][at(r), :] + ld
        plane["ld"][at(r), :] = ld
        pad["vc"][pl.ds(PAD + r, BLOCK), :] = vc
        return s0 + fold(rc * rc), s1 + fold(rc * vc), s2 + fold(vc * vc)

    coarse = (nothing,) * 3
    vc_in = {}

    def take_d(chunks, coarse):
        for c in chunks:
            arrive(d_in[c])
            coarse = sweep(c * chunk, chunk, third_field, coarse)
            onward(inner("vc", c * chunk, chunk), "xvc", c, early)
            if c >= half:
                vc_in[c - half] = give_half("vc", c - half)
        return coarse

    take_b(each[:4])
    (y_wait,) = reduce_y(0, z_wait)
    take_b(each[4:])
    c0, c1 = [whole(x) for x in factors(total_own(0, y_wait), 0, WIDTH[0])]

    def second_node(r, carry):
        s0, s1, s2 = carry
        at_pad = pl.ds(PAD + r, BLOCK)
        a, la, lla = pad["a"][at_pad, :], pad["la"][at_pad, :], plane["lla"][at(r), :]
        move = c0 * a + c1 * la
        fine[0, at(r), :] = pad["u0"][at_pad, :] + move
        r2 = pad["b"][at_pad, :] + move
        v2 = plane["lb"][at(r), :] + c0 * la + c1 * lla
        plane["r2"][at(r), :] = r2
        pad["v2"][at_pad, :] = v2
        return s0 + fold(r2 * r2), s1 + fold(r2 * v2), s2 + fold(v2 * v2)

    sums = (nothing,) * 3
    v_in, w_in = {}, {}
    for c in order:
        sums = sweep(c * chunk, chunk, second_node, sums)
        if c >= half:
            v_in[c - half] = swap_half("v2", c - half, False)
    coarse = take_d(order[:4], coarse)
    s3 = nothing
    for i in range(half):
        arrive(v_in[i])
        for c in (i, i + half):
            s3 = s3 + moments("v2", lambda s: side["v2"].at[s], c)
    z_wait = reduce_z(1, list(sums) + [s3])
    for i in range(half):
        w_in[i] = swap_half("v2", i, True)
    for c in order[4:]:
        d_in[c] = swap("d", c)

    def third_heat(r, carry):
        plane["lv2"][at(r), :] = heat("v2", r)[1]
        return carry

    def take_w(pairs):
        for i in pairs:
            arrive(w_in[i])
            for c in (i, i + half):
                sweep(c * chunk, chunk, third_heat, 0)

    take_w(range(2))
    (y_wait,) = reduce_y(1, z_wait)
    take_w(range(2, half))
    coarse = take_d(order[4:6], coarse)
    e0, e1 = [whole(x) for x in factors(total_own(1, y_wait), 0, WIDTH[1])]
    coarse = take_d(order[6:], coarse)

    def third_node(r, carry):
        s0, s1, s2 = carry
        at_pad = pl.ds(PAD + r, BLOCK)
        r2, v2, lv2 = plane["r2"][at(r), :], pad["v2"][at_pad, :], plane["lv2"][at(r), :]
        move = e0 * r2 + e1 * v2
        fine[1, at(r), :] = pad["u1"][at_pad, :] + move
        r3 = pad["d"][at_pad, :] + move
        v3 = plane["ld"][at(r), :] + e0 * v2 + e1 * lv2
        plane["r3"][at(r), :] = r3
        pad["v3"][at_pad, :] = v3
        return s0 + fold(r3 * r3), s1 + fold(r3 * v3), s2 + fold(v3 * v3)

    sums = (nothing,) * 3
    v3_in = {}
    for c in order:
        sums = sweep(c * chunk, chunk, third_node, sums)
        if c >= half:
            v3_in[c - half] = give_half("v3", c - half)
        onward(plane["r3"].at[pl.ds(c * chunk, chunk), :], "xr3", c, late)
        onward(inner("v3", c * chunk, chunk), "xv3", c, late)
    coarse3 = nothing
    for i in range(half):
        arrive(vc_in[i])
        for c in (i, i + half):
            coarse3 = coarse3 + moments("vc", lambda s: plane["hvc"], c)
    s3 = nothing
    for i in range(half):
        arrive(v3_in[i])
        for c in (i, i + half):
            s3 = s3 + moments("v3", lambda s: plane["hv3"], c)
    z_wait = reduce_z(2, list(sums) + [s3] + list(coarse) + [coarse3])
    expect(planes.at[pl.ds(0, 3)], 2, early).wait_recv()

    def first_slice(r, carry):
        plane["xu"][at(r), :] = jnp.where(me_t == 0, plane["s"][at(r), :], plane["xu"][at(r), :])
        return carry

    sweep(0, rows, first_slice, 0)
    y_wait, x_wait = reduce_y(2, z_wait, also=True)
    expect(planes.at[pl.ds(0, 2)], 2, late).wait_recv()
    expect(sides.at[pl.ds(1, len(SIDES) - 1)], 0, 0).wait_send()
    expect(planes.at[pl.ds(0, 2)], 1, 0).wait_send()
    expect(planes.at[pl.ds(0, 5)], 2, 0).wait_send()
    k_in.wait_send()
    for waits in bursts[:-2]:
        waits.wait_send()
    g0, g1 = [whole(x) for x in factors(total_own(2, y_wait), 0, WIDTH[2])]

    def last_node(r, carry):
        at_pad = pl.ds(PAD + r, BLOCK)
        move = g0 * plane["r3"][at(r), :] + g1 * pad["v3"][at_pad, :]
        fine[2, at(r), :] = pad["u2"][at_pad, :] + move
        return carry

    sweep(0, rows, last_node, 0)
    sums = total_last(x_wait)
    passed = [jnp.where(me_t == 0, 0.0, x) for x in factors(sums, 0, WIDTH[2]) + factors(sums, 4, STEP)]
    p0, p1, q0, q1 = [whole(x) for x in passed]

    def next_slice(r, carry):
        guess = plane["xu"][at(r), :]
        following[at(r), :] = guess + (p0 * plane["xr3"][at(r), :] + p1 * plane["xv3"][at(r), :])
        coarse_next[at(r), :] = guess + (q0 * plane["xrc"][at(r), :] + q1 * plane["xvc"][at(r), :])
        return carry

    sweep(0, rows, next_slice, 0)
    for waits in bursts[-2:]:
        waits.wait_send()


def slots_needed():
    return 1 + 2 + 5 * CHUNKS + 4 * (CHUNKS // 2)


def leave(fine, following, coarse, fine_hbm, following_hbm, coarse_hbm, sem):
    copies = [
        pltpu.make_async_copy(src, dst, sem.at[i])
        for i, (src, dst) in enumerate(
            [(fine, fine_hbm), (following, following_hbm), (coarse, coarse_hbm)]
        )
    ]
    for copy in copies:
        copy.start()
    for copy in copies:
        copy.wait()


def on_device(dims, start_value, old_nodes, diffusivity):
    nt, ny, nz, rows, cols = dims
    anywhere = pl.BlockSpec(memory_space=pl.ANY)
    near = pl.BlockSpec(memory_space=pltpu.VMEM)
    plane = jax.ShapeDtypeStruct((rows, cols), jnp.float32)
    inputs = [
        pltpu.with_memory_space_constraint(value, pltpu.MemorySpace.HBM)
        for value in (
            start_value.reshape(rows, cols),
            old_nodes.reshape(3, rows, cols),
            diffusivity.reshape(rows, cols),
        )
    ]
    fine, following, coarse = pl.pallas_call(
        functools.partial(kernel, dims),
        out_shape=(jax.ShapeDtypeStruct((3, rows, cols), jnp.float32), plane, plane),
        in_specs=[anywhere] * 3,
        out_specs=(near,) * 3,
        scratch_shapes=[
            pltpu.VMEM((len(PADDED), rows + 2 * PAD, cols), jnp.float32),
            pltpu.VMEM((len(PLANES), rows, cols), jnp.float32),
            pltpu.VMEM((len(SIDES), 2, rows, cols), jnp.float32),
            pltpu.VMEM((3, 8, 128), jnp.float32),
            pltpu.VMEM((3, 8, 128), jnp.float32),
            pltpu.VMEM((3, 16, 128), jnp.float32),
            pltpu.VMEM((3, 8, 128), jnp.float32),
            pltpu.VMEM((8, 128), jnp.float32),
            pltpu.SemaphoreType.DMA((4,)),
            pltpu.SemaphoreType.DMA((slots_needed(),)),
            pltpu.SemaphoreType.DMA((10,)),
            pltpu.SemaphoreType.DMA((10,)),
            pltpu.SemaphoreType.DMA((5,)),
        ],
        compiler_params=pltpu.CompilerParams(
            collective_id=0, has_side_effects=True, vmem_limit_bytes=40 * 1024 * 1024
        ),
    )(*inputs)
    fine, following, coarse = pl.pallas_call(
        leave,
        out_shape=(jax.ShapeDtypeStruct((3, rows, cols), jnp.float32), plane, plane),
        in_specs=[anywhere] * 3,
        out_specs=(anywhere,) * 3,
        scratch_shapes=[pltpu.SemaphoreType.DMA((3,))],
        compiler_params=pltpu.CompilerParams(vmem_limit_bytes=40 * 1024 * 1024),
    )(fine, following, coarse)
    return (
        fine.reshape(1, 3, 1, rows, cols),
        following.reshape(1, 1, rows, cols),
        coarse.reshape(1, 1, rows, cols),
    )


def build(split, rows, cols):
    dims = (split.shape["tm"], split.shape["y"], split.shape["z"], rows, cols)
    in_specs = (P("tm", SPACE, None, None), P("tm", None, SPACE, None, None), P(SPACE, None, None))
    out_specs = (
        P("tm", None, SPACE, None, None),
        P("tm", SPACE, None, None),
        P("tm", SPACE, None, None),
    )
    return jax.shard_map(
        functools.partial(on_device, dims), mesh=split, in_specs=in_specs, out_specs=out_specs,
        check_vma=False,
    )


def solution(mesh):
    split = Mesh(
        mesh.devices.reshape(mesh.shape["tm"], ROWS_Y, mesh.shape["space"] // ROWS_Y), ("tm",) + SPACE
    )
    return build(split, 512, 256)
```

```python
import functools
import math

import jax
import jax.numpy as jnp
from jax import lax
from jax.experimental import pallas as pl
from jax.experimental.pallas import tpu as pltpu
from jax.sharding import Mesh
from jax.sharding import PartitionSpec as P

MESH = pl.DeviceIdType.MESH
SPACE = ("y", "z")
ROWS_Y = 8
STEP = 2.0
ROOT_SIX = math.sqrt(6.0)
NODE_TIMES = [(4.0 - ROOT_SIX) / 10.0, (4.0 + ROOT_SIX) / 10.0, 1.0]
COLLOC = [
    [
        (88.0 - 7.0 * ROOT_SIX) / 360.0,
        (296.0 - 169.0 * ROOT_SIX) / 1800.0,
        (-2.0 + 3.0 * ROOT_SIX) / 225.0,
    ],
    [
        (296.0 + 169.0 * ROOT_SIX) / 1800.0,
        (88.0 + 7.0 * ROOT_SIX) / 360.0,
        (-2.0 - 3.0 * ROOT_SIX) / 225.0,
    ],
    [(16.0 - ROOT_SIX) / 36.0, (16.0 + ROOT_SIX) / 36.0, 1.0 / 9.0],
]
WEIGHT = [
    [STEP * (COLLOC[m][j] - (COLLOC[m - 1][j] if m else 0.0)) for j in range(3)] for m in range(3)
]
WIDTH = [STEP * (NODE_TIMES[m] - (NODE_TIMES[m - 1] if m else 0.0)) for m in range(3)]
PAD = 8
BLOCK = 32
CHUNKS = 8

PADDED = ["k", "u0", "u1", "u2", "a", "b", "d", "la", "v2", "v3", "vc"]
PLANES = ["s", "wxm", "wxp", "wym", "wyp", "wzm", "wzp", "dg", "lb", "ld", "lla", "lv2"]
PLANES += ["r2", "r3", "rc", "hv3", "hvc", "xu", "xrc", "xvc", "xr3", "xv3"]
SIDES = ["k", "u0", "u1", "u2", "a", "b", "d", "la", "v2"]


def kernel(dims, start_hbm, old_hbm, kappa_hbm, fine, following, coarse_next, padded, planes, sides,
           tiles, ztiles, zslots, yslots, xslots, send, recv, gsend, grecv, local):
    nt, ny, nz, rows, cols = dims
    chunk = rows // CHUNKS
    half = CHUNKS // 2
    each = range(CHUNKS)
    order = [i // 2 + (i % 2) * half for i in each]
    me_t, me_y, me_z = lax.axis_index("tm"), lax.axis_index("y"), lax.axis_index("z")
    place = me_y * nz + me_z
    slabs = ny * nz

    def chain(shift):
        other = lax.rem(place + (slabs + shift), slabs)
        return (me_t, lax.div(other, nz), lax.rem(other, nz))

    after, before = chain(1), chain(-1)
    next_t = lax.rem(me_t + 1, nt)
    last_t = lax.rem(me_t + (nt - 1), nt)

    def z_peer(k):
        return (me_t, me_y, lax.rem(me_z + k, nz))

    def y_peer(k, t=me_t):
        return (t, lax.rem(me_y + k, ny), me_z)

    def t_peer(k):
        return (lax.rem(me_t + k, nt), me_y, me_z)

    pad = {name: padded.at[i] for i, name in enumerate(PADDED)}
    plane = {name: planes.at[i] for i, name in enumerate(PLANES)}
    side = {name: sides.at[i] for i, name in enumerate(SIDES)}

    def inner(name, first=0, count=rows):
        return pad[name].at[pl.ds(PAD + first, count), :]

    loads = [(kappa_hbm, "k"), (old_hbm.at[0], "u0"), (old_hbm.at[1], "u1"), (old_hbm.at[2], "u2")]
    copies = [pltpu.make_async_copy(src, inner(name), local.at[i]) for i, (src, name) in enumerate(loads)]
    copies.append(pltpu.make_async_copy(start_hbm, plane["s"], local.at[4]))
    for copy in copies:
        copy.start()
    barrier = pltpu.get_barrier_semaphore()
    greeted = [after, before]
    greeted += [z_peer(k) for k in range(1, nz)]
    greeted += [y_peer(k) for k in range(1, ny)]
    greeted += [t_peer(k) for k in range(1, nt)]
    greeted += [y_peer(k, last_t) for k in range(ny)]
    for device in greeted:
        pl.semaphore_signal(barrier, inc=1, device_id=device, device_id_type=MESH)
    edge = jnp.zeros((PAD, cols), jnp.float32)
    for name in PADDED:
        pad[name][pl.ds(0, PAD), :] = edge
        pad[name][pl.ds(PAD + rows, PAD), :] = edge
    for copy in copies:
        copy.wait()
    pl.semaphore_wait(barrier, len(greeted))

    taken = []

    def put(src, dst, device, group, slot):
        pltpu.make_async_remote_copy(
            src_ref=src, dst_ref=dst, send_sem=send.at[group], recv_sem=recv.at[slot],
            device_id=device, device_id_type=MESH,
        ).start()

    def expect(region, group, slot):
        return pltpu.make_async_remote_copy(
            src_ref=region, dst_ref=region, send_sem=send.at[group], recv_sem=recv.at[slot],
            device_id=after, device_id_type=MESH,
        )

    def fresh_slot():
        taken.append(0)
        return len(taken) - 1

    def swap_all(names, c):
        slot = fresh_slot()
        there = pl.ds(c * chunk, chunk)
        for name in names:
            here = inner(name, c * chunk, chunk)
            put(here, side[name].at[0, there, :], after, 0, slot)
            put(here, side[name].at[1, there, :], before, 0, slot)
        first = SIDES.index(names[0])
        return expect(sides.at[pl.ds(first, len(names)), :, there, :], 0, slot)

    def swap(name, c):
        return swap_all([name], c)

    def swap_half(name, i, second):
        slot = fresh_slot()
        for c, up in ((i, not second), (i + half, second)):
            there = pl.ds(c * chunk, chunk)
            dst = side[name].at[0 if up else 1, there, :]
            put(inner(name, c * chunk, chunk), dst, after if up else before, 0, slot)
        return expect(side[name].at[:, pl.ds(0, chunk), :], 0, slot)

    def give_half(name, i):
        slot = fresh_slot()
        for c, up in ((i, True), (i + half, False)):
            dst = plane["h" + name].at[pl.ds(c * chunk, chunk), :]
            put(inner(name, c * chunk, chunk), dst, after if up else before, 1, slot)
        return expect(side["v2"].at[:, pl.ds(0, chunk), :], 1, slot)

    next_device = (next_t, me_y, me_z)
    early, late = fresh_slot(), fresh_slot()

    def onward(src, name, c, slot):
        put(src, plane[name].at[pl.ds(c * chunk, chunk), :], next_device, 2, slot)

    def arrive(waiter):
        waiter.wait_recv()

    share = rows // nt
    own = pl.multiple_of(me_t * share, share)
    mine = pl.ds(own, share)
    k_src = pad["k"].at[pl.ds(pl.multiple_of(PAD + own, PAD), share), :]
    k_slot = fresh_slot()
    put(k_src, side["k"].at[0, mine, :], after, 3, k_slot)
    put(k_src, side["k"].at[1, mine, :], before, 3, k_slot)
    k_in = expect(side["k"].at[:, mine, :], 3, k_slot)
    u_in = [swap_all(["u0", "u1", "u2"], c) for c in range(CHUNKS)]
    put(inner("u2"), plane["xu"], next_device, 2, early)
    arrive(k_in)
    for s in range(2):
        block = side["k"].at[s, mine, :]
        for k in range(1, nt):
            pltpu.make_async_remote_copy(
                src_ref=block, dst_ref=block, send_sem=gsend.at[0], recv_sem=grecv.at[0],
                device_id=t_peer(k), device_id_type=MESH,
            ).start()
    spread = side["k"].at[:, pl.ds(0, share * (nt - 1)), :]
    shared = pltpu.make_async_remote_copy(
        src_ref=spread, dst_ref=spread, send_sem=gsend.at[0], recv_sem=grecv.at[0],
        device_id=after, device_id_type=MESH,
    )
    shared.wait_recv()

    lane = lax.broadcasted_iota(jnp.int32, (BLOCK, cols), 1)
    first_lane, last_lane = lane == 0, lane == cols - 1
    zero = jnp.zeros((BLOCK, cols), jnp.float32)

    def to_right(x):
        return pltpu.roll(x, cols - 1, 1)

    def to_left(x):
        return pltpu.roll(x, 1, 1)

    def at(r):
        return pl.ds(r, BLOCK)

    def column(name, r):
        x = pad[name][pl.ds(r, BLOCK + 2 * PAD), :]
        return x[PAD:PAD + BLOCK], x[PAD - 1:PAD + BLOCK - 1], x[PAD + 1:PAD + BLOCK + 1]

    def sweep(first, count, body, carry):
        def step(i, carry):
            return body(pl.multiple_of(first + i * BLOCK, BLOCK), carry)

        return lax.fori_loop(0, count // BLOCK, step, carry)

    def weights(r, carry):
        k, k_down, k_up = column("k", r)
        row = lax.broadcasted_iota(jnp.int32, (BLOCK, cols), 0) + r
        k_before = jnp.where(place == 0, zero, side["k"][0, at(r), :])
        k_after = jnp.where(place == slabs - 1, zero, side["k"][1, at(r), :])
        faces = [
            0.5 * (k + k_before),
            0.5 * (k + k_after),
            0.5 * (k + k_down),
            0.5 * (k + k_up),
            0.5 * (k + jnp.where(first_lane, zero, to_left(k))),
            0.5 * (k + jnp.where(last_lane, zero, to_right(k))),
        ]
        total = faces[1] + faces[0] + faces[3] + faces[2] + faces[5] + faces[4]
        plane["dg"][at(r), :] = -total
        plane["wxm"][at(r), :] = jnp.where(place == 0, zero, faces[0])
        plane["wxp"][at(r), :] = jnp.where(place == slabs - 1, zero, faces[1])
        plane["wym"][at(r), :] = jnp.where(row == 0, zero, faces[2])
        plane["wyp"][at(r), :] = jnp.where(row == rows - 1, zero, faces[3])
        plane["wzm"][at(r), :] = jnp.where(first_lane, zero, faces[4])
        plane["wzp"][at(r), :] = jnp.where(last_lane, zero, faces[5])
        return carry

    sweep(0, rows, weights, 0)

    def heat(name, r):
        mid, down, up = column(name, r)
        out = plane["wxp"][at(r), :] * side[name][1, at(r), :]
        out = out + plane["wxm"][at(r), :] * side[name][0, at(r), :]
        out = out + plane["wyp"][at(r), :] * up + plane["wym"][at(r), :] * down
        out = out + plane["wzp"][at(r), :] * to_right(mid) + plane["wzm"][at(r), :] * to_left(mid)
        return mid, out + plane["dg"][at(r), :] * mid

    def fold(x):
        return jnp.sum(x.reshape(BLOCK // 8, 8, cols), axis=0)

    nothing = jnp.zeros((8, cols), jnp.float32)

    def quadratic(name, beside, weight, r):
        mid, _, up = column(name, r)
        twice = plane[weight][at(r), :] * beside[at(r), :]
        twice = twice + plane["wyp"][at(r), :] * up + plane["wzp"][at(r), :] * to_right(mid)
        return fold(mid * (twice + twice + plane["dg"][at(r), :] * mid))

    def moments(name, beside, c):
        weight = "wxm" if c < CHUNKS // 2 else "wxp"
        beside = beside(0 if c < CHUNKS // 2 else 1)
        return sweep(c * chunk, chunk, lambda r, acc: acc + quadratic(name, beside, weight, r), nothing)

    spot = lax.broadcasted_iota(jnp.int32, (1, 128), 1)

    def lanes(acc):
        both = acc[:, 0:128]
        for i in range(1, cols // 128):
            both = both + acc[:, i * 128:(i + 1) * 128]
        return jnp.sum(both, axis=0, keepdims=True)

    def burst(src, slots, devices, sem):
        middle = (len(devices) - 1) / 2
        for k in sorted(range(len(devices)), key=lambda k: abs(k - middle)):
            pltpu.make_async_remote_copy(
                src_ref=src, dst_ref=slots.at[pl.ds(k, 1), :],
                send_sem=gsend.at[sem], recv_sem=grecv.at[sem],
                device_id=devices[k], device_id_type=MESH,
            ).start()
        whole = slots.at[pl.ds(0, len(devices)), :]
        return pltpu.make_async_remote_copy(
            src_ref=whole, dst_ref=whole, send_sem=gsend.at[sem], recv_sem=grecv.at[sem],
            device_id=after, device_id_type=MESH,
        )

    bursts = [shared]

    def reduce_z(n, accs):
        rows_of = jnp.concatenate([lanes(acc) for acc in accs + [nothing] * (8 - len(accs))], axis=0)
        sums = jnp.sum(rows_of, axis=1, keepdims=True)
        row = jnp.zeros((1, 128), jnp.float32)
        for q in range(len(accs)):
            row = jnp.where(spot == q, sums[q:q + 1, :], row)
        tiles[n, 0:1, :] = row
        devices = [z_peer(k) for k in range(1, nz)]
        waits = burst(tiles.at[n, pl.ds(0, 1), :], zslots.at[n], devices, 1 + 3 * n)
        bursts.append(waits)
        return waits

    def reduce_y(n, waits, also=False):
        waits.wait_recv()
        ztiles[n, 0:1, :] = tiles[n, 0:1, :] + jnp.sum(zslots[n, 0:nz - 1, :], axis=0, keepdims=True)
        src = ztiles.at[n, pl.ds(0, 1), :]
        out = [burst(src, yslots.at[n], [y_peer(k) for k in range(1, ny)], 2 + 3 * n)]
        if also:
            out.append(burst(src, xslots, [y_peer(k, next_t) for k in range(ny)], 3 + 3 * n))
        bursts.extend(out)
        return out

    def total_own(n, waits):
        waits.wait_recv()
        return ztiles[n, 0:1, :] + jnp.sum(yslots[n, 0:ny - 1, :], axis=0, keepdims=True)

    def total_last(waits):
        waits.wait_recv()
        return jnp.sum(xslots[0:ny, :], axis=0, keepdims=True)

    def factors(sums, first, h):
        s0, s1, s2, s3 = [sums[:, first + i:first + i + 1] for i in range(4)]
        sigma = s1 / s0
        spread = jnp.maximum(s2 - s1 * sigma, 1e-30)
        bent = s3 - sigma * (s2 + s2) + sigma * sigma * s1
        one = s0 / (s0 - h * s1)
        part = spread / s0
        two = 1.0 / jnp.maximum(1.0 - h * bent / spread - one * (h * h) * part, 1.0)
        slope = (one * h) * (one * h) * part
        c1 = one * two * h
        c0 = one + two * slope - c1 * sigma
        return c0, c1

    def whole(x):
        return jnp.concatenate([jnp.broadcast_to(x, (8, cols))] * (BLOCK // 8), axis=0)

    def first_fields(r, carry):
        mids, images = zip(*[heat("u%d" % j, r) for j in range(3)])
        begin = plane["s"][at(r), :]
        leads = [begin - mids[0], mids[0] - mids[1], mids[1] - mids[2]]
        rc = None
        for m, name in enumerate(["a", "b", "d"]):
            value = leads[m]
            for j in range(3):
                value = value + WEIGHT[m][j] * images[j]
            pad[name][pl.ds(PAD + r, BLOCK), :] = value
            rc = value if rc is None else rc + value
        plane["rc"][at(r), :] = rc
        return carry

    a_in, b_in, d_in, la_in = {}, {}, {}, {}
    for c in each:
        arrive(u_in[c])
        sweep(c * chunk, chunk, first_fields, 0)
        a_in[c] = swap("a", c)
    put(plane["rc"], plane["xrc"], next_device, 2, early)

    def first_heat(r, carry):
        s0, s1, s2 = carry
        mid, out = heat("a", r)
        pad["la"][pl.ds(PAD + r, BLOCK), :] = out
        return s0 + fold(mid * mid), s1 + fold(mid * out), s2 + fold(out * out)

    sums = (nothing,) * 3
    for c in each:
        arrive(a_in[c])
        sums = sweep(c * chunk, chunk, first_heat, sums)
        la_in[c] = swap("la", c)
    for c in each[:3]:
        b_in[c] = swap("b", c)

    def second_field(r, carry):
        plane["lb"][at(r), :] = heat("b", r)[1]
        return carry

    def take_b(chunks):
        for c in chunks:
            arrive(b_in[c])
            sweep(c * chunk, chunk, second_field, 0)

    def second_heat(r, carry):
        mid, out = heat("la", r)
        plane["lla"][at(r), :] = out
        return carry + fold(mid * out)

    s3 = nothing
    for c in each:
        arrive(la_in[c])
        s3 = sweep(c * chunk, chunk, second_heat, s3)
    z_wait = reduce_z(0, list(sums) + [s3])
    for c in each[3:]:
        b_in[c] = swap("b", c)
    for c in order[:4]:
        d_in[c] = swap("d", c)

    def third_field(r, carry):
        s0, s1, s2 = carry
        ld = heat("d", r)[1]
        rc = plane["rc"][at(r), :]
        vc = pad["la"][pl.ds(PAD + r, BLOCK), :] + plane["lb"][at(r), :] + ld
        plane["ld"][at(r), :] = ld
        pad["vc"][pl.ds(PAD + r, BLOCK), :] = vc
        return s0 + fold(rc * rc), s1 + fold(rc * vc), s2 + fold(vc * vc)

    coarse = (nothing,) * 3
    vc_in = {}

    def take_d(chunks, coarse):
        for c in chunks:
            arrive(d_in[c])
            coarse = sweep(c * chunk, chunk, third_field, coarse)
            onward(inner("vc", c * chunk, chunk), "xvc", c, early)
            if c >= half:
                vc_in[c - half] = give_half("vc", c - half)
        return coarse

    take_b(each[:4])
    (y_wait,) = reduce_y(0, z_wait)
    take_b(each[4:])
    c0, c1 = [whole(x) for x in factors(total_own(0, y_wait), 0, WIDTH[0])]

    def second_node(r, carry):
        s0, s1, s2 = carry
        at_pad = pl.ds(PAD + r, BLOCK)
        a, la, lla = pad["a"][at_pad, :], pad["la"][at_pad, :], plane["lla"][at(r), :]
        move = c0 * a + c1 * la
        fine[0, at(r), :] = pad["u0"][at_pad, :] + move
        r2 = pad["b"][at_pad, :] + move
        v2 = plane["lb"][at(r), :] + c0 * la + c1 * lla
        plane["r2"][at(r), :] = r2
        pad["v2"][at_pad, :] = v2
        return s0 + fold(r2 * r2), s1 + fold(r2 * v2), s2 + fold(v2 * v2)

    sums = (nothing,) * 3
    v_in, w_in = {}, {}
    for c in order:
        sums = sweep(c * chunk, chunk, second_node, sums)
        if c >= half:
            v_in[c - half] = swap_half("v2", c - half, False)
    coarse = take_d(order[:4], coarse)
    w_in[0] = swap_half("v2", 0, True)
    s3 = nothing
    for i in range(half):
        arrive(v_in[i])
        for c in (i, i + half):
            s3 = s3 + moments("v2", lambda s: side["v2"].at[s], c)
    z_wait = reduce_z(1, list(sums) + [s3])
    for i in range(1, half):
        w_in[i] = swap_half("v2", i, True)
    for c in order[4:]:
        d_in[c] = swap("d", c)

    def third_heat(r, carry):
        plane["lv2"][at(r), :] = heat("v2", r)[1]
        return carry

    def take_w(pairs):
        for i in pairs:
            arrive(w_in[i])
            for c in (i, i + half):
                sweep(c * chunk, chunk, third_heat, 0)

    take_w(range(2))
    (y_wait,) = reduce_y(1, z_wait)
    take_w(range(2, half))
    coarse = take_d(order[4:6], coarse)
    e0, e1 = [whole(x) for x in factors(total_own(1, y_wait), 0, WIDTH[1])]

    def third_node(r, carry):
        s0, s1, s2 = carry
        at_pad = pl.ds(PAD + r, BLOCK)
        r2, v2, lv2 = plane["r2"][at(r), :], pad["v2"][at_pad, :], plane["lv2"][at(r), :]
        move = e0 * r2 + e1 * v2
        fine[1, at(r), :] = pad["u1"][at_pad, :] + move
        r3 = pad["d"][at_pad, :] + move
        v3 = plane["ld"][at(r), :] + e0 * v2 + e1 * lv2
        plane["r3"][at(r), :] = r3
        pad["v3"][at_pad, :] = v3
        return s0 + fold(r3 * r3), s1 + fold(r3 * v3), s2 + fold(v3 * v3)

    sums = (nothing,) * 3
    v3_in = {}

    def take_node(chunks, sums):
        for c in chunks:
            sums = sweep(c * chunk, chunk, third_node, sums)
            if c >= half:
                v3_in[c - half] = give_half("v3", c - half)
            onward(plane["r3"].at[pl.ds(c * chunk, chunk), :], "xr3", c, late)
            onward(inner("v3", c * chunk, chunk), "xv3", c, late)
        return sums

    sums = take_node(order[:4], sums)
    coarse = take_d(order[6:], coarse)
    sums = take_node(order[4:], sums)
    coarse3, s3 = nothing, nothing
    for i in range(half):
        arrive(vc_in[i])
        for c in (i, i + half):
            coarse3 = coarse3 + moments("vc", lambda s: plane["hvc"], c)
    for i in range(half):
        arrive(v3_in[i])
        for c in (i, i + half):
            s3 = s3 + moments("v3", lambda s: plane["hv3"], c)
    z_wait = reduce_z(2, list(sums) + [s3] + list(coarse) + [coarse3])
    expect(planes.at[pl.ds(0, 3)], 2, early).wait_recv()

    def first_slice(r, carry):
        plane["xu"][at(r), :] = jnp.where(me_t == 0, plane["s"][at(r), :], plane["xu"][at(r), :])
        return carry

    sweep(0, rows, first_slice, 0)
    y_wait, x_wait = reduce_y(2, z_wait, also=True)
    expect(planes.at[pl.ds(0, 2)], 2, late).wait_recv()
    expect(sides.at[pl.ds(1, len(SIDES) - 1)], 0, 0).wait_send()
    expect(planes.at[pl.ds(0, 2)], 1, 0).wait_send()
    expect(planes.at[pl.ds(0, 5)], 2, 0).wait_send()
    k_in.wait_send()
    for waits in bursts[:-2]:
        waits.wait_send()
    g0, g1 = [whole(x) for x in factors(total_own(2, y_wait), 0, WIDTH[2])]

    def last_node(r, carry):
        at_pad = pl.ds(PAD + r, BLOCK)
        move = g0 * plane["r3"][at(r), :] + g1 * pad["v3"][at_pad, :]
        fine[2, at(r), :] = pad["u2"][at_pad, :] + move
        return carry

    sweep(0, rows, last_node, 0)
    sums = total_last(x_wait)
    passed = [jnp.where(me_t == 0, 0.0, x) for x in factors(sums, 0, WIDTH[2]) + factors(sums, 4, STEP)]
    p0, p1, q0, q1 = [whole(x) for x in passed]

    def next_slice(r, carry):
        guess = plane["xu"][at(r), :]
        following[at(r), :] = guess + (p0 * plane["xr3"][at(r), :] + p1 * plane["xv3"][at(r), :])
        coarse_next[at(r), :] = guess + (q0 * plane["xrc"][at(r), :] + q1 * plane["xvc"][at(r), :])
        return carry

    sweep(0, rows, next_slice, 0)
    for waits in bursts[-2:]:
        waits.wait_send()


def slots_needed():
    return 1 + 2 + 5 * CHUNKS + 4 * (CHUNKS // 2)


def leave(fine, following, coarse, fine_hbm, following_hbm, coarse_hbm, sem):
    copies = [
        pltpu.make_async_copy(src, dst, sem.at[i])
        for i, (src, dst) in enumerate(
            [(fine, fine_hbm), (following, following_hbm), (coarse, coarse_hbm)]
        )
    ]
    for copy in copies:
        copy.start()
    for copy in copies:
        copy.wait()


def on_device(dims, start_value, old_nodes, diffusivity):
    nt, ny, nz, rows, cols = dims
    anywhere = pl.BlockSpec(memory_space=pl.ANY)
    near = pl.BlockSpec(memory_space=pltpu.VMEM)
    plane = jax.ShapeDtypeStruct((rows, cols), jnp.float32)
    inputs = [
        pltpu.with_memory_space_constraint(value, pltpu.MemorySpace.HBM)
        for value in (
            start_value.reshape(rows, cols),
            old_nodes.reshape(3, rows, cols),
            diffusivity.reshape(rows, cols),
        )
    ]
    fine, following, coarse = pl.pallas_call(
        functools.partial(kernel, dims),
        out_shape=(jax.ShapeDtypeStruct((3, rows, cols), jnp.float32), plane, plane),
        in_specs=[anywhere] * 3,
        out_specs=(near,) * 3,
        scratch_shapes=[
            pltpu.VMEM((len(PADDED), rows + 2 * PAD, cols), jnp.float32),
            pltpu.VMEM((len(PLANES), rows, cols), jnp.float32),
            pltpu.VMEM((len(SIDES), 2, rows, cols), jnp.float32),
            pltpu.VMEM((3, 8, 128), jnp.float32),
            pltpu.VMEM((3, 8, 128), jnp.float32),
            pltpu.VMEM((3, 16, 128), jnp.float32),
            pltpu.VMEM((3, 8, 128), jnp.float32),
            pltpu.VMEM((8, 128), jnp.float32),
            pltpu.SemaphoreType.DMA((4,)),
            pltpu.SemaphoreType.DMA((slots_needed(),)),
            pltpu.SemaphoreType.DMA((10,)),
            pltpu.SemaphoreType.DMA((10,)),
            pltpu.SemaphoreType.DMA((5,)),
        ],
        compiler_params=pltpu.CompilerParams(
            collective_id=0, has_side_effects=True, vmem_limit_bytes=40 * 1024 * 1024
        ),
    )(*inputs)
    fine, following, coarse = pl.pallas_call(
        leave,
        out_shape=(jax.ShapeDtypeStruct((3, rows, cols), jnp.float32), plane, plane),
        in_specs=[anywhere] * 3,
        out_specs=(anywhere,) * 3,
        scratch_shapes=[pltpu.SemaphoreType.DMA((3,))],
        compiler_params=pltpu.CompilerParams(vmem_limit_bytes=40 * 1024 * 1024),
    )(fine, following, coarse)
    return (
        fine.reshape(1, 3, 1, rows, cols),
        following.reshape(1, 1, rows, cols),
        coarse.reshape(1, 1, rows, cols),
    )


def build(split, rows, cols):
    dims = (split.shape["tm"], split.shape["y"], split.shape["z"], rows, cols)
    in_specs = (P("tm", SPACE, None, None), P("tm", None, SPACE, None, None), P(SPACE, None, None))
    out_specs = (
        P("tm", None, SPACE, None, None),
        P("tm", SPACE, None, None),
        P("tm", SPACE, None, None),
    )
    return jax.shard_map(
        functools.partial(on_device, dims), mesh=split, in_specs=in_specs, out_specs=out_specs,
        check_vma=False,
    )


def solution(mesh):
    split = Mesh(
        mesh.devices.reshape(mesh.shape["tm"], ROWS_Y, mesh.shape["space"] // ROWS_Y), ("tm",) + SPACE
    )
    return build(split, 512, 256)
```

```python
import functools
import math

import jax
import jax.numpy as jnp
from jax import lax
from jax.experimental import pallas as pl
from jax.experimental.pallas import tpu as pltpu
from jax.sharding import Mesh
from jax.sharding import PartitionSpec as P

MESH = pl.DeviceIdType.MESH
SPACE = ("y", "z")
ROWS_Y = 8
STEP = 2.0
ROOT_SIX = math.sqrt(6.0)
NODE_TIMES = [(4.0 - ROOT_SIX) / 10.0, (4.0 + ROOT_SIX) / 10.0, 1.0]
COLLOC = [
    [
        (88.0 - 7.0 * ROOT_SIX) / 360.0,
        (296.0 - 169.0 * ROOT_SIX) / 1800.0,
        (-2.0 + 3.0 * ROOT_SIX) / 225.0,
    ],
    [
        (296.0 + 169.0 * ROOT_SIX) / 1800.0,
        (88.0 + 7.0 * ROOT_SIX) / 360.0,
        (-2.0 - 3.0 * ROOT_SIX) / 225.0,
    ],
    [(16.0 - ROOT_SIX) / 36.0, (16.0 + ROOT_SIX) / 36.0, 1.0 / 9.0],
]
WEIGHT = [
    [STEP * (COLLOC[m][j] - (COLLOC[m - 1][j] if m else 0.0)) for j in range(3)] for m in range(3)
]
WIDTH = [STEP * (NODE_TIMES[m] - (NODE_TIMES[m - 1] if m else 0.0)) for m in range(3)]
PAD = 8
BLOCK = 32
CHUNKS = 8

PADDED = ["k", "u0", "u1", "u2", "a", "b", "d", "la", "v2", "v3", "vc"]
PLANES = ["s", "wxm", "wxp", "wym", "wyp", "wzm", "wzp", "dg", "lb", "ld", "lla", "lv2"]
PLANES += ["r2", "r3", "rc", "hv3", "hvc", "xu", "xrc", "xvc", "xr3", "xv3"]
SIDES = ["k", "u0", "u1", "u2", "a", "b", "d", "la", "v2"]


def kernel(dims, start_hbm, old_hbm, kappa_hbm, fine, following, coarse_next, padded, planes, sides,
           tiles, ztiles, zslots, yslots, xslots, send, recv, gsend, grecv, local):
    nt, ny, nz, rows, cols = dims
    chunk = rows // CHUNKS
    half = CHUNKS // 2
    each = range(CHUNKS)
    order = [i // 2 + (i % 2) * half for i in each]
    me_t, me_y, me_z = lax.axis_index("tm"), lax.axis_index("y"), lax.axis_index("z")
    place = me_y * nz + me_z
    slabs = ny * nz

    def chain(shift):
        other = lax.rem(place + (slabs + shift), slabs)
        return (me_t, lax.div(other, nz), lax.rem(other, nz))

    after, before = chain(1), chain(-1)
    next_t = lax.rem(me_t + 1, nt)
    last_t = lax.rem(me_t + (nt - 1), nt)

    def z_peer(k):
        return (me_t, me_y, lax.rem(me_z + k, nz))

    def y_peer(k, t=me_t):
        return (t, lax.rem(me_y + k, ny), me_z)

    def t_peer(k):
        return (lax.rem(me_t + k, nt), me_y, me_z)

    pad = {name: padded.at[i] for i, name in enumerate(PADDED)}
    plane = {name: planes.at[i] for i, name in enumerate(PLANES)}
    side = {name: sides.at[i] for i, name in enumerate(SIDES)}

    def inner(name, first=0, count=rows):
        return pad[name].at[pl.ds(PAD + first, count), :]

    loads = [(kappa_hbm, "k"), (old_hbm.at[0], "u0"), (old_hbm.at[1], "u1"), (old_hbm.at[2], "u2")]
    copies = [pltpu.make_async_copy(src, inner(name), local.at[i]) for i, (src, name) in enumerate(loads)]
    copies.append(pltpu.make_async_copy(start_hbm, plane["s"], local.at[4]))
    for copy in copies:
        copy.start()
    barrier = pltpu.get_barrier_semaphore()
    greeted = [after, before]
    greeted += [z_peer(k) for k in range(1, nz)]
    greeted += [y_peer(k) for k in range(1, ny)]
    greeted += [t_peer(k) for k in range(1, nt)]
    greeted += [y_peer(k, last_t) for k in range(ny)]
    for device in greeted:
        pl.semaphore_signal(barrier, inc=1, device_id=device, device_id_type=MESH)
    pl.semaphore_wait(barrier, len(greeted))

    taken = []

    def put(src, dst, device, group, slot):
        pltpu.make_async_remote_copy(
            src_ref=src, dst_ref=dst, send_sem=send.at[group], recv_sem=recv.at[slot],
            device_id=device, device_id_type=MESH,
        ).start()

    def expect(region, group, slot):
        return pltpu.make_async_remote_copy(
            src_ref=region, dst_ref=region, send_sem=send.at[group], recv_sem=recv.at[slot],
            device_id=after, device_id_type=MESH,
        )

    def fresh_slot():
        taken.append(0)
        return len(taken) - 1

    def swap_all(names, c):
        slot = fresh_slot()
        there = pl.ds(c * chunk, chunk)
        for name in names:
            here = inner(name, c * chunk, chunk)
            put(here, side[name].at[0, there, :], after, 0, slot)
            put(here, side[name].at[1, there, :], before, 0, slot)
        first = SIDES.index(names[0])
        return expect(sides.at[pl.ds(first, len(names)), :, there, :], 0, slot)

    def swap(name, c):
        return swap_all([name], c)

    def swap_half(name, i, second):
        slot = fresh_slot()
        for c, up in ((i, not second), (i + half, second)):
            there = pl.ds(c * chunk, chunk)
            dst = side[name].at[0 if up else 1, there, :]
            put(inner(name, c * chunk, chunk), dst, after if up else before, 0, slot)
        return expect(side[name].at[:, pl.ds(0, chunk), :], 0, slot)

    def give_half(name, i):
        slot = fresh_slot()
        for c, up in ((i, True), (i + half, False)):
            dst = plane["h" + name].at[pl.ds(c * chunk, chunk), :]
            put(inner(name, c * chunk, chunk), dst, after if up else before, 1, slot)
        return expect(side["v2"].at[:, pl.ds(0, chunk), :], 1, slot)

    next_device = (next_t, me_y, me_z)
    early, late = fresh_slot(), fresh_slot()

    def onward(src, name, c, slot):
        put(src, plane[name].at[pl.ds(c * chunk, chunk), :], next_device, 2, slot)

    def arrive(waiter):
        waiter.wait_recv()

    givers = nt // 2
    share = rows // givers
    own = pl.multiple_of(lax.div(me_t, 2) * share, share)
    mine = pl.ds(own, share)
    gives = lax.rem(me_t, 2) == 1
    k_slot = fresh_slot()
    k_in = expect(side["k"].at[:, mine, :], 3, k_slot)
    copies[0].wait()

    @pl.when(gives)
    def _():
        k_src = pad["k"].at[pl.ds(pl.multiple_of(PAD + own, PAD), share), :]
        put(k_src, side["k"].at[0, mine, :], after, 3, k_slot)
        put(k_src, side["k"].at[1, mine, :], before, 3, k_slot)

    for copy in copies[1:4]:
        copy.wait()
    u_in = [swap_all(["u0", "u1", "u2"], c) for c in each]
    put(inner("u2"), plane["xu"], next_device, 2, early)
    edge = jnp.zeros((PAD, cols), jnp.float32)
    for name in PADDED:
        pad[name][pl.ds(0, PAD), :] = edge
        pad[name][pl.ds(PAD + rows, PAD), :] = edge
    copies[4].wait()

    def spread(region):
        return pltpu.make_async_remote_copy(
            src_ref=region, dst_ref=region, send_sem=gsend.at[0], recv_sem=grecv.at[0],
            device_id=after, device_id_type=MESH,
        )

    @pl.when(gives)
    def _():
        arrive(k_in)
        for s in range(2):
            block = side["k"].at[s, mine, :]
            for k in range(1, nt):
                pltpu.make_async_remote_copy(
                    src_ref=block, dst_ref=block, send_sem=gsend.at[0], recv_sem=grecv.at[0],
                    device_id=t_peer(k), device_id_type=MESH,
                ).start()
        if givers > 1:
            spread(side["k"].at[:, pl.ds(0, share * (givers - 1)), :]).wait_recv()

    @pl.when(jnp.logical_not(gives))
    def _():
        spread(side["k"]).wait_recv()

    lane = lax.broadcasted_iota(jnp.int32, (BLOCK, cols), 1)
    first_lane, last_lane = lane == 0, lane == cols - 1
    zero = jnp.zeros((BLOCK, cols), jnp.float32)

    def to_right(x):
        return pltpu.roll(x, cols - 1, 1)

    def to_left(x):
        return pltpu.roll(x, 1, 1)

    def at(r):
        return pl.ds(r, BLOCK)

    def column(name, r):
        x = pad[name][pl.ds(r, BLOCK + 2 * PAD), :]
        return x[PAD:PAD + BLOCK], x[PAD - 1:PAD + BLOCK - 1], x[PAD + 1:PAD + BLOCK + 1]

    def sweep(first, count, body, carry):
        def step(i, carry):
            return body(pl.multiple_of(first + i * BLOCK, BLOCK), carry)

        return lax.fori_loop(0, count // BLOCK, step, carry)

    def weights(r, carry):
        k, k_down, k_up = column("k", r)
        row = lax.broadcasted_iota(jnp.int32, (BLOCK, cols), 0) + r
        k_before = jnp.where(place == 0, zero, side["k"][0, at(r), :])
        k_after = jnp.where(place == slabs - 1, zero, side["k"][1, at(r), :])
        faces = [
            0.5 * (k + k_before),
            0.5 * (k + k_after),
            0.5 * (k + k_down),
            0.5 * (k + k_up),
            0.5 * (k + jnp.where(first_lane, zero, to_left(k))),
            0.5 * (k + jnp.where(last_lane, zero, to_right(k))),
        ]
        total = faces[1] + faces[0] + faces[3] + faces[2] + faces[5] + faces[4]
        plane["dg"][at(r), :] = -total
        plane["wxm"][at(r), :] = jnp.where(place == 0, zero, faces[0])
        plane["wxp"][at(r), :] = jnp.where(place == slabs - 1, zero, faces[1])
        plane["wym"][at(r), :] = jnp.where(row == 0, zero, faces[2])
        plane["wyp"][at(r), :] = jnp.where(row == rows - 1, zero, faces[3])
        plane["wzm"][at(r), :] = jnp.where(first_lane, zero, faces[4])
        plane["wzp"][at(r), :] = jnp.where(last_lane, zero, faces[5])
        return carry

    sweep(0, rows, weights, 0)

    def heat(name, r):
        mid, down, up = column(name, r)
        out = plane["wxp"][at(r), :] * side[name][1, at(r), :]
        out = out + plane["wxm"][at(r), :] * side[name][0, at(r), :]
        out = out + plane["wyp"][at(r), :] * up + plane["wym"][at(r), :] * down
        out = out + plane["wzp"][at(r), :] * to_right(mid) + plane["wzm"][at(r), :] * to_left(mid)
        return mid, out + plane["dg"][at(r), :] * mid

    def fold(x):
        return jnp.sum(x.reshape(BLOCK // 8, 8, cols), axis=0)

    nothing = jnp.zeros((8, cols), jnp.float32)

    def quadratic(name, beside, weight, r):
        mid, _, up = column(name, r)
        twice = plane[weight][at(r), :] * beside[at(r), :]
        twice = twice + plane["wyp"][at(r), :] * up + plane["wzp"][at(r), :] * to_right(mid)
        return fold(mid * (twice + twice + plane["dg"][at(r), :] * mid))

    def moments(name, beside, c):
        weight = "wxm" if c < CHUNKS // 2 else "wxp"
        beside = beside(0 if c < CHUNKS // 2 else 1)
        return sweep(c * chunk, chunk, lambda r, acc: acc + quadratic(name, beside, weight, r), nothing)

    spot = lax.broadcasted_iota(jnp.int32, (1, 128), 1)

    def lanes(acc):
        both = acc[:, 0:128]
        for i in range(1, cols // 128):
            both = both + acc[:, i * 128:(i + 1) * 128]
        return jnp.sum(both, axis=0, keepdims=True)

    def burst(src, slots, devices, sem):
        middle = (len(devices) - 1) / 2
        for k in sorted(range(len(devices)), key=lambda k: abs(k - middle)):
            pltpu.make_async_remote_copy(
                src_ref=src, dst_ref=slots.at[pl.ds(k, 1), :],
                send_sem=gsend.at[sem], recv_sem=grecv.at[sem],
                device_id=devices[k], device_id_type=MESH,
            ).start()
        whole = slots.at[pl.ds(0, len(devices)), :]
        return pltpu.make_async_remote_copy(
            src_ref=whole, dst_ref=whole, send_sem=gsend.at[sem], recv_sem=grecv.at[sem],
            device_id=after, device_id_type=MESH,
        )

    bursts = []

    def reduce_z(n, accs):
        rows_of = jnp.concatenate([lanes(acc) for acc in accs + [nothing] * (8 - len(accs))], axis=0)
        sums = jnp.sum(rows_of, axis=1, keepdims=True)
        row = jnp.zeros((1, 128), jnp.float32)
        for q in range(len(accs)):
            row = jnp.where(spot == q, sums[q:q + 1, :], row)
        tiles[n, 0:1, :] = row
        devices = [z_peer(k) for k in range(1, nz)]
        waits = burst(tiles.at[n, pl.ds(0, 1), :], zslots.at[n], devices, 1 + 3 * n)
        bursts.append(waits)
        return waits

    def reduce_y(n, waits, also=False):
        waits.wait_recv()
        ztiles[n, 0:1, :] = tiles[n, 0:1, :] + jnp.sum(zslots[n, 0:nz - 1, :], axis=0, keepdims=True)
        src = ztiles.at[n, pl.ds(0, 1), :]
        out = [burst(src, yslots.at[n], [y_peer(k) for k in range(1, ny)], 2 + 3 * n)]
        if also:
            out.append(burst(src, xslots, [y_peer(k, next_t) for k in range(ny)], 3 + 3 * n))
        bursts.extend(out)
        return out

    def total_own(n, waits):
        waits.wait_recv()
        return ztiles[n, 0:1, :] + jnp.sum(yslots[n, 0:ny - 1, :], axis=0, keepdims=True)

    def total_last(waits):
        waits.wait_recv()
        return jnp.sum(xslots[0:ny, :], axis=0, keepdims=True)

    def factors(row, h):
        s0, s1, s2, s3 = row, pltpu.roll(row, 127, 1), pltpu.roll(row, 126, 1), pltpu.roll(row, 125, 1)
        sigma = s1 / s0
        spread = jnp.maximum(s2 - s1 * sigma, 1e-30)
        bent = s3 - sigma * (s2 + s2) + sigma * sigma * s1
        one = s0 / (s0 - h * s1)
        part = spread / s0
        two = 1.0 / jnp.maximum(1.0 - h * bent / spread - one * (h * h) * part, 1.0)
        slope = (one * h) * (one * h) * part
        c1 = one * two * h
        c0 = one + two * slope - c1 * sigma
        return c0, c1

    def whole(x):
        return jnp.concatenate([jnp.broadcast_to(x, (8, cols))] * (BLOCK // 8), axis=0)

    def first_fields(r, carry):
        mids, images = zip(*[heat("u%d" % j, r) for j in range(3)])
        begin = plane["s"][at(r), :]
        leads = [begin - mids[0], mids[0] - mids[1], mids[1] - mids[2]]
        rc = None
        for m, name in enumerate(["a", "b", "d"]):
            value = leads[m]
            for j in range(3):
                value = value + WEIGHT[m][j] * images[j]
            pad[name][pl.ds(PAD + r, BLOCK), :] = value
            rc = value if rc is None else rc + value
        plane["rc"][at(r), :] = rc
        return carry

    a_in, b_in, d_in, la_in = {}, {}, {}, {}
    for c in each:
        arrive(u_in[c])
        sweep(c * chunk, chunk, first_fields, 0)
        a_in[c] = swap("a", c)
    put(plane["rc"], plane["xrc"], next_device, 2, early)

    def first_heat(r, carry):
        s0, s1, s2 = carry
        mid, out = heat("a", r)
        pad["la"][pl.ds(PAD + r, BLOCK), :] = out
        return s0 + fold(mid * mid), s1 + fold(mid * out), s2 + fold(out * out)

    sums = (nothing,) * 3
    for c in each:
        arrive(a_in[c])
        sums = sweep(c * chunk, chunk, first_heat, sums)
        la_in[c] = swap("la", c)
    for c in each[:3]:
        b_in[c] = swap("b", c)

    def second_field(r, carry):
        plane["lb"][at(r), :] = heat("b", r)[1]
        return carry

    def take_b(chunks):
        for c in chunks:
            arrive(b_in[c])
            sweep(c * chunk, chunk, second_field, 0)

    def second_heat(r, carry):
        mid, out = heat("la", r)
        plane["lla"][at(r), :] = out
        return carry + fold(mid * out)

    s3 = nothing
    for c in each:
        arrive(la_in[c])
        s3 = sweep(c * chunk, chunk, second_heat, s3)
    z_wait = reduce_z(0, list(sums) + [s3])
    for c in each[3:]:
        b_in[c] = swap("b", c)
    for c in order[:4]:
        d_in[c] = swap("d", c)

    def third_field(r, carry):
        s0, s1, s2 = carry
        ld = heat("d", r)[1]
        rc = plane["rc"][at(r), :]
        vc = pad["la"][pl.ds(PAD + r, BLOCK), :] + plane["lb"][at(r), :] + ld
        plane["ld"][at(r), :] = ld
        pad["vc"][pl.ds(PAD + r, BLOCK), :] = vc
        return s0 + fold(rc * rc), s1 + fold(rc * vc), s2 + fold(vc * vc)

    coarse = (nothing,) * 3
    vc_in = {}

    def take_d(chunks, coarse):
        for c in chunks:
            arrive(d_in[c])
            coarse = sweep(c * chunk, chunk, third_field, coarse)
            onward(inner("vc", c * chunk, chunk), "xvc", c, early)
            if c >= half:
                vc_in[c - half] = give_half("vc", c - half)
        return coarse

    take_b(each[:4])
    (y_wait,) = reduce_y(0, z_wait)
    take_b(each[4:])
    c0, c1 = [whole(x[:, 0:1]) for x in factors(total_own(0, y_wait), WIDTH[0])]

    def second_node(r, carry):
        s0, s1, s2 = carry
        at_pad = pl.ds(PAD + r, BLOCK)
        a, la, lla = pad["a"][at_pad, :], pad["la"][at_pad, :], plane["lla"][at(r), :]
        move = c0 * a + c1 * la
        fine[0, at(r), :] = pad["u0"][at_pad, :] + move
        r2 = pad["b"][at_pad, :] + move
        v2 = plane["lb"][at(r), :] + c0 * la + c1 * lla
        plane["r2"][at(r), :] = r2
        pad["v2"][at_pad, :] = v2
        return s0 + fold(r2 * r2), s1 + fold(r2 * v2), s2 + fold(v2 * v2)

    sums = (nothing,) * 3
    v_in, w_in = {}, {}
    for c in order:
        sums = sweep(c * chunk, chunk, second_node, sums)
        if c >= half:
            v_in[c - half] = swap_half("v2", c - half, False)
    coarse = take_d(order[:4], coarse)
    w_in[0] = swap_half("v2", 0, True)
    s3 = nothing
    for i in range(half):
        arrive(v_in[i])
        for c in (i, i + half):
            s3 = s3 + moments("v2", lambda s: side["v2"].at[s], c)
    z_wait = reduce_z(1, list(sums) + [s3])
    for i in range(1, half):
        w_in[i] = swap_half("v2", i, True)
    for c in order[4:]:
        d_in[c] = swap("d", c)

    def third_heat(r, carry):
        plane["lv2"][at(r), :] = heat("v2", r)[1]
        return carry

    def take_w(pairs):
        for i in pairs:
            arrive(w_in[i])
            for c in (i, i + half):
                sweep(c * chunk, chunk, third_heat, 0)

    take_w(range(2))
    (y_wait,) = reduce_y(1, z_wait)
    take_w(range(2, half))
    coarse = take_d(order[4:6], coarse)
    e0, e1 = [whole(x[:, 0:1]) for x in factors(total_own(1, y_wait), WIDTH[1])]

    def third_node(r, carry):
        s0, s1, s2 = carry
        at_pad = pl.ds(PAD + r, BLOCK)
        r2, v2, lv2 = plane["r2"][at(r), :], pad["v2"][at_pad, :], plane["lv2"][at(r), :]
        move = e0 * r2 + e1 * v2
        fine[1, at(r), :] = pad["u1"][at_pad, :] + move
        r3 = pad["d"][at_pad, :] + move
        v3 = plane["ld"][at(r), :] + e0 * v2 + e1 * lv2
        plane["r3"][at(r), :] = r3
        pad["v3"][at_pad, :] = v3
        return s0 + fold(r3 * r3), s1 + fold(r3 * v3), s2 + fold(v3 * v3)

    sums = (nothing,) * 3
    v3_in = {}

    def take_node(chunks, sums):
        for c in chunks:
            sums = sweep(c * chunk, chunk, third_node, sums)
            if c >= half:
                v3_in[c - half] = give_half("v3", c - half)
            onward(plane["r3"].at[pl.ds(c * chunk, chunk), :], "xr3", c, late)
            onward(inner("v3", c * chunk, chunk), "xv3", c, late)
        return sums

    sums = take_node(order[:4], sums)
    coarse = take_d(order[6:], coarse)
    sums = take_node(order[4:], sums)
    coarse3, s3 = nothing, nothing
    for i in range(half):
        arrive(vc_in[i])
        for c in (i, i + half):
            coarse3 = coarse3 + moments("vc", lambda s: plane["hvc"], c)
    for i in range(half):
        arrive(v3_in[i])
        for c in (i, i + half):
            s3 = s3 + moments("v3", lambda s: plane["hv3"], c)
    z_wait = reduce_z(2, list(sums) + [s3] + list(coarse) + [coarse3])
    expect(planes.at[pl.ds(0, 3)], 2, early).wait_recv()

    def first_slice(r, carry):
        plane["xu"][at(r), :] = jnp.where(me_t == 0, plane["s"][at(r), :], plane["xu"][at(r), :])
        return carry

    sweep(0, rows, first_slice, 0)
    y_wait, x_wait = reduce_y(2, z_wait, also=True)
    expect(planes.at[pl.ds(0, 2)], 2, late).wait_recv()
    expect(sides.at[pl.ds(1, len(SIDES) - 1)], 0, 0).wait_send()
    expect(planes.at[pl.ds(0, 2)], 1, 0).wait_send()
    expect(planes.at[pl.ds(0, 5)], 2, 0).wait_send()

    @pl.when(gives)
    def _():
        k_in.wait_send()
        spread(sides.at[pl.ds(0, 2), :, pl.ds(0, share * (nt - 1) // 2), :]).wait_send()

    for waits in bursts[:-2]:
        waits.wait_send()
    both = jnp.concatenate([total_own(2, y_wait), total_last(x_wait)], axis=0)
    width = jnp.where(lax.broadcasted_iota(jnp.int32, (2, 128), 1) == 4, STEP, WIDTH[2])
    f0, f1 = factors(both, width)
    g0, g1 = whole(f0[0:1, 0:1]), whole(f1[0:1, 0:1])
    passed = [x[1:2, q:q + 1] for q in (0, 4) for x in (f0, f1)]
    p0, p1, q0, q1 = [whole(jnp.where(me_t == 0, 0.0, x)) for x in passed]

    def last_node(r, carry):
        at_pad = pl.ds(PAD + r, BLOCK)
        fine[2, at(r), :] = pad["u2"][at_pad, :] + (g0 * plane["r3"][at(r), :] + g1 * pad["v3"][at_pad, :])
        guess = plane["xu"][at(r), :]
        following[at(r), :] = guess + (p0 * plane["xr3"][at(r), :] + p1 * plane["xv3"][at(r), :])
        coarse_next[at(r), :] = guess + (q0 * plane["xrc"][at(r), :] + q1 * plane["xvc"][at(r), :])
        return carry

    sweep(0, rows, last_node, 0)
    for waits in bursts[-2:]:
        waits.wait_send()


def slots_needed():
    return 1 + 2 + 5 * CHUNKS + 4 * (CHUNKS // 2)


def leave(fine, following, coarse, fine_hbm, following_hbm, coarse_hbm, sem):
    rows = following.shape[0] // 2
    pairs = [(fine.at[m], fine_hbm.at[m]) for m in range(3)]
    pairs += [(following, following_hbm), (coarse, coarse_hbm)]
    copies = []
    for src, dst in pairs:
        for first in (0, rows):
            part = pl.ds(first, rows)
            copies.append(
                pltpu.make_async_copy(src.at[part, :], dst.at[part, :], sem.at[len(copies)])
            )
    for copy in copies:
        copy.start()
    for copy in copies:
        copy.wait()


def on_device(dims, start_value, old_nodes, diffusivity):
    nt, ny, nz, rows, cols = dims
    anywhere = pl.BlockSpec(memory_space=pl.ANY)
    near = pl.BlockSpec(memory_space=pltpu.VMEM)
    plane = jax.ShapeDtypeStruct((rows, cols), jnp.float32)
    inputs = [
        pltpu.with_memory_space_constraint(value, pltpu.MemorySpace.HBM)
        for value in (
            start_value.reshape(rows, cols),
            old_nodes.reshape(3, rows, cols),
            diffusivity.reshape(rows, cols),
        )
    ]
    fine, following, coarse = pl.pallas_call(
        functools.partial(kernel, dims),
        out_shape=(jax.ShapeDtypeStruct((3, rows, cols), jnp.float32), plane, plane),
        in_specs=[anywhere] * 3,
        out_specs=(near,) * 3,
        scratch_shapes=[
            pltpu.VMEM((len(PADDED), rows + 2 * PAD, cols), jnp.float32),
            pltpu.VMEM((len(PLANES), rows, cols), jnp.float32),
            pltpu.VMEM((len(SIDES), 2, rows, cols), jnp.float32),
            pltpu.VMEM((3, 8, 128), jnp.float32),
            pltpu.VMEM((3, 8, 128), jnp.float32),
            pltpu.VMEM((3, 16, 128), jnp.float32),
            pltpu.VMEM((3, 8, 128), jnp.float32),
            pltpu.VMEM((8, 128), jnp.float32),
            pltpu.SemaphoreType.DMA((4,)),
            pltpu.SemaphoreType.DMA((slots_needed(),)),
            pltpu.SemaphoreType.DMA((10,)),
            pltpu.SemaphoreType.DMA((10,)),
            pltpu.SemaphoreType.DMA((5,)),
        ],
        compiler_params=pltpu.CompilerParams(
            collective_id=0, has_side_effects=True, vmem_limit_bytes=40 * 1024 * 1024
        ),
    )(*inputs)
    fine, following, coarse = pl.pallas_call(
        leave,
        out_shape=(jax.ShapeDtypeStruct((3, rows, cols), jnp.float32), plane, plane),
        in_specs=[anywhere] * 3,
        out_specs=(anywhere,) * 3,
        scratch_shapes=[pltpu.SemaphoreType.DMA((10,))],
        compiler_params=pltpu.CompilerParams(vmem_limit_bytes=40 * 1024 * 1024),
    )(fine, following, coarse)
    return (
        fine.reshape(1, 3, 1, rows, cols),
        following.reshape(1, 1, rows, cols),
        coarse.reshape(1, 1, rows, cols),
    )


def build(split, rows, cols):
    dims = (split.shape["tm"], split.shape["y"], split.shape["z"], rows, cols)
    in_specs = (P("tm", SPACE, None, None), P("tm", None, SPACE, None, None), P(SPACE, None, None))
    out_specs = (
        P("tm", None, SPACE, None, None),
        P("tm", SPACE, None, None),
        P("tm", SPACE, None, None),
    )
    return jax.shard_map(
        functools.partial(on_device, dims), mesh=split, in_specs=in_specs, out_specs=out_specs,
        check_vma=False,
    )


def solution(mesh):
    split = Mesh(
        mesh.devices.reshape(mesh.shape["tm"], ROWS_Y, mesh.shape["space"] // ROWS_Y), ("tm",) + SPACE
    )
    return build(split, 512, 256)
```

```python
import functools
import math

import jax
import jax.numpy as jnp
from jax import lax
from jax.experimental import pallas as pl
from jax.experimental.pallas import tpu as pltpu
from jax.sharding import Mesh
from jax.sharding import PartitionSpec as P

MESH = pl.DeviceIdType.MESH
SPACE = ("y", "z")
ROWS_Y = 8
STEP = 2.0
ROOT_SIX = math.sqrt(6.0)
NODE_TIMES = [(4.0 - ROOT_SIX) / 10.0, (4.0 + ROOT_SIX) / 10.0, 1.0]
COLLOC = [
    [
        (88.0 - 7.0 * ROOT_SIX) / 360.0,
        (296.0 - 169.0 * ROOT_SIX) / 1800.0,
        (-2.0 + 3.0 * ROOT_SIX) / 225.0,
    ],
    [
        (296.0 + 169.0 * ROOT_SIX) / 1800.0,
        (88.0 + 7.0 * ROOT_SIX) / 360.0,
        (-2.0 - 3.0 * ROOT_SIX) / 225.0,
    ],
    [(16.0 - ROOT_SIX) / 36.0, (16.0 + ROOT_SIX) / 36.0, 1.0 / 9.0],
]
WEIGHT = [
    [STEP * (COLLOC[m][j] - (COLLOC[m - 1][j] if m else 0.0)) for j in range(3)] for m in range(3)
]
WIDTH = [STEP * (NODE_TIMES[m] - (NODE_TIMES[m - 1] if m else 0.0)) for m in range(3)]
PAD = 8
BLOCK = 32
CHUNKS = 8

PADDED = ["k", "u0", "u1", "u2", "a", "b", "d", "la", "v2", "v3", "vc"]
PLANES = ["s", "wxm", "wxp", "wym", "wyp", "wzm", "wzp", "dg", "lb", "ld", "lla", "lv2"]
PLANES += ["r2", "r3", "rc", "hv3", "hvc", "xu", "xrc", "xvc", "xr3", "xv3"]
SIDES = ["k", "u0", "u1", "u2", "a", "b", "d", "la", "v2"]


def kernel(dims, start_hbm, old_hbm, kappa_hbm, fine, following, coarse_next, padded, planes, sides,
           tiles, ztiles, zslots, yslots, xslots, send, recv, gsend, grecv, local, words):
    nt, ny, nz, rows, cols = dims
    chunk = rows // CHUNKS
    half = CHUNKS // 2
    each = range(CHUNKS)
    order = [i // 2 + (i % 2) * half for i in each]
    me_t, me_y, me_z = lax.axis_index("tm"), lax.axis_index("y"), lax.axis_index("z")
    place = me_y * nz + me_z
    slabs = ny * nz

    def chain(shift):
        other = lax.rem(place + (slabs + shift), slabs)
        return (me_t, lax.div(other, nz), lax.rem(other, nz))

    after, before = chain(1), chain(-1)
    next_t = lax.rem(me_t + 1, nt)
    last_t = lax.rem(me_t + (nt - 1), nt)

    def z_peer(k):
        return (me_t, me_y, lax.rem(me_z + k, nz))

    def y_peer(k, t=me_t):
        return (t, lax.rem(me_y + k, ny), me_z)

    def t_peer(k):
        return (lax.rem(me_t + k, nt), me_y, me_z)

    pad = {name: padded.at[i] for i, name in enumerate(PADDED)}
    plane = {name: planes.at[i] for i, name in enumerate(PLANES)}
    side = {name: sides.at[i] for i, name in enumerate(SIDES)}

    def inner(name, first=0, count=rows):
        return pad[name].at[pl.ds(PAD + first, count), :]

    loads = [(kappa_hbm, "k"), (old_hbm.at[0], "u0"), (old_hbm.at[1], "u1"), (old_hbm.at[2], "u2")]
    copies = [pltpu.make_async_copy(src, inner(name), local.at[i]) for i, (src, name) in enumerate(loads)]
    copies.append(pltpu.make_async_copy(start_hbm, plane["s"], local.at[4]))
    for copy in copies:
        copy.start()
    barrier = pltpu.get_barrier_semaphore()
    greeted = [after, before]
    greeted += [z_peer(k) for k in (1, nz - 1)]
    greeted += [y_peer(k) for k in (1, ny - 1)]
    greeted += [t_peer(k) for k in (1, nt - 1)]
    for device in greeted:
        pl.semaphore_signal(barrier, inc=1, device_id=device, device_id_type=MESH)
    pl.semaphore_wait(barrier, len(greeted))

    def ring_peers(k):
        return [
            peer(shift % size)
            for peer, size in ((z_peer, nz), (y_peer, ny), (t_peer, nt))
            for shift in (k, size - k)
        ]

    def tell(n, devices):
        for device in devices:
            pl.semaphore_signal(words.at[n], inc=1, device_id=device, device_id_type=MESH)

    nearest, second = ring_peers(1), ring_peers(2)
    third = [z_peer(2), z_peer(nz - 2), t_peer(1), t_peer(nt - 1)]

    taken = []

    def put(src, dst, device, group, slot):
        pltpu.make_async_remote_copy(
            src_ref=src, dst_ref=dst, send_sem=send.at[group], recv_sem=recv.at[slot],
            device_id=device, device_id_type=MESH,
        ).start()

    def expect(region, group, slot):
        return pltpu.make_async_remote_copy(
            src_ref=region, dst_ref=region, send_sem=send.at[group], recv_sem=recv.at[slot],
            device_id=after, device_id_type=MESH,
        )

    def fresh_slot():
        taken.append(0)
        return len(taken) - 1

    def swap_all(names, c):
        slot = fresh_slot()
        there = pl.ds(c * chunk, chunk)
        for name in names:
            here = inner(name, c * chunk, chunk)
            put(here, side[name].at[0, there, :], after, 0, slot)
            put(here, side[name].at[1, there, :], before, 0, slot)
        first = SIDES.index(names[0])
        return expect(sides.at[pl.ds(first, len(names)), :, there, :], 0, slot)

    def swap(name, c):
        return swap_all([name], c)

    def swap_half(name, i, second):
        slot = fresh_slot()
        for c, up in ((i, not second), (i + half, second)):
            there = pl.ds(c * chunk, chunk)
            dst = side[name].at[0 if up else 1, there, :]
            put(inner(name, c * chunk, chunk), dst, after if up else before, 0, slot)
        return expect(side[name].at[:, pl.ds(0, chunk), :], 0, slot)

    def give_half(name, i):
        slot = fresh_slot()
        for c, up in ((i, True), (i + half, False)):
            dst = plane["h" + name].at[pl.ds(c * chunk, chunk), :]
            put(inner(name, c * chunk, chunk), dst, after if up else before, 1, slot)
        return expect(side["v2"].at[:, pl.ds(0, chunk), :], 1, slot)

    next_device = (next_t, me_y, me_z)
    early, late = fresh_slot(), fresh_slot()

    def onward(src, name, c, slot):
        put(src, plane[name].at[pl.ds(c * chunk, chunk), :], next_device, 2, slot)

    def arrive(waiter):
        waiter.wait_recv()

    givers = nt // 2
    share = rows // givers
    own = pl.multiple_of(lax.div(me_t, 2) * share, share)
    mine = pl.ds(own, share)
    gives = lax.rem(me_t, 2) == 1
    k_slot = fresh_slot()
    k_in = expect(side["k"].at[:, mine, :], 3, k_slot)
    copies[0].wait()

    @pl.when(gives)
    def _():
        k_src = pad["k"].at[pl.ds(pl.multiple_of(PAD + own, PAD), share), :]
        put(k_src, side["k"].at[0, mine, :], after, 3, k_slot)
        put(k_src, side["k"].at[1, mine, :], before, 3, k_slot)

    for copy in copies[1:4]:
        copy.wait()
    u_in = [swap_all(["u0", "u1", "u2"], c) for c in each]
    put(inner("u2"), plane["xu"], next_device, 2, early)
    tell(0, nearest)
    edge = jnp.zeros((PAD, cols), jnp.float32)
    for name in PADDED:
        pad[name][pl.ds(0, PAD), :] = edge
        pad[name][pl.ds(PAD + rows, PAD), :] = edge
    copies[4].wait()
    pl.semaphore_wait(words.at[0], len(nearest))
    tell(1, second)
    pl.semaphore_wait(words.at[1], len(second))
    tell(2, third)

    def spread(region):
        return pltpu.make_async_remote_copy(
            src_ref=region, dst_ref=region, send_sem=gsend.at[0], recv_sem=grecv.at[0],
            device_id=after, device_id_type=MESH,
        )

    @pl.when(gives)
    def _():
        arrive(k_in)
        for s in range(2):
            block = side["k"].at[s, mine, :]
            for k in range(1, nt):
                pltpu.make_async_remote_copy(
                    src_ref=block, dst_ref=block, send_sem=gsend.at[0], recv_sem=grecv.at[0],
                    device_id=t_peer(k), device_id_type=MESH,
                ).start()
        if givers > 1:
            spread(side["k"].at[:, pl.ds(0, share * (givers - 1)), :]).wait_recv()

    @pl.when(jnp.logical_not(gives))
    def _():
        spread(side["k"]).wait_recv()

    pl.semaphore_wait(words.at[2], len(third))
    lane = lax.broadcasted_iota(jnp.int32, (BLOCK, cols), 1)
    first_lane, last_lane = lane == 0, lane == cols - 1
    zero = jnp.zeros((BLOCK, cols), jnp.float32)

    def to_right(x):
        return pltpu.roll(x, cols - 1, 1)

    def to_left(x):
        return pltpu.roll(x, 1, 1)

    def at(r):
        return pl.ds(r, BLOCK)

    def column(name, r):
        x = pad[name][pl.ds(r, BLOCK + 2 * PAD), :]
        return x[PAD:PAD + BLOCK], x[PAD - 1:PAD + BLOCK - 1], x[PAD + 1:PAD + BLOCK + 1]

    def sweep(first, count, body, carry):
        def step(i, carry):
            return body(pl.multiple_of(first + i * BLOCK, BLOCK), carry)

        return lax.fori_loop(0, count // BLOCK, step, carry)

    def weights(r, carry):
        k, k_down, k_up = column("k", r)
        row = lax.broadcasted_iota(jnp.int32, (BLOCK, cols), 0) + r
        k_before = jnp.where(place == 0, zero, side["k"][0, at(r), :])
        k_after = jnp.where(place == slabs - 1, zero, side["k"][1, at(r), :])
        faces = [
            0.5 * (k + k_before),
            0.5 * (k + k_after),
            0.5 * (k + k_down),
            0.5 * (k + k_up),
            0.5 * (k + jnp.where(first_lane, zero, to_left(k))),
            0.5 * (k + jnp.where(last_lane, zero, to_right(k))),
        ]
        total = faces[1] + faces[0] + faces[3] + faces[2] + faces[5] + faces[4]
        plane["dg"][at(r), :] = -total
        plane["wxm"][at(r), :] = jnp.where(place == 0, zero, faces[0])
        plane["wxp"][at(r), :] = jnp.where(place == slabs - 1, zero, faces[1])
        plane["wym"][at(r), :] = jnp.where(row == 0, zero, faces[2])
        plane["wyp"][at(r), :] = jnp.where(row == rows - 1, zero, faces[3])
        plane["wzm"][at(r), :] = jnp.where(first_lane, zero, faces[4])
        plane["wzp"][at(r), :] = jnp.where(last_lane, zero, faces[5])
        return carry

    sweep(0, rows, weights, 0)

    def heat(name, r):
        mid, down, up = column(name, r)
        out = plane["wxp"][at(r), :] * side[name][1, at(r), :]
        out = out + plane["wxm"][at(r), :] * side[name][0, at(r), :]
        out = out + plane["wyp"][at(r), :] * up + plane["wym"][at(r), :] * down
        out = out + plane["wzp"][at(r), :] * to_right(mid) + plane["wzm"][at(r), :] * to_left(mid)
        return mid, out + plane["dg"][at(r), :] * mid

    def fold(x):
        return jnp.sum(x.reshape(BLOCK // 8, 8, cols), axis=0)

    nothing = jnp.zeros((8, cols), jnp.float32)

    def quadratic(name, beside, weight, r):
        mid, _, up = column(name, r)
        twice = plane[weight][at(r), :] * beside[at(r), :]
        twice = twice + plane["wyp"][at(r), :] * up + plane["wzp"][at(r), :] * to_right(mid)
        return fold(mid * (twice + twice + plane["dg"][at(r), :] * mid))

    def moments(name, beside, c):
        weight = "wxm" if c < CHUNKS // 2 else "wxp"
        beside = beside(0 if c < CHUNKS // 2 else 1)
        return sweep(c * chunk, chunk, lambda r, acc: acc + quadratic(name, beside, weight, r), nothing)

    spot = lax.broadcasted_iota(jnp.int32, (1, 128), 1)

    def lanes(acc):
        both = acc[:, 0:128]
        for i in range(1, cols // 128):
            both = both + acc[:, i * 128:(i + 1) * 128]
        return jnp.sum(both, axis=0, keepdims=True)

    def burst(src, slots, devices, sem):
        middle = (len(devices) - 1) / 2
        for k in sorted(range(len(devices)), key=lambda k: abs(k - middle)):
            pltpu.make_async_remote_copy(
                src_ref=src, dst_ref=slots.at[pl.ds(k, 1), :],
                send_sem=gsend.at[sem], recv_sem=grecv.at[sem],
                device_id=devices[k], device_id_type=MESH,
            ).start()
        whole = slots.at[pl.ds(0, len(devices)), :]
        return pltpu.make_async_remote_copy(
            src_ref=whole, dst_ref=whole, send_sem=gsend.at[sem], recv_sem=grecv.at[sem],
            device_id=after, device_id_type=MESH,
        )

    bursts = []

    def reduce_z(n, accs):
        rows_of = jnp.concatenate([lanes(acc) for acc in accs + [nothing] * (8 - len(accs))], axis=0)
        sums = jnp.sum(rows_of, axis=1, keepdims=True)
        row = jnp.zeros((1, 128), jnp.float32)
        for q in range(len(accs)):
            row = jnp.where(spot == q, sums[q:q + 1, :], row)
        tiles[n, 0:1, :] = row
        devices = [z_peer(k) for k in range(1, nz)]
        waits = burst(tiles.at[n, pl.ds(0, 1), :], zslots.at[n], devices, 1 + 3 * n)
        bursts.append(waits)
        return waits

    def reduce_y(n, waits, also=False):
        waits.wait_recv()
        ztiles[n, 0:1, :] = tiles[n, 0:1, :] + jnp.sum(zslots[n, 0:nz - 1, :], axis=0, keepdims=True)
        src = ztiles.at[n, pl.ds(0, 1), :]
        out = [burst(src, yslots.at[n], [y_peer(k) for k in range(1, ny)], 2 + 3 * n)]
        if also:
            out.append(burst(src, xslots, [y_peer(k, next_t) for k in range(ny)], 3 + 3 * n))
        bursts.extend(out)
        return out

    def total_own(n, waits):
        waits.wait_recv()
        return ztiles[n, 0:1, :] + jnp.sum(yslots[n, 0:ny - 1, :], axis=0, keepdims=True)

    def total_last(waits):
        waits.wait_recv()
        return jnp.sum(xslots[0:ny, :], axis=0, keepdims=True)

    def factors(row, h):
        s0, s1, s2, s3 = row, pltpu.roll(row, 127, 1), pltpu.roll(row, 126, 1), pltpu.roll(row, 125, 1)
        sigma = s1 / s0
        spread = jnp.maximum(s2 - s1 * sigma, 1e-30)
        bent = s3 - sigma * (s2 + s2) + sigma * sigma * s1
        one = s0 / (s0 - h * s1)
        part = spread / s0
        two = 1.0 / jnp.maximum(1.0 - h * bent / spread - one * (h * h) * part, 1.0)
        slope = (one * h) * (one * h) * part
        c1 = one * two * h
        c0 = one + two * slope - c1 * sigma
        return c0, c1

    def whole(x):
        return jnp.concatenate([jnp.broadcast_to(x, (8, cols))] * (BLOCK // 8), axis=0)

    def first_fields(r, carry):
        mids, images = zip(*[heat("u%d" % j, r) for j in range(3)])
        begin = plane["s"][at(r), :]
        leads = [begin - mids[0], mids[0] - mids[1], mids[1] - mids[2]]
        rc = None
        for m, name in enumerate(["a", "b", "d"]):
            value = leads[m]
            for j in range(3):
                value = value + WEIGHT[m][j] * images[j]
            pad[name][pl.ds(PAD + r, BLOCK), :] = value
            rc = value if rc is None else rc + value
        plane["rc"][at(r), :] = rc
        return carry

    a_in, b_in, d_in, la_in = {}, {}, {}, {}
    for c in each:
        arrive(u_in[c])
        sweep(c * chunk, chunk, first_fields, 0)
        a_in[c] = swap("a", c)
    put(plane["rc"], plane["xrc"], next_device, 2, early)

    def first_heat(r, carry):
        s0, s1, s2 = carry
        mid, out = heat("a", r)
        pad["la"][pl.ds(PAD + r, BLOCK), :] = out
        return s0 + fold(mid * mid), s1 + fold(mid * out), s2 + fold(out * out)

    sums = (nothing,) * 3
    for c in each:
        arrive(a_in[c])
        sums = sweep(c * chunk, chunk, first_heat, sums)
        la_in[c] = swap("la", c)
    for c in each[:3]:
        b_in[c] = swap("b", c)

    def second_field(r, carry):
        plane["lb"][at(r), :] = heat("b", r)[1]
        return carry

    def take_b(chunks):
        for c in chunks:
            arrive(b_in[c])
            sweep(c * chunk, chunk, second_field, 0)

    def second_heat(r, carry):
        mid, out = heat("la", r)
        plane["lla"][at(r), :] = out
        return carry + fold(mid * out)

    s3 = nothing
    for c in each:
        arrive(la_in[c])
        s3 = sweep(c * chunk, chunk, second_heat, s3)
    z_wait = reduce_z(0, list(sums) + [s3])
    for c in each[3:]:
        b_in[c] = swap("b", c)
    for c in order[:4]:
        d_in[c] = swap("d", c)

    def third_field(r, carry):
        s0, s1, s2 = carry
        ld = heat("d", r)[1]
        rc = plane["rc"][at(r), :]
        vc = pad["la"][pl.ds(PAD + r, BLOCK), :] + plane["lb"][at(r), :] + ld
        plane["ld"][at(r), :] = ld
        pad["vc"][pl.ds(PAD + r, BLOCK), :] = vc
        return s0 + fold(rc * rc), s1 + fold(rc * vc), s2 + fold(vc * vc)

    coarse = (nothing,) * 3
    vc_in = {}

    def take_d(chunks, coarse):
        for c in chunks:
            arrive(d_in[c])
            coarse = sweep(c * chunk, chunk, third_field, coarse)
            onward(inner("vc", c * chunk, chunk), "xvc", c, early)
            if c >= half:
                vc_in[c - half] = give_half("vc", c - half)
        return coarse

    take_b(each[:4])
    (y_wait,) = reduce_y(0, z_wait)
    take_b(each[4:])
    c0, c1 = [whole(x[:, 0:1]) for x in factors(total_own(0, y_wait), WIDTH[0])]

    def second_node(r, carry):
        s0, s1, s2 = carry
        at_pad = pl.ds(PAD + r, BLOCK)
        a, la, lla = pad["a"][at_pad, :], pad["la"][at_pad, :], plane["lla"][at(r), :]
        move = c0 * a + c1 * la
        fine[0, at(r), :] = pad["u0"][at_pad, :] + move
        r2 = pad["b"][at_pad, :] + move
        v2 = plane["lb"][at(r), :] + c0 * la + c1 * lla
        plane["r2"][at(r), :] = r2
        pad["v2"][at_pad, :] = v2
        return s0 + fold(r2 * r2), s1 + fold(r2 * v2), s2 + fold(v2 * v2)

    sums = (nothing,) * 3
    v_in, w_in = {}, {}
    for c in order:
        sums = sweep(c * chunk, chunk, second_node, sums)
        if c >= half:
            v_in[c - half] = swap_half("v2", c - half, False)
    coarse = take_d(order[:4], coarse)
    w_in[0] = swap_half("v2", 0, True)
    s3 = nothing
    for i in range(half):
        arrive(v_in[i])
        for c in (i, i + half):
            s3 = s3 + moments("v2", lambda s: side["v2"].at[s], c)
    z_wait = reduce_z(1, list(sums) + [s3])
    for i in range(1, half):
        w_in[i] = swap_half("v2", i, True)
    for c in order[4:]:
        d_in[c] = swap("d", c)

    def third_heat(r, carry):
        plane["lv2"][at(r), :] = heat("v2", r)[1]
        return carry

    def take_w(pairs):
        for i in pairs:
            arrive(w_in[i])
            for c in (i, i + half):
                sweep(c * chunk, chunk, third_heat, 0)

    take_w(range(2))
    (y_wait,) = reduce_y(1, z_wait)
    take_w(range(2, half))
    coarse = take_d(order[4:6], coarse)
    e0, e1 = [whole(x[:, 0:1]) for x in factors(total_own(1, y_wait), WIDTH[1])]

    def third_node(r, carry):
        s0, s1, s2 = carry
        at_pad = pl.ds(PAD + r, BLOCK)
        r2, v2, lv2 = plane["r2"][at(r), :], pad["v2"][at_pad, :], plane["lv2"][at(r), :]
        move = e0 * r2 + e1 * v2
        fine[1, at(r), :] = pad["u1"][at_pad, :] + move
        r3 = pad["d"][at_pad, :] + move
        v3 = plane["ld"][at(r), :] + e0 * v2 + e1 * lv2
        plane["r3"][at(r), :] = r3
        pad["v3"][at_pad, :] = v3
        return s0 + fold(r3 * r3), s1 + fold(r3 * v3), s2 + fold(v3 * v3)

    sums = (nothing,) * 3
    v3_in = {}

    def take_node(chunks, sums):
        for c in chunks:
            sums = sweep(c * chunk, chunk, third_node, sums)
            if c >= half:
                v3_in[c - half] = give_half("v3", c - half)
            onward(plane["r3"].at[pl.ds(c * chunk, chunk), :], "xr3", c, late)
            onward(inner("v3", c * chunk, chunk), "xv3", c, late)
        return sums

    sums = take_node(order[:4], sums)
    coarse = take_d(order[6:], coarse)
    sums = take_node(order[4:], sums)
    coarse3, s3 = nothing, nothing
    for i in range(half):
        arrive(vc_in[i])
        for c in (i, i + half):
            coarse3 = coarse3 + moments("vc", lambda s: plane["hvc"], c)
    for i in range(half):
        arrive(v3_in[i])
        for c in (i, i + half):
            s3 = s3 + moments("v3", lambda s: plane["hv3"], c)
    z_wait = reduce_z(2, list(sums) + [s3] + list(coarse) + [coarse3])
    expect(planes.at[pl.ds(0, 3)], 2, early).wait_recv()

    def first_slice(r, carry):
        plane["xu"][at(r), :] = jnp.where(me_t == 0, plane["s"][at(r), :], plane["xu"][at(r), :])
        return carry

    sweep(0, rows, first_slice, 0)
    y_wait, x_wait = reduce_y(2, z_wait, also=True)
    expect(planes.at[pl.ds(0, 2)], 2, late).wait_recv()
    expect(sides.at[pl.ds(1, len(SIDES) - 1)], 0, 0).wait_send()
    expect(planes.at[pl.ds(0, 2)], 1, 0).wait_send()
    expect(planes.at[pl.ds(0, 5)], 2, 0).wait_send()

    @pl.when(gives)
    def _():
        k_in.wait_send()
        spread(sides.at[pl.ds(0, 2), :, pl.ds(0, share * (nt - 1) // 2), :]).wait_send()

    for waits in bursts[:-2]:
        waits.wait_send()
    both = jnp.concatenate([total_own(2, y_wait), total_last(x_wait)], axis=0)
    width = jnp.where(lax.broadcasted_iota(jnp.int32, (2, 128), 1) == 4, STEP, WIDTH[2])
    f0, f1 = factors(both, width)
    g0, g1 = whole(f0[0:1, 0:1]), whole(f1[0:1, 0:1])
    passed = [x[1:2, q:q + 1] for q in (0, 4) for x in (f0, f1)]
    p0, p1, q0, q1 = [whole(jnp.where(me_t == 0, 0.0, x)) for x in passed]

    def last_node(r, carry):
        at_pad = pl.ds(PAD + r, BLOCK)
        fine[2, at(r), :] = pad["u2"][at_pad, :] + (g0 * plane["r3"][at(r), :] + g1 * pad["v3"][at_pad, :])
        guess = plane["xu"][at(r), :]
        following[at(r), :] = guess + (p0 * plane["xr3"][at(r), :] + p1 * plane["xv3"][at(r), :])
        coarse_next[at(r), :] = guess + (q0 * plane["xrc"][at(r), :] + q1 * plane["xvc"][at(r), :])
        return carry

    sweep(0, rows, last_node, 0)
    for waits in bursts[-2:]:
        waits.wait_send()


def slots_needed():
    return 1 + 2 + 5 * CHUNKS + 4 * (CHUNKS // 2)


def leave(fine, following, coarse, fine_hbm, following_hbm, coarse_hbm, sem):
    rows = following.shape[0] // 2
    pairs = [(fine.at[m], fine_hbm.at[m]) for m in range(3)]
    pairs += [(following, following_hbm), (coarse, coarse_hbm)]
    copies = []
    for src, dst in pairs:
        for first in (0, rows):
            part = pl.ds(first, rows)
            copies.append(
                pltpu.make_async_copy(src.at[part, :], dst.at[part, :], sem.at[len(copies)])
            )
    for copy in copies:
        copy.start()
    for copy in copies:
        copy.wait()


def on_device(dims, start_value, old_nodes, diffusivity):
    nt, ny, nz, rows, cols = dims
    anywhere = pl.BlockSpec(memory_space=pl.ANY)
    near = pl.BlockSpec(memory_space=pltpu.VMEM)
    plane = jax.ShapeDtypeStruct((rows, cols), jnp.float32)
    inputs = [
        pltpu.with_memory_space_constraint(value, pltpu.MemorySpace.HBM)
        for value in (
            start_value.reshape(rows, cols),
            old_nodes.reshape(3, rows, cols),
            diffusivity.reshape(rows, cols),
        )
    ]
    fine, following, coarse = pl.pallas_call(
        functools.partial(kernel, dims),
        out_shape=(jax.ShapeDtypeStruct((3, rows, cols), jnp.float32), plane, plane),
        in_specs=[anywhere] * 3,
        out_specs=(near,) * 3,
        scratch_shapes=[
            pltpu.VMEM((len(PADDED), rows + 2 * PAD, cols), jnp.float32),
            pltpu.VMEM((len(PLANES), rows, cols), jnp.float32),
            pltpu.VMEM((len(SIDES), 2, rows, cols), jnp.float32),
            pltpu.VMEM((3, 8, 128), jnp.float32),
            pltpu.VMEM((3, 8, 128), jnp.float32),
            pltpu.VMEM((3, 16, 128), jnp.float32),
            pltpu.VMEM((3, 8, 128), jnp.float32),
            pltpu.VMEM((8, 128), jnp.float32),
            pltpu.SemaphoreType.DMA((4,)),
            pltpu.SemaphoreType.DMA((slots_needed(),)),
            pltpu.SemaphoreType.DMA((10,)),
            pltpu.SemaphoreType.DMA((10,)),
            pltpu.SemaphoreType.DMA((5,)),
            pltpu.SemaphoreType.REGULAR((3,)),
        ],
        compiler_params=pltpu.CompilerParams(
            collective_id=0, has_side_effects=True, vmem_limit_bytes=40 * 1024 * 1024
        ),
    )(*inputs)
    fine, following, coarse = pl.pallas_call(
        leave,
        out_shape=(jax.ShapeDtypeStruct((3, rows, cols), jnp.float32), plane, plane),
        in_specs=[anywhere] * 3,
        out_specs=(anywhere,) * 3,
        scratch_shapes=[pltpu.SemaphoreType.DMA((10,))],
        compiler_params=pltpu.CompilerParams(vmem_limit_bytes=40 * 1024 * 1024),
    )(fine, following, coarse)
    return (
        fine.reshape(1, 3, 1, rows, cols),
        following.reshape(1, 1, rows, cols),
        coarse.reshape(1, 1, rows, cols),
    )


def build(split, rows, cols):
    dims = (split.shape["tm"], split.shape["y"], split.shape["z"], rows, cols)
    in_specs = (P("tm", SPACE, None, None), P("tm", None, SPACE, None, None), P(SPACE, None, None))
    out_specs = (
        P("tm", None, SPACE, None, None),
        P("tm", SPACE, None, None),
        P("tm", SPACE, None, None),
    )
    return jax.shard_map(
        functools.partial(on_device, dims), mesh=split, in_specs=in_specs, out_specs=out_specs,
        check_vma=False,
    )


def solution(mesh):
    split = Mesh(
        mesh.devices.reshape(mesh.shape["tm"], ROWS_Y, mesh.shape["space"] // ROWS_Y), ("tm",) + SPACE
    )
    return build(split, 512, 256)
```

```python
import functools
import math

import jax
import jax.numpy as jnp
from jax import lax
from jax.experimental import pallas as pl
from jax.experimental.pallas import tpu as pltpu
from jax.sharding import Mesh
from jax.sharding import PartitionSpec as P

MESH = pl.DeviceIdType.MESH
SPACE = ("y", "z")
ROWS_Y = 8
STEP = 2.0
ROOT_SIX = math.sqrt(6.0)
NODE_TIMES = [(4.0 - ROOT_SIX) / 10.0, (4.0 + ROOT_SIX) / 10.0, 1.0]
COLLOC = [
    [
        (88.0 - 7.0 * ROOT_SIX) / 360.0,
        (296.0 - 169.0 * ROOT_SIX) / 1800.0,
        (-2.0 + 3.0 * ROOT_SIX) / 225.0,
    ],
    [
        (296.0 + 169.0 * ROOT_SIX) / 1800.0,
        (88.0 + 7.0 * ROOT_SIX) / 360.0,
        (-2.0 - 3.0 * ROOT_SIX) / 225.0,
    ],
    [(16.0 - ROOT_SIX) / 36.0, (16.0 + ROOT_SIX) / 36.0, 1.0 / 9.0],
]
WEIGHT = [
    [STEP * (COLLOC[m][j] - (COLLOC[m - 1][j] if m else 0.0)) for j in range(3)] for m in range(3)
]
WIDTH = [STEP * (NODE_TIMES[m] - (NODE_TIMES[m - 1] if m else 0.0)) for m in range(3)]
PAD = 8
BLOCK = 32
CHUNKS = 8

PADDED = ["k", "u0", "u1", "u2", "a", "b", "d", "la", "v2", "v3", "vc"]
PLANES = ["s", "wxm", "wxp", "wym", "wyp", "wzm", "wzp", "dg", "lb", "ld", "lla", "lv2"]
PLANES += ["r2", "r3", "rc", "hv3", "hvc", "xu", "xrc", "xvc", "xr3", "xv3"]
SIDES = ["k", "u0", "u1", "u2", "a", "b", "d", "la", "v2"]


def kernel(dims, start_hbm, old_hbm, kappa_hbm, fine, following, coarse_next, padded, planes, sides,
           tiles, ztiles, zslots, yslots, xslots, send, recv, gsend, grecv, local, words):
    nt, ny, nz, rows, cols = dims
    chunk = rows // CHUNKS
    half = CHUNKS // 2
    each = range(CHUNKS)
    order = [i // 2 + (i % 2) * half for i in each]
    me_t, me_y, me_z = lax.axis_index("tm"), lax.axis_index("y"), lax.axis_index("z")
    place = me_y * nz + me_z
    slabs = ny * nz

    def chain(shift):
        other = lax.rem(place + (slabs + shift), slabs)
        return (me_t, lax.div(other, nz), lax.rem(other, nz))

    after, before = chain(1), chain(-1)
    next_t = lax.rem(me_t + 1, nt)
    last_t = lax.rem(me_t + (nt - 1), nt)

    def z_peer(k):
        return (me_t, me_y, lax.rem(me_z + k, nz))

    def y_peer(k, t=me_t):
        return (t, lax.rem(me_y + k, ny), me_z)

    def t_peer(k):
        return (lax.rem(me_t + k, nt), me_y, me_z)

    pad = {name: padded.at[i] for i, name in enumerate(PADDED)}
    plane = {name: planes.at[i] for i, name in enumerate(PLANES)}
    side = {name: sides.at[i] for i, name in enumerate(SIDES)}

    def inner(name, first=0, count=rows):
        return pad[name].at[pl.ds(PAD + first, count), :]

    loads = [(kappa_hbm, "k"), (old_hbm.at[0], "u0"), (old_hbm.at[1], "u1"), (old_hbm.at[2], "u2")]
    copies = [pltpu.make_async_copy(src, inner(name), local.at[i]) for i, (src, name) in enumerate(loads)]
    copies.append(pltpu.make_async_copy(start_hbm, plane["s"], local.at[4]))
    for copy in copies:
        copy.start()
    barrier = pltpu.get_barrier_semaphore()
    greeted = [after, before]
    greeted += [z_peer(k) for k in (1, nz - 1)]
    greeted += [y_peer(k) for k in (1, ny - 1)]
    greeted += [t_peer(k) for k in (1, nt - 1)]
    for device in greeted:
        pl.semaphore_signal(barrier, inc=1, device_id=device, device_id_type=MESH)
    pl.semaphore_wait(barrier, len(greeted))

    def ring_peers(k):
        return [
            peer(shift % size)
            for peer, size in ((z_peer, nz), (y_peer, ny), (t_peer, nt))
            for shift in (k, size - k)
        ]

    def tell(n, devices):
        for device in devices:
            pl.semaphore_signal(words.at[n], inc=1, device_id=device, device_id_type=MESH)

    nearest, second = ring_peers(1), ring_peers(2)
    third = [z_peer(2), z_peer(nz - 2), t_peer(1), t_peer(nt - 1)]

    taken = []

    def put(src, dst, device, group, slot):
        pltpu.make_async_remote_copy(
            src_ref=src, dst_ref=dst, send_sem=send.at[group], recv_sem=recv.at[slot],
            device_id=device, device_id_type=MESH,
        ).start()

    def expect(region, group, slot):
        return pltpu.make_async_remote_copy(
            src_ref=region, dst_ref=region, send_sem=send.at[group], recv_sem=recv.at[slot],
            device_id=after, device_id_type=MESH,
        )

    def fresh_slot():
        taken.append(0)
        return len(taken) - 1

    def swap_all(names, c):
        slot = fresh_slot()
        there = pl.ds(c * chunk, chunk)
        for name in names:
            here = inner(name, c * chunk, chunk)
            put(here, side[name].at[0, there, :], after, 0, slot)
            put(here, side[name].at[1, there, :], before, 0, slot)
        first = SIDES.index(names[0])
        return expect(sides.at[pl.ds(first, len(names)), :, there, :], 0, slot)

    def swap(name, c):
        return swap_all([name], c)

    def swap_half(name, i, second):
        slot = fresh_slot()
        for c, up in ((i, not second), (i + half, second)):
            there = pl.ds(c * chunk, chunk)
            dst = side[name].at[0 if up else 1, there, :]
            put(inner(name, c * chunk, chunk), dst, after if up else before, 0, slot)
        return expect(side[name].at[:, pl.ds(0, chunk), :], 0, slot)

    def give_half(name, i):
        slot = fresh_slot()
        for c, up in ((i, True), (i + half, False)):
            dst = plane["h" + name].at[pl.ds(c * chunk, chunk), :]
            put(inner(name, c * chunk, chunk), dst, after if up else before, 1, slot)
        return expect(side["v2"].at[:, pl.ds(0, chunk), :], 1, slot)

    next_device = (next_t, me_y, me_z)
    early, late = fresh_slot(), fresh_slot()

    def onward(src, name, c, slot):
        put(src, plane[name].at[pl.ds(c * chunk, chunk), :], next_device, 2, slot)

    def arrive(waiter):
        waiter.wait_recv()

    givers = nt // 2
    share = rows // givers
    own = pl.multiple_of(lax.div(me_t, 2) * share, share)
    mine = pl.ds(own, share)
    gives = lax.rem(me_t, 2) == 1
    k_slot = fresh_slot()
    k_in = expect(side["k"].at[:, mine, :], 3, k_slot)
    copies[0].wait()

    @pl.when(gives)
    def _():
        k_src = pad["k"].at[pl.ds(pl.multiple_of(PAD + own, PAD), share), :]
        put(k_src, side["k"].at[0, mine, :], after, 3, k_slot)
        put(k_src, side["k"].at[1, mine, :], before, 3, k_slot)

    for copy in copies[1:4]:
        copy.wait()
    u_in = [swap_all(["u0", "u1", "u2"], c) for c in each]
    put(inner("u2"), plane["xu"], next_device, 2, early)
    tell(0, nearest)
    edge = jnp.zeros((PAD, cols), jnp.float32)
    for name in PADDED:
        pad[name][pl.ds(0, PAD), :] = edge
        pad[name][pl.ds(PAD + rows, PAD), :] = edge
    copies[4].wait()
    pl.semaphore_wait(words.at[0], len(nearest))
    tell(1, second)
    pl.semaphore_wait(words.at[1], len(second))
    tell(2, third)

    def spread(region):
        return pltpu.make_async_remote_copy(
            src_ref=region, dst_ref=region, send_sem=gsend.at[0], recv_sem=grecv.at[0],
            device_id=after, device_id_type=MESH,
        )

    @pl.when(gives)
    def _():
        arrive(k_in)
        for s in range(2):
            block = side["k"].at[s, mine, :]
            for k in range(1, nt):
                pltpu.make_async_remote_copy(
                    src_ref=block, dst_ref=block, send_sem=gsend.at[0], recv_sem=grecv.at[0],
                    device_id=t_peer(k), device_id_type=MESH,
                ).start()
        if givers > 1:
            spread(side["k"].at[:, pl.ds(0, share * (givers - 1)), :]).wait_recv()

    @pl.when(jnp.logical_not(gives))
    def _():
        spread(side["k"]).wait_recv()

    pl.semaphore_wait(words.at[2], len(third))
    lane = lax.broadcasted_iota(jnp.int32, (BLOCK, cols), 1)
    first_lane, last_lane = lane == 0, lane == cols - 1
    zero = jnp.zeros((BLOCK, cols), jnp.float32)

    def to_right(x):
        return pltpu.roll(x, cols - 1, 1)

    def to_left(x):
        return pltpu.roll(x, 1, 1)

    def at(r):
        return pl.ds(r, BLOCK)

    def column(name, r):
        x = pad[name][pl.ds(r, BLOCK + 2 * PAD), :]
        return x[PAD:PAD + BLOCK], x[PAD - 1:PAD + BLOCK - 1], x[PAD + 1:PAD + BLOCK + 1]

    def sweep(first, count, body, carry):
        def step(i, carry):
            return body(pl.multiple_of(first + i * BLOCK, BLOCK), carry)

        return lax.fori_loop(0, count // BLOCK, step, carry)

    def weights(r, carry):
        k, k_down, k_up = column("k", r)
        row = lax.broadcasted_iota(jnp.int32, (BLOCK, cols), 0) + r
        k_before = jnp.where(place == 0, zero, side["k"][0, at(r), :])
        k_after = jnp.where(place == slabs - 1, zero, side["k"][1, at(r), :])
        faces = [
            0.5 * (k + k_before),
            0.5 * (k + k_after),
            0.5 * (k + k_down),
            0.5 * (k + k_up),
            0.5 * (k + jnp.where(first_lane, zero, to_left(k))),
            0.5 * (k + jnp.where(last_lane, zero, to_right(k))),
        ]
        total = faces[1] + faces[0] + faces[3] + faces[2] + faces[5] + faces[4]
        plane["dg"][at(r), :] = -total
        plane["wxm"][at(r), :] = jnp.where(place == 0, zero, faces[0])
        plane["wxp"][at(r), :] = jnp.where(place == slabs - 1, zero, faces[1])
        plane["wym"][at(r), :] = jnp.where(row == 0, zero, faces[2])
        plane["wyp"][at(r), :] = jnp.where(row == rows - 1, zero, faces[3])
        plane["wzm"][at(r), :] = jnp.where(first_lane, zero, faces[4])
        plane["wzp"][at(r), :] = jnp.where(last_lane, zero, faces[5])
        return carry

    sweep(0, rows, weights, 0)

    def heat(name, r):
        mid, down, up = column(name, r)
        out = plane["wxp"][at(r), :] * side[name][1, at(r), :]
        out = out + plane["wxm"][at(r), :] * side[name][0, at(r), :]
        out = out + plane["wyp"][at(r), :] * up + plane["wym"][at(r), :] * down
        out = out + plane["wzp"][at(r), :] * to_right(mid) + plane["wzm"][at(r), :] * to_left(mid)
        return mid, out + plane["dg"][at(r), :] * mid

    def fold(x):
        return jnp.sum(x.reshape(BLOCK // 8, 8, cols), axis=0)

    nothing = jnp.zeros((8, cols), jnp.float32)

    def quadratic(name, beside, weight, r):
        mid, _, up = column(name, r)
        twice = plane[weight][at(r), :] * beside[at(r), :]
        twice = twice + plane["wyp"][at(r), :] * up + plane["wzp"][at(r), :] * to_right(mid)
        return fold(mid * (twice + twice + plane["dg"][at(r), :] * mid))

    def moments(name, beside, c):
        weight = "wxm" if c < CHUNKS // 2 else "wxp"
        beside = beside(0 if c < CHUNKS // 2 else 1)
        return sweep(c * chunk, chunk, lambda r, acc: acc + quadratic(name, beside, weight, r), nothing)

    spot = lax.broadcasted_iota(jnp.int32, (1, 128), 1)

    def lanes(acc):
        both = acc[:, 0:128]
        for i in range(1, cols // 128):
            both = both + acc[:, i * 128:(i + 1) * 128]
        return jnp.sum(both, axis=0, keepdims=True)

    def burst(src, slots, devices, sem):
        middle = (len(devices) - 1) / 2
        for k in sorted(range(len(devices)), key=lambda k: abs(k - middle)):
            pltpu.make_async_remote_copy(
                src_ref=src, dst_ref=slots.at[pl.ds(k, 1), :],
                send_sem=gsend.at[sem], recv_sem=grecv.at[sem],
                device_id=devices[k], device_id_type=MESH,
            ).start()
        whole = slots.at[pl.ds(0, len(devices)), :]
        return pltpu.make_async_remote_copy(
            src_ref=whole, dst_ref=whole, send_sem=gsend.at[sem], recv_sem=grecv.at[sem],
            device_id=after, device_id_type=MESH,
        )

    bursts = []

    def reduce_z(n, accs):
        rows_of = jnp.concatenate(
            [acc if acc.shape[0] == 1 else lanes(acc) for acc in accs + [nothing] * (8 - len(accs))], axis=0
        )
        sums = jnp.sum(rows_of, axis=1, keepdims=True)
        row = jnp.zeros((1, 128), jnp.float32)
        for q in range(len(accs)):
            row = jnp.where(spot == q, sums[q:q + 1, :], row)
        tiles[n, 0:1, :] = row
        devices = [z_peer(k) for k in range(1, nz)]
        waits = burst(tiles.at[n, pl.ds(0, 1), :], zslots.at[n], devices, 1 + 3 * n)
        bursts.append(waits)
        return waits

    def reduce_y(n, waits, also=False):
        waits.wait_recv()
        ztiles[n, 0:1, :] = tiles[n, 0:1, :] + jnp.sum(zslots[n, 0:nz - 1, :], axis=0, keepdims=True)
        src = ztiles.at[n, pl.ds(0, 1), :]
        out = [burst(src, yslots.at[n], [y_peer(k) for k in range(1, ny)], 2 + 3 * n)]
        if also:
            out.append(burst(src, xslots, [y_peer(k, next_t) for k in range(ny)], 3 + 3 * n))
        bursts.extend(out)
        return out

    def total_own(n, waits):
        waits.wait_recv()
        return ztiles[n, 0:1, :] + jnp.sum(yslots[n, 0:ny - 1, :], axis=0, keepdims=True)

    def total_last(waits):
        waits.wait_recv()
        return jnp.sum(xslots[0:ny, :], axis=0, keepdims=True)

    def factors(row, h):
        s0, s1, s2, s3 = row, pltpu.roll(row, 127, 1), pltpu.roll(row, 126, 1), pltpu.roll(row, 125, 1)
        sigma = s1 / s0
        spread = jnp.maximum(s2 - s1 * sigma, 1e-30)
        bent = s3 - sigma * (s2 + s2) + sigma * sigma * s1
        one = s0 / (s0 - h * s1)
        part = spread / s0
        two = 1.0 / jnp.maximum(1.0 - h * bent / spread - one * (h * h) * part, 1.0)
        slope = (one * h) * (one * h) * part
        c1 = one * two * h
        c0 = one + two * slope - c1 * sigma
        return c0, c1

    def whole(x):
        return jnp.concatenate([jnp.broadcast_to(x, (8, cols))] * (BLOCK // 8), axis=0)

    def first_fields(r, carry):
        mids, images = zip(*[heat("u%d" % j, r) for j in range(3)])
        begin = plane["s"][at(r), :]
        leads = [begin - mids[0], mids[0] - mids[1], mids[1] - mids[2]]
        rc = None
        for m, name in enumerate(["a", "b", "d"]):
            value = leads[m]
            for j in range(3):
                value = value + WEIGHT[m][j] * images[j]
            pad[name][pl.ds(PAD + r, BLOCK), :] = value
            rc = value if rc is None else rc + value
        plane["rc"][at(r), :] = rc
        return carry

    a_in, b_in, d_in, la_in = {}, {}, {}, {}
    for c in each:
        arrive(u_in[c])
        sweep(c * chunk, chunk, first_fields, 0)
        a_in[c] = swap("a", c)
    put(plane["rc"], plane["xrc"], next_device, 2, early)

    def first_heat(r, carry):
        s0, s1, s2 = carry
        mid, out = heat("a", r)
        pad["la"][pl.ds(PAD + r, BLOCK), :] = out
        return s0 + fold(mid * mid), s1 + fold(mid * out), s2 + fold(out * out)

    sums = (nothing,) * 3
    for c in each:
        arrive(a_in[c])
        sums = sweep(c * chunk, chunk, first_heat, sums)
        la_in[c] = swap("la", c)
    for c in each[:3]:
        b_in[c] = swap("b", c)

    def second_field(r, carry):
        plane["lb"][at(r), :] = heat("b", r)[1]
        return carry

    def take_b(chunks):
        for c in chunks:
            arrive(b_in[c])
            sweep(c * chunk, chunk, second_field, 0)

    def second_heat(r, carry):
        mid, out = heat("la", r)
        plane["lla"][at(r), :] = out
        return carry + fold(mid * out)

    s3 = nothing
    for c in each:
        arrive(la_in[c])
        s3 = sweep(c * chunk, chunk, second_heat, s3)
    z_wait = reduce_z(0, list(sums) + [s3])
    for c in each[3:]:
        b_in[c] = swap("b", c)
    for c in order[:4]:
        d_in[c] = swap("d", c)

    def third_field(r, carry):
        s0, s1, s2 = carry
        ld = heat("d", r)[1]
        rc = plane["rc"][at(r), :]
        vc = pad["la"][pl.ds(PAD + r, BLOCK), :] + plane["lb"][at(r), :] + ld
        plane["ld"][at(r), :] = ld
        pad["vc"][pl.ds(PAD + r, BLOCK), :] = vc
        return s0 + fold(rc * rc), s1 + fold(rc * vc), s2 + fold(vc * vc)

    coarse = (nothing,) * 3
    vc_in = {}

    def take_d(chunks, coarse):
        for c in chunks:
            arrive(d_in[c])
            coarse = sweep(c * chunk, chunk, third_field, coarse)
            onward(inner("vc", c * chunk, chunk), "xvc", c, early)
            if c >= half:
                vc_in[c - half] = give_half("vc", c - half)
        return coarse

    take_b(each[:4])
    (y_wait,) = reduce_y(0, z_wait)
    take_b(each[4:])
    c0, c1 = [whole(x[:, 0:1]) for x in factors(total_own(0, y_wait), WIDTH[0])]

    def second_node(r, carry):
        s0, s1, s2 = carry
        at_pad = pl.ds(PAD + r, BLOCK)
        a, la, lla = pad["a"][at_pad, :], pad["la"][at_pad, :], plane["lla"][at(r), :]
        move = c0 * a + c1 * la
        fine[0, at(r), :] = pad["u0"][at_pad, :] + move
        r2 = pad["b"][at_pad, :] + move
        v2 = plane["lb"][at(r), :] + c0 * la + c1 * lla
        plane["r2"][at(r), :] = r2
        pad["v2"][at_pad, :] = v2
        return s0 + fold(r2 * r2), s1 + fold(r2 * v2), s2 + fold(v2 * v2)

    sums = (nothing,) * 3
    v_in, w_in = {}, {}
    for c in order:
        sums = sweep(c * chunk, chunk, second_node, sums)
        if c >= half:
            v_in[c - half] = swap_half("v2", c - half, False)
    coarse = take_d(order[:4], coarse)
    w_in[0] = swap_half("v2", 0, True)
    s3 = nothing
    for i in range(half):
        arrive(v_in[i])
        for c in (i, i + half):
            s3 = s3 + moments("v2", lambda s: side["v2"].at[s], c)
    z_wait = reduce_z(1, list(sums) + [s3])
    for i in range(1, half):
        w_in[i] = swap_half("v2", i, True)
    for c in order[4:]:
        d_in[c] = swap("d", c)

    def third_heat(r, carry):
        plane["lv2"][at(r), :] = heat("v2", r)[1]
        return carry

    def take_w(pairs):
        for i in pairs:
            arrive(w_in[i])
            for c in (i, i + half):
                sweep(c * chunk, chunk, third_heat, 0)

    take_w(range(2))
    (y_wait,) = reduce_y(1, z_wait)
    take_w(range(2, half))
    coarse = take_d(order[4:6], coarse)
    e0, e1 = [whole(x[:, 0:1]) for x in factors(total_own(1, y_wait), WIDTH[1])]

    def third_node(r, carry):
        s0, s1, s2 = carry
        at_pad = pl.ds(PAD + r, BLOCK)
        r2, v2, lv2 = plane["r2"][at(r), :], pad["v2"][at_pad, :], plane["lv2"][at(r), :]
        move = e0 * r2 + e1 * v2
        fine[1, at(r), :] = pad["u1"][at_pad, :] + move
        r3 = pad["d"][at_pad, :] + move
        v3 = plane["ld"][at(r), :] + e0 * v2 + e1 * lv2
        plane["r3"][at(r), :] = r3
        pad["v3"][at_pad, :] = v3
        return s0 + fold(r3 * r3), s1 + fold(r3 * v3), s2 + fold(v3 * v3)

    sums = (nothing,) * 3
    v3_in = {}

    def take_node(chunks, sums):
        for c in chunks:
            sums = sweep(c * chunk, chunk, third_node, sums)
            if c >= half:
                v3_in[c - half] = give_half("v3", c - half)
            onward(plane["r3"].at[pl.ds(c * chunk, chunk), :], "xr3", c, late)
            onward(inner("v3", c * chunk, chunk), "xv3", c, late)
        return sums

    sums = take_node(order[:4], sums)
    coarse = take_d(order[6:], coarse)
    sums = take_node(order[4:], sums)
    coarse3, s3 = nothing, nothing
    for i in range(half):
        arrive(vc_in[i])
        for c in (i, i + half):
            coarse3 = coarse3 + moments("vc", lambda s: plane["hvc"], c)
    sums, coarse = [[lanes(acc) for acc in accs] for accs in (sums, coarse)]
    coarse3 = lanes(coarse3)
    for i in range(half):
        arrive(v3_in[i])
        for c in (i, i + half):
            s3 = s3 + moments("v3", lambda s: plane["hv3"], c)
    z_wait = reduce_z(2, list(sums) + [s3] + list(coarse) + [coarse3])
    expect(planes.at[pl.ds(0, 3)], 2, early).wait_recv()

    def first_slice(r, carry):
        plane["xu"][at(r), :] = jnp.where(me_t == 0, plane["s"][at(r), :], plane["xu"][at(r), :])
        return carry

    sweep(0, rows, first_slice, 0)
    y_wait, x_wait = reduce_y(2, z_wait, also=True)
    expect(planes.at[pl.ds(0, 2)], 2, late).wait_recv()
    expect(sides.at[pl.ds(1, len(SIDES) - 1)], 0, 0).wait_send()
    expect(planes.at[pl.ds(0, 2)], 1, 0).wait_send()
    expect(planes.at[pl.ds(0, 5)], 2, 0).wait_send()

    @pl.when(gives)
    def _():
        k_in.wait_send()
        spread(sides.at[pl.ds(0, 2), :, pl.ds(0, share * (nt - 1) // 2), :]).wait_send()

    for waits in bursts[:-2]:
        waits.wait_send()
    both = jnp.concatenate([total_own(2, y_wait), total_last(x_wait)], axis=0)
    width = jnp.where(lax.broadcasted_iota(jnp.int32, (2, 128), 1) == 4, STEP, WIDTH[2])
    f0, f1 = factors(both, width)
    g0, g1 = whole(f0[0:1, 0:1]), whole(f1[0:1, 0:1])
    passed = [x[1:2, q:q + 1] for q in (0, 4) for x in (f0, f1)]
    p0, p1, q0, q1 = [whole(jnp.where(me_t == 0, 0.0, x)) for x in passed]

    def last_node(r, carry):
        at_pad = pl.ds(PAD + r, BLOCK)
        fine[2, at(r), :] = pad["u2"][at_pad, :] + (g0 * plane["r3"][at(r), :] + g1 * pad["v3"][at_pad, :])
        guess = plane["xu"][at(r), :]
        following[at(r), :] = guess + (p0 * plane["xr3"][at(r), :] + p1 * plane["xv3"][at(r), :])
        coarse_next[at(r), :] = guess + (q0 * plane["xrc"][at(r), :] + q1 * plane["xvc"][at(r), :])
        return carry

    sweep(0, rows, last_node, 0)
    for waits in bursts[-2:]:
        waits.wait_send()


def slots_needed():
    return 1 + 2 + 5 * CHUNKS + 4 * (CHUNKS // 2)


def leave(fine, following, coarse, fine_hbm, following_hbm, coarse_hbm, sem):
    rows = following.shape[0] // 2
    pairs = [(fine.at[m], fine_hbm.at[m]) for m in range(3)]
    pairs += [(following, following_hbm), (coarse, coarse_hbm)]
    copies = []
    for src, dst in pairs:
        for first in (0, rows):
            part = pl.ds(first, rows)
            copies.append(
                pltpu.make_async_copy(src.at[part, :], dst.at[part, :], sem.at[len(copies)])
            )
    for copy in copies:
        copy.start()
    for copy in copies:
        copy.wait()


def on_device(dims, start_value, old_nodes, diffusivity):
    nt, ny, nz, rows, cols = dims
    anywhere = pl.BlockSpec(memory_space=pl.ANY)
    near = pl.BlockSpec(memory_space=pltpu.VMEM)
    plane = jax.ShapeDtypeStruct((rows, cols), jnp.float32)
    inputs = [
        pltpu.with_memory_space_constraint(value, pltpu.MemorySpace.HBM)
        for value in (
            start_value.reshape(rows, cols),
            old_nodes.reshape(3, rows, cols),
            diffusivity.reshape(rows, cols),
        )
    ]
    fine, following, coarse = pl.pallas_call(
        functools.partial(kernel, dims),
        out_shape=(jax.ShapeDtypeStruct((3, rows, cols), jnp.float32), plane, plane),
        in_specs=[anywhere] * 3,
        out_specs=(near,) * 3,
        scratch_shapes=[
            pltpu.VMEM((len(PADDED), rows + 2 * PAD, cols), jnp.float32),
            pltpu.VMEM((len(PLANES), rows, cols), jnp.float32),
            pltpu.VMEM((len(SIDES), 2, rows, cols), jnp.float32),
            pltpu.VMEM((3, 8, 128), jnp.float32),
            pltpu.VMEM((3, 8, 128), jnp.float32),
            pltpu.VMEM((3, 16, 128), jnp.float32),
            pltpu.VMEM((3, 8, 128), jnp.float32),
            pltpu.VMEM((8, 128), jnp.float32),
            pltpu.SemaphoreType.DMA((4,)),
            pltpu.SemaphoreType.DMA((slots_needed(),)),
            pltpu.SemaphoreType.DMA((10,)),
            pltpu.SemaphoreType.DMA((10,)),
            pltpu.SemaphoreType.DMA((5,)),
            pltpu.SemaphoreType.REGULAR((3,)),
        ],
        compiler_params=pltpu.CompilerParams(
            collective_id=0, has_side_effects=True, vmem_limit_bytes=40 * 1024 * 1024
        ),
    )(*inputs)
    fine, following, coarse = pl.pallas_call(
        leave,
        out_shape=(jax.ShapeDtypeStruct((3, rows, cols), jnp.float32), plane, plane),
        in_specs=[anywhere] * 3,
        out_specs=(anywhere,) * 3,
        scratch_shapes=[pltpu.SemaphoreType.DMA((10,))],
        compiler_params=pltpu.CompilerParams(vmem_limit_bytes=40 * 1024 * 1024),
    )(fine, following, coarse)
    return (
        fine.reshape(1, 3, 1, rows, cols),
        following.reshape(1, 1, rows, cols),
        coarse.reshape(1, 1, rows, cols),
    )


def build(split, rows, cols):
    dims = (split.shape["tm"], split.shape["y"], split.shape["z"], rows, cols)
    in_specs = (P("tm", SPACE, None, None), P("tm", None, SPACE, None, None), P(SPACE, None, None))
    out_specs = (
        P("tm", None, SPACE, None, None),
        P("tm", SPACE, None, None),
        P("tm", SPACE, None, None),
    )
    return jax.shard_map(
        functools.partial(on_device, dims), mesh=split, in_specs=in_specs, out_specs=out_specs,
        check_vma=False,
    )


def solution(mesh):
    split = Mesh(
        mesh.devices.reshape(mesh.shape["tm"], ROWS_Y, mesh.shape["space"] // ROWS_Y), ("tm",) + SPACE
    )
    return build(split, 512, 256)
```
